64 devices in a mesh: batch: 4 (over x, y), dap: 16 (over z, core).
Axes of the slice: x: 2, y: 2, z: 8, core: 2. Of those that a mesh axis runs over, the one named last changes fastest.
The devices are a block of a 4x4x8 slice.
Arguments:
- pair_act: bfloat16 [1024, 256, 128], P(('batch', 'dap')), parts along dimension 0
- pair_mask: int32 [1024, 256], P(('batch', 'dap')), parts along dimension 0
- msa_act: bfloat16 [512, 1024, 256], P(None, ('batch', 'dap')), parts along dimension 1
- opm_norm: bfloat16 [2, 2, 256], replicated
- opm_w_in: bfloat16 [2, 256, 2, 32], replicated
- opm_b_in: bfloat16 [2, 2, 32], replicated
- opm_w_out: bfloat16 [2, 1024, 128], replicated
- opm_b_out: bfloat16 [2, 128], replicated
- tri_norm_in: bfloat16 [2, 2, 128], replicated
- tri_w_ab: bfloat16 [2, 128, 4, 128], replicated
- tri_b_ab: bfloat16 [2, 4, 128], replicated
- tri_w_gate: bfloat16 [2, 128, 128], replicated
- tri_b_gate: bfloat16 [2, 128], replicated
- tri_norm_out: bfloat16 [2, 2, 128], replicated
- tri_w_out: bfloat16 [2, 128, 128], replicated
- tri_b_out: bfloat16 [2, 128], replicated
Outputs:
- output: bfloat16 [1024, 256, 128], P(('batch', 'dap')), parts along dimension 0
There are 4 independent parts. The reference program is written for one: setup_inputs(seed, part) draws one part's arguments, and reference() takes and returns one part's arrays. A program takes and returns all parts, laid end to end along the dimension named above; an argument that names none is the same for every part.
All inputs are finite; a program needn't handle non-finite values.
Results may differ from the reference program's by a relative error of at most 0.0106456.
Values are sent between devices in bfloat16 or wider.
A program may use at most 768 MiB of HBM per device.

```python
import jax
import jax.numpy as jnp
from jax import lax

RESIDUES = 256
MSA_ROWS = 512
PAIR_DIM = 128
TRI_DIM = 128
MSA_DIM = 256
OPM_DIM = 32
LAYERS = 2
ROW_BLOCK = 8

LN_EPS = 1e-5


def normal_draw(base_key, arr_shape, draw_scale):
    return (draw_scale * jax.random.normal(base_key, arr_shape, jnp.float32)).astype(jnp.bfloat16)


def norm_draw(base_key, arr_shape):
    noise_val = 0.3 * jax.random.normal(base_key, arr_shape, jnp.float32)
    return (noise_val + jnp.array([1.0, 0.0], jnp.float32)[None, :, None]).astype(jnp.bfloat16)


def setup_inputs(seed: int = 0, part: int = 0) -> dict:
    part_keys = jax.random.split(jax.random.fold_in(jax.random.key(seed), part), 6)
    weight_keys = jax.random.split(jax.random.key(seed + 1), 13)
    row_part = jax.random.normal(part_keys[0], (RESIDUES, 1, PAIR_DIM), jnp.float32)
    col_part = jax.random.normal(part_keys[1], (1, RESIDUES, PAIR_DIM), jnp.float32)
    pair_noise = jax.random.normal(part_keys[2], (RESIDUES, RESIDUES, PAIR_DIM), jnp.float32)
    pair_act = (0.6 * row_part + 0.6 * col_part + 0.5 * pair_noise).astype(jnp.bfloat16)
    profile = jax.random.normal(part_keys[3], (1, RESIDUES, MSA_DIM), jnp.float32)
    msa_noise = jax.random.normal(part_keys[4], (MSA_ROWS, RESIDUES, MSA_DIM), jnp.float32)
    msa_act = (0.8 * profile + 0.6 * msa_noise).astype(jnp.bfloat16)
    valid_len = RESIDUES // 2 + jax.random.randint(part_keys[5], (), 0, RESIDUES // 2 + 1)
    seq_valid = (jnp.arange(RESIDUES) < valid_len).astype(jnp.int32)
    pair_mask = seq_valid[:, None] * seq_valid[None, :]
    return {
        'pair_act': pair_act,
        'pair_mask': pair_mask,
        'msa_act': msa_act,
        'opm_norm': norm_draw(weight_keys[0], (LAYERS, 2, MSA_DIM)),
        'opm_w_in': normal_draw(weight_keys[1], (LAYERS, MSA_DIM, 2, OPM_DIM), MSA_DIM ** -0.5),
        'opm_b_in': normal_draw(weight_keys[2], (LAYERS, 2, OPM_DIM), 0.5),
        'opm_w_out': normal_draw(weight_keys[3], (LAYERS, OPM_DIM * OPM_DIM, PAIR_DIM), (OPM_DIM * OPM_DIM) ** -0.5),
        'opm_b_out': normal_draw(weight_keys[4], (LAYERS, PAIR_DIM), 0.5),
        'tri_norm_in': norm_draw(weight_keys[5], (LAYERS, 2, PAIR_DIM)),
        'tri_w_ab': normal_draw(weight_keys[6], (LAYERS, PAIR_DIM, 4, TRI_DIM), PAIR_DIM ** -0.5),
        'tri_b_ab': normal_draw(weight_keys[7], (LAYERS, 4, TRI_DIM), 0.3),
        'tri_w_gate': normal_draw(weight_keys[8], (LAYERS, PAIR_DIM, PAIR_DIM), PAIR_DIM ** -0.5),
        'tri_b_gate': normal_draw(weight_keys[9], (LAYERS, PAIR_DIM), 0.5),
        'tri_norm_out': norm_draw(weight_keys[10], (LAYERS, 2, TRI_DIM)),
        'tri_w_out': normal_draw(weight_keys[11], (LAYERS, TRI_DIM, PAIR_DIM), TRI_DIM ** -0.5),
        'tri_b_out': normal_draw(weight_keys[12], (LAYERS, PAIR_DIM), 0.5),
    }


def layer_norm(values, norm_gains):
    x_f32 = values.astype(jnp.float32)
    mean_val = jnp.mean(x_f32, axis=-1, keepdims=True)
    centered = x_f32 - mean_val
    var_val = jnp.mean(centered * centered, axis=-1, keepdims=True)
    scaled = centered * lax.rsqrt(var_val + LN_EPS)
    return (scaled * norm_gains[0].astype(jnp.float32) + norm_gains[1].astype(jnp.float32)).astype(jnp.bfloat16)


def outer_mean_update(pair_act, msa_act, norm_w, w_in, b_in, w_out, b_out):
    msa_norm = layer_norm(msa_act, norm_w).astype(jnp.float32)
    w_in_f = w_in.astype(jnp.float32)
    b_in_f = b_in.astype(jnp.float32)
    left_proj = (jnp.einsum('snm,mc->snc', msa_norm, w_in_f[:, 0, :]) + b_in_f[0]).astype(jnp.bfloat16).astype(jnp.float32)
    right_proj = (jnp.einsum('snm,mc->snc', msa_norm, w_in_f[:, 1, :]) + b_in_f[1]).astype(jnp.bfloat16).astype(jnp.float32)
    w_out_f = w_out.astype(jnp.float32).reshape(OPM_DIM, OPM_DIM, PAIR_DIM)
    b_out_f = b_out.astype(jnp.float32)
    num_blocks = RESIDUES // ROW_BLOCK
    left_blocks = jnp.moveaxis(left_proj.reshape(MSA_ROWS, num_blocks, ROW_BLOCK, OPM_DIM), 1, 0)
    pair_blocks = pair_act.reshape(num_blocks, ROW_BLOCK, RESIDUES, PAIR_DIM)

    def block_update(block_args):
        left_blk, pair_blk = block_args
        outer_prod = jnp.einsum('sic,sjd->ijcd', left_blk, right_proj) / MSA_ROWS
        outer_prod = outer_prod.astype(jnp.bfloat16).astype(jnp.float32)
        pair_upd = (jnp.einsum('ijcd,cdz->ijz', outer_prod, w_out_f) + b_out_f).astype(jnp.bfloat16)
        return (pair_blk.astype(jnp.float32) + pair_upd.astype(jnp.float32)).astype(jnp.bfloat16)

    return lax.map(block_update, (left_blocks, pair_blocks)).reshape(RESIDUES, RESIDUES, PAIR_DIM)


def triangle_update(pair_act, mask_f, norm_in, w_ab, b_ab, w_gate, b_gate, norm_out, w_out, b_out):
    num_blocks = RESIDUES // ROW_BLOCK
    pair_blocks = pair_act.reshape(num_blocks, ROW_BLOCK, RESIDUES, PAIR_DIM)
    mask_blocks = mask_f.reshape(num_blocks, ROW_BLOCK, RESIDUES)
    w_ab_f = w_ab.astype(jnp.float32)
    b_ab_f = b_ab.astype(jnp.float32)
    w_gate_f = w_gate.astype(jnp.float32)
    b_gate_f = b_gate.astype(jnp.float32)
    w_out_f = w_out.astype(jnp.float32)
    b_out_f = b_out.astype(jnp.float32)

    def project_block(block_args):
        pair_blk, mask_blk = block_args
        normed = layer_norm(pair_blk, norm_in).astype(jnp.float32)
        projected = jnp.einsum('ikz,zqc->qikc', normed, w_ab_f) + b_ab_f[:, None, None, :]
        mask_col = mask_blk[:, :, None]
        left_val = (mask_col * jax.nn.sigmoid(projected[1]) * projected[0]).astype(jnp.bfloat16)
        right_val = (mask_col * jax.nn.sigmoid(projected[3]) * projected[2]).astype(jnp.bfloat16)
        return left_val, right_val

    left_all, right_all = lax.map(project_block, (pair_blocks, mask_blocks))
    right_f = right_all.reshape(RESIDUES, RESIDUES, TRI_DIM).astype(jnp.float32)

    def update_block(block_args):
        pair_blk, left_blk = block_args
        normed = layer_norm(pair_blk, norm_in).astype(jnp.float32)
        gate_val = jax.nn.sigmoid(jnp.einsum('ikz,zy->iky', normed, w_gate_f) + b_gate_f)
        tri_prod = jnp.einsum('ikc,jkc->ijc', left_blk.astype(jnp.float32), right_f)
        prod_norm = layer_norm(tri_prod, norm_out).astype(jnp.float32)
        pair_upd = (jnp.einsum('ijc,cz->ijz', prod_norm, w_out_f) + b_out_f).astype(jnp.bfloat16)
        return (pair_blk.astype(jnp.float32) + gate_val * pair_upd.astype(jnp.float32)).astype(jnp.bfloat16)

    return lax.map(update_block, (pair_blocks, left_all)).reshape(RESIDUES, RESIDUES, PAIR_DIM)


def reference(pair_act, pair_mask, msa_act, opm_norm, opm_w_in, opm_b_in, opm_w_out, opm_b_out, tri_norm_in, tri_w_ab, tri_b_ab, tri_w_gate, tri_b_gate, tri_norm_out, tri_w_out, tri_b_out):
    mask_f = pair_mask.astype(jnp.float32)
    for layer_idx in range(LAYERS):
        pair_act = outer_mean_update(pair_act, msa_act, opm_norm[layer_idx], opm_w_in[layer_idx], opm_b_in[layer_idx], opm_w_out[layer_idx], opm_b_out[layer_idx])
        pair_act = triangle_update(pair_act, mask_f, tri_norm_in[layer_idx], tri_w_ab[layer_idx], tri_b_ab[layer_idx], tri_w_gate[layer_idx], tri_b_gate[layer_idx], tri_norm_out[layer_idx], tri_w_out[layer_idx], tri_b_out[layer_idx])
    return pair_act
```

```python
import functools

import jax
import jax.numpy as jnp
from jax import lax
from jax.experimental import pallas as pl
from jax.experimental.pallas import tpu as pltpu
from jax.sharding import PartitionSpec as P

F32 = jnp.float32
BF16 = jnp.bfloat16
EPS = 1e-5
VMEM_LIMIT = 63 * 1024 * 1024
NT = (((1,), (1,)), ((), ()))
LANES = 128

V_BQ, V_BP, V_BG, V_AP, V_AG, V_GATE, V_NI0, V_NI1, V_NO0, V_NO1, V_BO, V_BIN = range(12)


def sigmoid(x):
    return 1.0 / (1.0 + jnp.exp(-x))


def norm_rows(x, scale, offset):
    inv = 1.0 / x.shape[0]
    xc = x - jnp.sum(x, axis=0, keepdims=True) * inv
    var = jnp.sum(xc * xc, axis=0, keepdims=True) * inv
    return (xc * lax.rsqrt(var + EPS) * scale + offset).astype(BF16)


def twice(x):
    return jnp.concatenate([x, x], axis=1)


def project_kernel(m_ref, w_ref, norm_ref, bias_ref, a_ref, b_ref, scr):
    r = pl.program_id(0)
    layers, width = w_ref.shape[0], w_ref.shape[1] // 2
    seqs, dim = m_ref.shape[1], m_ref.shape[2]
    rows = b_ref.shape[1] // width
    x = m_ref[0].astype(F32)
    xc = x - jnp.sum(x, axis=1, keepdims=True) * (1.0 / dim)
    var = jnp.sum(xc * xc, axis=1, keepdims=True) * (1.0 / dim)
    xn = xc * lax.rsqrt(var + EPS)
    for l in range(layers):
        mn = (xn * norm_ref[l, 0:1] + norm_ref[l, 1:2]).astype(BF16)
        out = lax.dot_general(w_ref[l], mn, NT, preferred_element_type=F32)
        bias = bias_ref[l][: 2 * width]
        for c in range(seqs // LANES):
            part = out[:, c * LANES : (c + 1) * LANES] + bias
            a_ref[l, 0, :, c * LANES : (c + 1) * LANES] = part[:width].astype(BF16)
            scr[l, c, pl.ds(r, width, stride=rows), :] = part[width:]

    @pl.when(r == pl.num_programs(0) - 1)
    def _():
        for l in range(layers):
            for c in range(seqs // LANES):
                b_ref[l, :, c * LANES : (c + 1) * LANES] = scr[l, c].astype(BF16)


def opm_half(l, h, a_ref, b_ref, wq_ref, vec_ref, z_ref, q_ref):
    pairs, cd, lanes2 = q_ref.shape
    seqs = a_ref.shape[2]
    width = a_ref.shape[1] // (2 * pairs)
    half = lanes2 // 2
    scale = 1.0 / seqs

    def outer(t, _):
        rhs = b_ref[h, pl.ds(2 * t, 2)].reshape(2 * half, seqs)
        out = lax.dot_general(a_ref[l], rhs, NT, preferred_element_type=F32)
        out = (out * scale).astype(BF16)
        for d in range(2):
            blk = out[:, d * half : (d + 1) * half].reshape(2 * pairs, width, half)
            at = pl.ds(pl.multiple_of((2 * t + d) * width, width), width)
            for e in range(2):
                q_ref[:, at, e * half : (e + 1) * half] = blk[e * pairs : (e + 1) * pairs]
        return 0

    lax.fori_loop(0, cd // width // 2, outer, 0)
    bq = twice(vec_ref[l, V_BQ])

    def project(p, _):
        u = jnp.dot(wq_ref[l], q_ref[p], preferred_element_type=F32) + bq
        z_ref[h, p] = (z_ref[h, p].astype(F32) + u.astype(BF16).astype(F32)).astype(BF16)
        return 0

    lax.fori_loop(0, pairs, project, 0)


def gate_half(l, h, z_ref, mask_ref, wall_ref, vec_ref, fa_ref, fb_ref, g_ref, a_out, b_out):
    pairs = z_ref.shape[1]
    dim = z_ref.shape[2]
    half = z_ref.shape[3] // 2

    def project(p, _):
        zn = norm_rows(z_ref[h, p].astype(F32), twice(vec_ref[l, V_NI0]), twice(vec_ref[l, V_NI1]))
        mask = mask_ref[h, p]
        at = pl.ds(pl.multiple_of(p * dim, dim), dim)

        def proj(q, v):
            w = wall_ref[l, q * dim : (q + 1) * dim]
            return jnp.dot(w, zn, preferred_element_type=F32) + twice(vec_ref[l, v])

        for q, f_ref, vp, vg in ((0, fb_ref, V_BP, V_BG), (2, fa_ref, V_AP, V_AG)):
            val = mask * sigmoid(proj(q + 1, vg)) * proj(q, vp)
            f_ref[0, at, :] = val[:, :half]
            f_ref[1, at, :] = val[:, half:]
        g_ref[h, p] = sigmoid(proj(4, V_GATE))
        return 0

    lax.fori_loop(0, pairs, project, 0)

    def relayout(t, _):
        for u in range(8):
            c = t * 8 + u
            for f_ref, out in ((fb_ref, b_out), (fa_ref, a_out)):
                lo = f_ref[0, pl.ds(c, pairs, stride=dim), :]
                hi = f_ref[1, pl.ds(c, pairs, stride=dim), :]
                out(c, h, jnp.concatenate([lo, hi], axis=0).astype(BF16))
        return 0

    lax.fori_loop(0, dim // 8, relayout, 0)


def triangle_half(jh, a_ref, b_ref, o_ref):
    dim = a_ref.shape[0]
    pairs = a_ref.shape[1] // 2

    def step(t, _):
        for u in range(8):
            c = t * 8 + u
            o = lax.dot_general(a_ref[c], b_ref[jh, c], NT, preferred_element_type=F32)
            o_ref[0, pl.ds(c, pairs, stride=dim), :] = o[:pairs]
            o_ref[1, pl.ds(c, pairs, stride=dim), :] = o[pairs:]
        return 0

    lax.fori_loop(0, dim // 8, step, 0)


def finish_half(l, jh, o_ref, g_ref, z_ref, wo_ref, vec_ref):
    pairs = z_ref.shape[1]
    dim = z_ref.shape[2]

    def step(p, _):
        at = pl.ds(pl.multiple_of(p * dim, dim), dim)
        o = jnp.concatenate([o_ref[0, at, :], o_ref[1, at, :]], axis=1)
        on = norm_rows(o, twice(vec_ref[l, V_NO0]), twice(vec_ref[l, V_NO1]))
        u = jnp.dot(wo_ref[l], on, preferred_element_type=F32) + twice(vec_ref[l, V_BO])
        z_ref[jh, p] = (z_ref[jh, p].astype(F32) + g_ref[jh, p] * u.astype(BF16).astype(F32)).astype(BF16)
        return 0

    lax.fori_loop(0, pairs, step, 0)


def collect(src_ref, dst_ref, sem):
    devices, _, rows, _ = src_ref.shape
    copies = []
    for d in range(devices):
        dst = dst_ref.at[d % 2, :, pl.ds((d // 2) * rows, rows), :]
        copies.append(pltpu.make_async_copy(src_ref.at[d], dst, sem.at[d]))
    for copy in copies:
        copy.start()
    for copy in copies:
        copy.wait()


def head_kernel(l, b_hbm, a_ref, z_in, mask_ref, wq_ref, wall_ref, vec_ref, z_ref, at_ref, bt_ref, g_ref,
                b_buf, q_scr, fa, fb, sem):
    collect(b_hbm, b_buf, sem)
    z_ref[...] = z_in[...]

    def a_out(c, h, v):
        at_ref[c, :, h * LANES : (h + 1) * LANES] = v

    def b_out(c, h, v):
        bt_ref[c, :, h * LANES : (h + 1) * LANES] = v

    for h in range(2):
        opm_half(l, h, a_ref, b_buf, wq_ref, vec_ref, z_ref, q_scr)
        gate_half(l, h, z_ref, mask_ref, wall_ref, vec_ref, fa, fb, g_ref, a_out, b_out)


def tail_kernel(l, bt_hbm, at_ref, g_ref, z_in, wo_ref, vec_ref, z_ref, b_buf, o_scr, sem):
    collect(bt_hbm, b_buf, sem)
    z_ref[...] = z_in[...]
    for jh in range(2):
        triangle_half(jh, at_ref, b_buf, o_scr)
        finish_half(l, jh, o_scr, g_ref, z_ref, wo_ref, vec_ref)


def solution(mesh):
    size = mesh.shape["dap"]
    chips = size // 2
    pair_spec = P(("batch", "dap"), None, None)
    mask_spec = P(("batch", "dap"), None)
    msa_spec = P(None, ("batch", "dap"), None)
    any_spec = pl.BlockSpec(memory_space=pl.ANY)
    vmem_spec = pl.BlockSpec(memory_space=pltpu.VMEM)

    def device_fn(pair_act, pair_mask, msa_act, opm_norm, opm_w_in, opm_b_in, opm_w_out, opm_b_out, tri_norm_in,
                  tri_w_ab, tri_b_ab, tri_w_gate, tri_b_gate, tri_norm_out, tri_w_out, tri_b_out):
        rows, cols, dim = pair_act.shape
        seqs, _, mdim = msa_act.shape
        layers = opm_norm.shape[0]
        width = opm_w_in.shape[-1]
        pairs = rows // 2
        half = cols // 2

        w_in = jnp.transpose(opm_w_in, (0, 2, 3, 1)).reshape(layers, 2 * width, mdim)
        wq = jnp.transpose(opm_w_out.reshape(layers, width, width, dim), (0, 3, 2, 1)).reshape(layers, dim, -1)
        w5 = jnp.concatenate([tri_w_ab[:, :, 2:4], tri_w_ab[:, :, 0:2], tri_w_gate[:, :, None]], axis=2)
        wall = jnp.transpose(w5, (0, 2, 3, 1)).reshape(layers, 5 * dim, dim)
        wo = jnp.transpose(tri_w_out, (0, 2, 1))
        b_in = jnp.pad(opm_b_in.reshape(layers, 1, 2 * width), ((0, 0), (0, 0), (0, dim - 2 * width)))
        vec = jnp.concatenate([opm_b_out[:, None], tri_b_ab[:, 2:4], tri_b_ab[:, 0:2], tri_b_gate[:, None],
                               tri_norm_in, tri_norm_out, tri_b_out[:, None], b_in], axis=1).astype(F32)
        vec = jnp.broadcast_to(vec[..., None], vec.shape + (LANES,))

        z = pair_act.reshape(2, pairs, chips, 2, rows, dim)
        z = jnp.transpose(z, (3, 1, 5, 0, 2, 4)).reshape(2, pairs, dim, 2 * half)
        mask = pair_mask.astype(F32).reshape(2, pairs, chips, 2, rows)
        mask = jnp.transpose(mask, (3, 1, 0, 2, 4)).reshape(2, pairs, 1, 2 * half)
        m = jnp.swapaxes(msa_act, 0, 1)

        a, b = pl.pallas_call(
            project_kernel,
            grid=(rows,),
            out_shape=(jax.ShapeDtypeStruct((layers, rows, width, seqs), BF16),
                       jax.ShapeDtypeStruct((layers, width * rows, seqs), BF16)),
            in_specs=[pl.BlockSpec((1, seqs, mdim), lambda r: (r, 0, 0)),
                      pl.BlockSpec(w_in.shape, lambda r: (0, 0, 0)),
                      pl.BlockSpec(opm_norm.shape, lambda r: (0, 0, 0)),
                      pl.BlockSpec((layers, dim, LANES), lambda r: (0, 0, 0))],
            out_specs=(pl.BlockSpec((layers, 1, width, seqs), lambda r: (0, r, 0, 0)),
                       pl.BlockSpec((layers, width * rows, seqs), lambda r: (0, 0, 0))),
            scratch_shapes=[pltpu.VMEM((layers, seqs // LANES, width * rows, LANES), F32)],
            compiler_params=pltpu.CompilerParams(vmem_limit_bytes=VMEM_LIMIT),
            name="project",
        )(m, w_in, opm_norm.astype(F32), vec[:, V_BIN])
        a = a.reshape(layers, rows * width, seqs)
        b = b.reshape(layers, width, rows, seqs)

        z_shape = jax.ShapeDtypeStruct((2, pairs, dim, 2 * half), BF16)
        t_shape = jax.ShapeDtypeStruct((dim, rows, cols), BF16)
        g_shape = jax.ShapeDtypeStruct((2, pairs, dim, 2 * half), F32)
        gathered = [lax.all_gather(b[l], "dap") for l in range(layers)]
        for l in range(layers):
            z, at, bt, g = pl.pallas_call(
                functools.partial(head_kernel, l),
                out_shape=(z_shape, t_shape, t_shape, g_shape),
                in_specs=[any_spec] + [vmem_spec] * 6,
                out_specs=(vmem_spec,) * 4,
                scratch_shapes=[pltpu.VMEM((2, width, half, seqs), BF16),
                                pltpu.VMEM((pairs, width * width, 2 * half), BF16),
                                pltpu.VMEM((2, pairs * dim, LANES), F32),
                                pltpu.VMEM((2, pairs * dim, LANES), F32),
                                pltpu.SemaphoreType.DMA((size,))],
                compiler_params=pltpu.CompilerParams(vmem_limit_bytes=VMEM_LIMIT),
                name="head",
            )(gathered[l], a, z, mask, wq, wall, vec)
            bt = lax.all_gather(bt, "dap")
            z = pl.pallas_call(
                functools.partial(tail_kernel, l),
                out_shape=z_shape,
                in_specs=[any_spec] + [vmem_spec] * 5,
                out_specs=vmem_spec,
                scratch_shapes=[pltpu.VMEM((2, dim, half, cols), BF16),
                                pltpu.VMEM((2, pairs * dim, LANES), F32),
                                pltpu.SemaphoreType.DMA((size,))],
                compiler_params=pltpu.CompilerParams(vmem_limit_bytes=VMEM_LIMIT),
                name="tail",
            )(bt, at, g, z, wo, vec)
        out = z.reshape(2, pairs, dim, 2, chips, rows)
        return jnp.transpose(out, (3, 1, 4, 0, 5, 2)).reshape(rows, cols, dim)

    return jax.shard_map(device_fn, mesh=mesh, in_specs=(pair_spec, mask_spec, msa_spec) + (P(),) * 13,
                         out_specs=pair_spec, check_vma=False)
```

```python
import functools

import jax
import jax.numpy as jnp
from jax import lax
from jax.experimental import pallas as pl
from jax.experimental.pallas import tpu as pltpu
from jax.sharding import PartitionSpec as P

F32 = jnp.float32
BF16 = jnp.bfloat16
EPS = 1e-5
VMEM_LIMIT = 63 * 1024 * 1024
NT = (((1,), (1,)), ((), ()))
LANES = 128

V_BQ, V_BP, V_BG, V_AP, V_AG, V_GATE, V_NI0, V_NI1, V_NO0, V_NO1, V_BO, V_BIN = range(12)


def sigmoid(x):
    return 1.0 / (1.0 + jnp.exp(-x))


def norm_rows(x, scale, offset):
    inv = 1.0 / x.shape[0]
    xc = x - jnp.sum(x, axis=0, keepdims=True) * inv
    var = jnp.sum(xc * xc, axis=0, keepdims=True) * inv
    return (xc * lax.rsqrt(var + EPS) * scale + offset).astype(BF16)


def twice(x):
    return jnp.concatenate([x, x], axis=1)


def project_kernel(m_ref, w_ref, norm_ref, bias_ref, a_ref, b_ref, scr):
    r = pl.program_id(0)
    layers, width = w_ref.shape[0], w_ref.shape[1] // 2
    seqs, dim = m_ref.shape[1], m_ref.shape[2]
    rows = b_ref.shape[1] // width
    x = m_ref[0].astype(F32)
    xc = x - jnp.sum(x, axis=1, keepdims=True) * (1.0 / dim)
    var = jnp.sum(xc * xc, axis=1, keepdims=True) * (1.0 / dim)
    xn = xc * lax.rsqrt(var + EPS)
    for l in range(layers):
        mn = (xn * norm_ref[l, 0:1] + norm_ref[l, 1:2]).astype(BF16)
        out = lax.dot_general(w_ref[l], mn, NT, preferred_element_type=F32)
        bias = bias_ref[l][: 2 * width]
        for c in range(seqs // LANES):
            part = out[:, c * LANES : (c + 1) * LANES] + bias
            a_ref[l, 0, :, c * LANES : (c + 1) * LANES] = part[:width].astype(BF16)
            scr[l, c, pl.ds(r, width, stride=rows), :] = part[width:]

    @pl.when(r == pl.num_programs(0) - 1)
    def _():
        for l in range(layers):
            for c in range(seqs // LANES):
                b_ref[l, :, c * LANES : (c + 1) * LANES] = scr[l, c].astype(BF16)


def opm_half(l, h, a_ref, b_ref, wq_ref, vec_ref, z_ref, q_ref):
    pairs, cd, lanes2 = q_ref.shape
    seqs = a_ref.shape[2]
    width = a_ref.shape[1] // (2 * pairs)
    half = lanes2 // 2
    scale = 1.0 / seqs

    def outer(t, _):
        rhs = b_ref[h, pl.ds(2 * t, 2)].reshape(2 * half, seqs)
        out = lax.dot_general(a_ref[l], rhs, NT, preferred_element_type=F32)
        out = (out * scale).astype(BF16)
        for d in range(2):
            blk = out[:, d * half : (d + 1) * half].reshape(2 * pairs, width, half)
            at = pl.ds(pl.multiple_of((2 * t + d) * width, width), width)
            for e in range(2):
                q_ref[:, at, e * half : (e + 1) * half] = blk[e * pairs : (e + 1) * pairs]
        return 0

    lax.fori_loop(0, cd // width // 2, outer, 0)
    bq = twice(vec_ref[l, V_BQ])

    def project(p, _):
        u = jnp.dot(wq_ref[l], q_ref[p], preferred_element_type=F32) + bq
        z_ref[h, p] = (z_ref[h, p].astype(F32) + u.astype(BF16).astype(F32)).astype(BF16)
        return 0

    lax.fori_loop(0, pairs, project, 0)


def gate_half(l, h, z_ref, mask_ref, wall_ref, vec_ref, fa_ref, fb_ref, g_ref, a_out, b_out):
    pairs = z_ref.shape[1]
    dim = z_ref.shape[2]
    half = z_ref.shape[3] // 2

    def project(p, _):
        zn = norm_rows(z_ref[h, p].astype(F32), twice(vec_ref[l, V_NI0]), twice(vec_ref[l, V_NI1]))
        mask = mask_ref[h, p]
        at = pl.ds(pl.multiple_of(p * dim, dim), dim)

        def proj(q, v):
            w = wall_ref[l, q * dim : (q + 1) * dim]
            return jnp.dot(w, zn, preferred_element_type=F32) + twice(vec_ref[l, v])

        for q, f_ref, vp, vg in ((0, fb_ref, V_BP, V_BG), (2, fa_ref, V_AP, V_AG)):
            val = mask * sigmoid(proj(q + 1, vg)) * proj(q, vp)
            f_ref[0, at, :] = val[:, :half]
            f_ref[1, at, :] = val[:, half:]
        g_ref[h, p] = sigmoid(proj(4, V_GATE))
        return 0

    lax.fori_loop(0, pairs, project, 0)

    for f_ref, out in ((fb_ref, b_out), (fa_ref, a_out)):
        def relayout(t, _):
            for u in range(8):
                c = t * 8 + u
                lo = f_ref[0, pl.ds(c, pairs, stride=dim), :]
                hi = f_ref[1, pl.ds(c, pairs, stride=dim), :]
                out(c, h, jnp.concatenate([lo, hi], axis=0).astype(BF16))
            return 0

        lax.fori_loop(0, dim // 8, relayout, 0)


def triangle_half(jh, a_ref, b_ref, o_ref):
    dim = a_ref.shape[0]
    pairs = a_ref.shape[1] // 2

    def step(t, _):
        for u in range(8):
            c = t * 8 + u
            o = lax.dot_general(a_ref[c], b_ref[jh, c], NT, preferred_element_type=F32)
            o_ref[0, pl.ds(c, pairs, stride=dim), :] = o[:pairs]
            o_ref[1, pl.ds(c, pairs, stride=dim), :] = o[pairs:]
        return 0

    lax.fori_loop(0, dim // 8, step, 0)


def finish_half(l, jh, o_ref, g_ref, z_ref, wo_ref, vec_ref):
    pairs = z_ref.shape[1]
    dim = z_ref.shape[2]

    def step(p, _):
        at = pl.ds(pl.multiple_of(p * dim, dim), dim)
        o = jnp.concatenate([o_ref[0, at, :], o_ref[1, at, :]], axis=1)
        on = norm_rows(o, twice(vec_ref[l, V_NO0]), twice(vec_ref[l, V_NO1]))
        u = jnp.dot(wo_ref[l], on, preferred_element_type=F32) + twice(vec_ref[l, V_BO])
        z_ref[jh, p] = (z_ref[jh, p].astype(F32) + g_ref[jh, p] * u.astype(BF16).astype(F32)).astype(BF16)
        return 0

    lax.fori_loop(0, pairs, step, 0)


class Stream:
    def __init__(self, buf, color, lo, lanes, rows, sems, where):
        self.buf, self.color, self.rows, self.lanes = buf, color, rows, lanes
        self.base, self.size = lo
        self.part = buf.shape[0] // 2
        self.ring_send, self.ring_recv, self.core_send, self.core_recv = sems
        self.chip, self.core, self.chips = where
        self.sent = []

    def block(self, chip, part, piece=None):
        lo, n = part * self.part + self.base, self.size
        if piece is not None:
            n = n // 2
            lo = lo + piece * n
        rows = pl.ds(pl.multiple_of(chip * self.rows, self.rows), self.rows)
        return self.buf.at[pl.ds(lo, n), rows, self.lanes]

    def copy(self, ref, send, recv, chip, core):
        return pltpu.make_async_remote_copy(
            src_ref=ref, dst_ref=ref, send_sem=send, recv_sem=recv,
            device_id={"dap": chip * 2 + core}, device_id_type=pl.DeviceIdType.MESH)

    def near(self, step):
        return lax.rem(self.chip + step + self.chips, self.chips)

    def ring(self, side, hop, chip, piece=None):
        return self.copy(self.block(chip, self.core, piece), self.ring_send.at[side, hop], self.ring_recv.at[side, hop],
                         self.near(1 - 2 * side), self.core)

    def across(self, slot, chip, part, piece=None):
        return self.copy(self.block(chip, part, piece), self.core_send.at[slot], self.core_recv.at[slot],
                         self.chip, 1 - self.core)

    def event(self, hop):
        if hop == 0:
            @pl.when(self.core == self.color)
            def _():
                self.across(0, self.chip, 1 - self.core).start()
                for side in range(2):
                    self.ring(side, 0, self.chip).start()
                self.across(1, self.chip, self.core).start()

            @pl.when(self.core != self.color)
            def _():
                self.across(0, self.chip, self.core).wait_recv()
                for side in range(2):
                    self.ring(side, 0, self.chip).start()
            return
        last = self.chips // 2
        for side in range(2):
            origin = self.near((2 * side - 1) * hop)
            piece = side if hop == last else None
            self.ring(side, hop - 1, origin, piece).wait_recv()
            if hop < last:
                self.ring(side, hop, origin, side if hop == last - 1 else None).start()
            self.across(2 + 2 * (hop - 1) + side, origin, self.core, piece).start()

    def finish(self):
        last = self.chips // 2

        @pl.when(self.core != self.color)
        def _():
            self.across(1, self.chip, 1 - self.core).wait_recv()

        for hop in range(1, last + 1):
            for side in range(2):
                origin = self.near((2 * side - 1) * hop)
                piece = side if hop == last else None
                self.across(2 + 2 * (hop - 1) + side, origin, 1 - self.core, piece).wait_recv()

    def drain(self):
        last = self.chips // 2

        @pl.when(self.core == self.color)
        def _():
            self.across(0, self.chip, 1 - self.core).wait_send()
            self.across(1, self.chip, self.core).wait_send()

        for side in range(2):
            for hop in range(last):
                self.ring(side, hop, self.chip, side if hop == last - 1 else None).wait_send()
            for hop in range(1, last + 1):
                self.across(2 + 2 * (hop - 1) + side, self.chip, self.core, side if hop == last else None).wait_send()


N_STREAMS = 12


def step_kernel(chips, a_hbm, b_hbm, z_hbm, mask_ref, wq_ref, wall_ref, wo_ref, vec_ref, out_hbm,
                b_buf, t_buf, a_ref, z_ref, at_ref, g_ref, q_scr, fa, fb,
                ring_send, ring_recv, core_send, core_recv, local_sem):
    me = lax.axis_index("dap")
    chip, core = me // 2, lax.rem(me, 2)
    rows = b_hbm.shape[2]
    own = pl.ds(pl.multiple_of(chip * rows, rows), rows)
    layers = b_hbm.shape[0]
    dim = at_ref.shape[1]
    half = z_ref.shape[3] // 2

    barrier = pltpu.get_barrier_semaphore()
    right, left = lax.rem(chip + 1, chips), lax.rem(chip + chips - 1, chips)
    for there in (right * 2 + core, left * 2 + core, chip * 2 + 1 - core):
        pl.semaphore_signal(barrier, inc=1, device_id={"dap": there}, device_id_type=pl.DeviceIdType.MESH)

    loads = [pltpu.make_async_copy(b_hbm.at[l], b_buf.at[l, core, :, own, :], local_sem.at[l]) for l in range(layers)]
    loads.append(pltpu.make_async_copy(a_hbm, a_ref, local_sem.at[2]))
    loads.append(pltpu.make_async_copy(z_hbm, z_ref, local_sem.at[3]))
    for load in loads:
        load.start()
    pl.semaphore_wait(barrier, 3)

    where = (chip, core, chips)

    def stream(n, buf, color, lo, lanes):
        sems = tuple(s.at[n] for s in (ring_send, ring_recv, core_send, core_recv))
        return Stream(buf, color, lo, lanes, rows, sems, where)

    width = b_buf.shape[2]
    full_b = pl.ds(0, b_buf.shape[4])
    full_t = pl.ds(0, 2 * half)
    b1 = [stream(q, b_buf.at[0, q], q, (0, width // 2), full_b) for q in range(2)]
    b2 = [stream(2 + q, b_buf.at[1, q], q, (0, width // 2), full_b) for q in range(2)]
    t1 = [[stream(4 + 2 * q + s, t_buf.at[0, q], q, (s * dim // 4, dim // 4), full_t) for s in range(2)]
          for q in range(2)]
    t2 = [[stream(8 + 2 * k + q, t_buf.at[1, q], q, (0, dim // 2), pl.ds(k * half, half)) for q in range(2)]
          for k in range(2)]

    def opm(l, h):
        opm_half(l, h, a_ref, b_buf.at[l], wq_ref, vec_ref, z_ref, q_scr)

    def gate(l, h):
        def a_out(c, h, v):
            at_ref[l, c, :, h * LANES : (h + 1) * LANES] = v

        def b_out(c, h, v):
            t_buf[l, core, c, own, h * LANES : (h + 1) * LANES] = v

        gate_half(l, h, z_ref, mask_ref, wall_ref, vec_ref, fa, fb, g_ref, a_out, b_out)

    def triangle(l, jh):
        triangle_half(jh, at_ref.at[l], t_buf.at[l], fa)

    def finish(l, jh):
        finish_half(l, jh, fa, g_ref, z_ref, wo_ref, vec_ref)

    def events(hop, *streams):
        for s in streams:
            s.event(hop)

    loads[0].wait()
    events(0, *b1)
    loads[1].wait()
    events(1, *b1)
    events(2, *b1)
    loads[2].wait()
    loads[3].wait()
    events(3, *b1)
    events(0, *b2)
    events(4, *b1)
    b1[0].finish()
    opm(0, 0)
    events(1, b2[0])
    b1[1].finish()
    opm(0, 1)
    events(1, b2[1])
    gate(0, 0)
    events(2, b2[0])
    gate(0, 1)
    events(2, b2[1])
    events(0, *t1[0])
    events(3, *b2)
    events(1, *t1[0])
    events(4, *b2)
    events(2, *t1[0])
    events(0, *t1[1])
    events(3, *t1[0])
    events(4, *t1[0])
    for s in t1[0]:
        s.finish()
    triangle(0, 0)
    events(1, *t1[1])
    finish(0, 0)
    events(2, t1[1][0])
    for s in b2:
        s.finish()
    opm(1, 0)
    events(2, t1[1][1])
    events(3, *t1[1])
    gate(1, 0)
    events(0, *t2[0])
    events(4, *t1[1])
    for s in t1[1]:
        s.finish()
    triangle(0, 1)
    finish(0, 1)
    events(1, *t2[0])
    opm(1, 1)
    events(2, *t2[0])
    gate(1, 1)
    events(0, *t2[1])
    events(3, *t2[0])
    events(1, *t2[1])
    events(4, *t2[0])
    events(2, *t2[1])
    events(3, *t2[1])
    events(4, *t2[1])
    for q in range(2):
        t2[0][q].finish()
        t2[1][q].finish()
        triangle(1, q)
        finish(1, q)
        store = pltpu.make_async_copy(z_ref.at[q], out_hbm.at[q], local_sem.at[q])
        store.start()
    for s in b1 + b2 + t1[0] + t1[1] + t2[0] + t2[1]:
        s.drain()
    for q in range(2):
        pltpu.make_async_copy(z_ref.at[q], out_hbm.at[q], local_sem.at[q]).wait()


def solution(mesh):
    size = mesh.shape["dap"]
    chips = size // 2
    pair_spec = P(("batch", "dap"), None, None)
    mask_spec = P(("batch", "dap"), None)
    msa_spec = P(None, ("batch", "dap"), None)
    any_spec = pl.BlockSpec(memory_space=pl.ANY)
    vmem_spec = pl.BlockSpec(memory_space=pltpu.VMEM)

    def device_fn(pair_act, pair_mask, msa_act, opm_norm, opm_w_in, opm_b_in, opm_w_out, opm_b_out, tri_norm_in,
                  tri_w_ab, tri_b_ab, tri_w_gate, tri_b_gate, tri_norm_out, tri_w_out, tri_b_out):
        rows, cols, dim = pair_act.shape
        seqs, _, mdim = msa_act.shape
        layers = opm_norm.shape[0]
        width = opm_w_in.shape[-1]
        pairs = rows // 2
        half = cols // 2

        w_in = jnp.transpose(opm_w_in, (0, 2, 3, 1)).reshape(layers, 2 * width, mdim)
        wq = jnp.transpose(opm_w_out.reshape(layers, width, width, dim), (0, 3, 2, 1)).reshape(layers, dim, -1)
        w5 = jnp.concatenate([tri_w_ab[:, :, 2:4], tri_w_ab[:, :, 0:2], tri_w_gate[:, :, None]], axis=2)
        wall = jnp.transpose(w5, (0, 2, 3, 1)).reshape(layers, 5 * dim, dim)
        wo = jnp.transpose(tri_w_out, (0, 2, 1))
        b_in = jnp.pad(opm_b_in.reshape(layers, 1, 2 * width), ((0, 0), (0, 0), (0, dim - 2 * width)))
        vec = jnp.concatenate([opm_b_out[:, None], tri_b_ab[:, 2:4], tri_b_ab[:, 0:2], tri_b_gate[:, None],
                               tri_norm_in, tri_norm_out, tri_b_out[:, None], b_in], axis=1).astype(F32)
        vec = jnp.broadcast_to(vec[..., None], vec.shape + (LANES,))

        z = pair_act.reshape(2, pairs, chips, 2, rows, dim)
        z = jnp.transpose(z, (3, 1, 5, 0, 2, 4)).reshape(2, pairs, dim, 2 * half)
        mask = pair_mask.astype(F32).reshape(2, pairs, chips, 2, rows)
        mask = jnp.transpose(mask, (3, 1, 0, 2, 4)).reshape(2, pairs, 1, 2 * half)
        m = jnp.swapaxes(msa_act, 0, 1)

        a, b = pl.pallas_call(
            project_kernel,
            grid=(rows,),
            out_shape=(jax.ShapeDtypeStruct((layers, rows, width, seqs), BF16),
                       jax.ShapeDtypeStruct((layers, width * rows, seqs), BF16)),
            in_specs=[pl.BlockSpec((1, seqs, mdim), lambda r: (r, 0, 0)),
                      pl.BlockSpec(w_in.shape, lambda r: (0, 0, 0)),
                      pl.BlockSpec(opm_norm.shape, lambda r: (0, 0, 0)),
                      pl.BlockSpec((layers, dim, LANES), lambda r: (0, 0, 0))],
            out_specs=(pl.BlockSpec((layers, 1, width, seqs), lambda r: (0, r, 0, 0)),
                       pl.BlockSpec((layers, width * rows, seqs), lambda r: (0, 0, 0))),
            scratch_shapes=[pltpu.VMEM((layers, seqs // LANES, width * rows, LANES), F32)],
            compiler_params=pltpu.CompilerParams(vmem_limit_bytes=VMEM_LIMIT),
            name="project",
        )(m, w_in, opm_norm.astype(F32), vec[:, V_BIN])
        a = a.reshape(layers, rows * width, seqs)
        b = b.reshape(layers, width, rows, seqs)

        hops = chips // 2
        z = pl.pallas_call(
            functools.partial(step_kernel, chips),
            out_shape=jax.ShapeDtypeStruct(z.shape, BF16),
            in_specs=[any_spec] * 3 + [vmem_spec] * 5,
            out_specs=any_spec,
            scratch_shapes=[pltpu.VMEM((layers, 2, width, half, seqs), BF16),
                            pltpu.VMEM((layers, 2, dim, half, cols), BF16),
                            pltpu.VMEM(a.shape, BF16),
                            pltpu.VMEM(z.shape, BF16),
                            pltpu.VMEM((layers, dim, rows, cols), BF16),
                            pltpu.VMEM(z.shape, F32),
                            pltpu.VMEM((pairs, width * width, 2 * half), BF16),
                            pltpu.VMEM((2, pairs * dim, LANES), F32),
                            pltpu.VMEM((2, pairs * dim, LANES), F32),
                            pltpu.SemaphoreType.DMA((N_STREAMS, 2, hops)),
                            pltpu.SemaphoreType.DMA((N_STREAMS, 2, hops)),
                            pltpu.SemaphoreType.DMA((N_STREAMS, 2 + 2 * hops)),
                            pltpu.SemaphoreType.DMA((N_STREAMS, 2 + 2 * hops)),
                            pltpu.SemaphoreType.DMA((4,))],
            compiler_params=pltpu.CompilerParams(vmem_limit_bytes=VMEM_LIMIT, collective_id=0, has_side_effects=True),
            name="layers",
        )(a, b, z, mask, wq, wall, wo, vec)
        out = z.reshape(2, pairs, dim, 2, chips, rows)
        return jnp.transpose(out, (3, 1, 4, 0, 5, 2)).reshape(rows, cols, dim)

    return jax.shard_map(device_fn, mesh=mesh, in_specs=(pair_spec, mask_spec, msa_spec) + (P(),) * 13,
                         out_specs=pair_spec, check_vma=False)
```

```python
import functools
import math

import jax
import jax.numpy as jnp
from jax import lax
from jax.experimental import pallas as pl
from jax.experimental.pallas import tpu as pltpu
from jax.sharding import PartitionSpec as P

F32 = jnp.float32
BF16 = jnp.bfloat16
EPS = 1e-5
VMEM_LIMIT = 63 * 1024 * 1024
NT = (((1,), (1,)), ((), ()))
LANES = 128

V_BQ, V_BP, V_BG, V_AP, V_AG, V_GATE, V_NI0, V_NI1, V_NO0, V_NO1, V_BO, V_BIN = range(12)


def sigmoid(x):
    return 1.0 / (1.0 + jnp.exp(-x))


def norm_rows(x, scale, offset):
    inv = 1.0 / x.shape[0]
    xc = x - jnp.sum(x, axis=0, keepdims=True) * inv
    var = jnp.sum(xc * xc, axis=0, keepdims=True) * inv
    return (xc * lax.rsqrt(var + EPS) * scale + offset).astype(BF16)


def twice(x):
    return jnp.concatenate([x, x], axis=1)


def project_rows(l, first, count, m_ref, w_ref, norm_ref, bias_ref, a_ref, b_out, xa, xb, scr):
    width = w_ref.shape[1] // 2
    dim = w_ref.shape[2]
    rows = scr.shape[0] // width
    depth = xa.shape[1] // rows
    block = 16
    scale, offset = norm_ref[l, 0:1].astype(F32), norm_ref[l, 1:2].astype(F32)

    def chunk(t, _):
        at = pl.ds(pl.multiple_of((first + t) * rows, rows), rows)
        lanes = pl.ds(pl.multiple_of((first + t) * LANES, LANES), LANES)

        for part, x_ref in enumerate((xa, xb)):
            def normalize(s, _):
                x = m_ref[pl.ds(part * depth + s * block, block), at, :].astype(F32).reshape(block * rows, dim)
                xc = x - jnp.sum(x, axis=1, keepdims=True) * (1.0 / dim)
                var = jnp.sum(xc * xc, axis=1, keepdims=True) * (1.0 / dim)
                xn = xc * lax.rsqrt(var + EPS)
                to = pl.ds(pl.multiple_of(s * block * rows, block * rows), block * rows)
                for f in range(dim // LANES):
                    x_ref[f, to, :] = xn[:, f * LANES : (f + 1) * LANES]
                return 0

            lax.fori_loop(0, depth // block, normalize, 0)

        def residue(t2, _):
            for u in range(2):
                r = 2 * t2 + u
                xn = jnp.concatenate(
                    [jnp.concatenate([x_ref[f, pl.ds(r, depth, stride=rows), :] for x_ref in (xa, xb)], axis=0)
                     for f in range(dim // LANES)], axis=1)
                mn = (xn * scale + offset).astype(BF16)
                out = lax.dot_general(w_ref[l], mn, NT, preferred_element_type=F32) + bias_ref[l]
                a_ref[l, pl.ds(pl.multiple_of(r * width, width), width), lanes] = out[:width].astype(BF16)
                scr[pl.ds(r, width, stride=rows), :] = out[width:]
            return 0

        lax.fori_loop(0, rows // 2, residue, 0)
        b_out(l, lanes, scr[...].astype(BF16).reshape(width, rows, LANES))
        return 0

    lax.fori_loop(0, count, chunk, 0)


def prepare_wq(l, raw_ref, tmp_ref, wq_ref):
    cd = raw_ref.shape[0]
    width = math.isqrt(cd)
    tmp_ref[0, :, :] = raw_ref[...].astype(F32)
    for g in range(cd // LANES):
        per = LANES // width
        w = jnp.concatenate([tmp_ref[0, pl.ds(g * per + d, width, stride=width), :] for d in range(per)], axis=0)
        wq_ref[l, :, g * LANES : (g + 1) * LANES] = w.T.astype(BF16)


def opm_half(l, h, a_ref, b_ref, wq_ref, vec_ref, z_ref, q_ref):
    pairs, cd, lanes2 = q_ref.shape
    seqs = a_ref.shape[2]
    width = a_ref.shape[1] // (2 * pairs)
    half = lanes2 // 2
    scale = 1.0 / seqs

    def outer(t, _):
        rhs = b_ref[h, pl.ds(2 * t, 2)].reshape(2 * half, seqs)
        out = lax.dot_general(a_ref[l], rhs, NT, preferred_element_type=F32)
        out = (out * scale).astype(BF16)
        for d in range(2):
            blk = out[:, d * half : (d + 1) * half].reshape(2 * pairs, width, half)
            at = pl.ds(pl.multiple_of((2 * t + d) * width, width), width)
            for e in range(2):
                q_ref[:, at, e * half : (e + 1) * half] = blk[e * pairs : (e + 1) * pairs]
        return 0

    lax.fori_loop(0, cd // width // 2, outer, 0)
    bq = twice(vec_ref[l, V_BQ])

    def project(p, _):
        u = jnp.dot(wq_ref[l], q_ref[p], preferred_element_type=F32) + bq
        z_ref[h, p] = (z_ref[h, p].astype(F32) + u.astype(BF16).astype(F32)).astype(BF16)
        return 0

    lax.fori_loop(0, pairs, project, 0)


def gate_half(l, h, z_ref, mask_ref, wall_ref, vec_ref, fa_ref, fb_ref, g_ref, a_out, b_out):
    pairs = z_ref.shape[1]
    dim = z_ref.shape[2]
    half = z_ref.shape[3] // 2

    def project(p, _):
        zn = norm_rows(z_ref[h, p].astype(F32), twice(vec_ref[l, V_NI0]), twice(vec_ref[l, V_NI1]))
        mask = jnp.concatenate([mask_ref[h, pl.ds(p + e * pairs, 1), :] for e in range(2)], axis=1)
        at = pl.ds(pl.multiple_of(p * dim, dim), dim)

        def proj(q, v):
            w = wall_ref[l, q * dim : (q + 1) * dim]
            return jnp.dot(w, zn, preferred_element_type=F32) + twice(vec_ref[l, v])

        for q, f_ref, vp, vg in ((0, fb_ref, V_BP, V_BG), (2, fa_ref, V_AP, V_AG)):
            val = mask * sigmoid(proj(q + 1, vg)) * proj(q, vp)
            f_ref[0, at, :] = val[:, :half]
            f_ref[1, at, :] = val[:, half:]
        g_ref[h, p] = sigmoid(proj(4, V_GATE))
        return 0

    lax.fori_loop(0, pairs, project, 0)

    for f_ref, out in ((fb_ref, b_out), (fa_ref, a_out)):
        def relayout(t, _):
            for u in range(8):
                c = t * 8 + u
                lo = f_ref[0, pl.ds(c, pairs, stride=dim), :]
                hi = f_ref[1, pl.ds(c, pairs, stride=dim), :]
                out(c, h, jnp.concatenate([lo, hi], axis=0).astype(BF16))
            return 0

        lax.fori_loop(0, dim // 8, relayout, 0)


def triangle_half(jh, a_ref, b_ref, o_ref):
    dim = a_ref.shape[0]
    pairs = a_ref.shape[1] // 2

    def step(t, _):
        for u in range(8):
            c = t * 8 + u
            o = lax.dot_general(a_ref[c], b_ref[jh, c], NT, preferred_element_type=F32)
            o_ref[0, pl.ds(c, pairs, stride=dim), :] = o[:pairs]
            o_ref[1, pl.ds(c, pairs, stride=dim), :] = o[pairs:]
        return 0

    lax.fori_loop(0, dim // 8, step, 0)


def finish_half(l, jh, o_ref, g_ref, z_ref, wo_ref, vec_ref):
    pairs = z_ref.shape[1]
    dim = z_ref.shape[2]

    def step(p, _):
        at = pl.ds(pl.multiple_of(p * dim, dim), dim)
        o = jnp.concatenate([o_ref[0, at, :], o_ref[1, at, :]], axis=1)
        on = norm_rows(o, twice(vec_ref[l, V_NO0]), twice(vec_ref[l, V_NO1]))
        u = jnp.dot(wo_ref[l], on, preferred_element_type=F32) + twice(vec_ref[l, V_BO])
        z_ref[jh, p] = (z_ref[jh, p].astype(F32) + g_ref[jh, p] * u.astype(BF16).astype(F32)).astype(BF16)
        return 0

    lax.fori_loop(0, pairs, step, 0)


class Stream:
    def __init__(self, buf, color, lo, lanes, rows, sems, where):
        self.buf, self.color, self.rows, self.lanes = buf, color, rows, lanes
        self.base, self.size = lo
        self.part = buf.shape[0] // 2
        self.ring_send, self.ring_recv, self.core_send, self.core_recv = sems
        self.chip, self.core, self.chips = where
        self.sent = []

    def block(self, chip, part, piece=None):
        lo, n = part * self.part + self.base, self.size
        if piece is not None:
            n = n // 2
            lo = lo + piece * n
        rows = pl.ds(pl.multiple_of(chip * self.rows, self.rows), self.rows)
        return self.buf.at[pl.ds(lo, n), rows, self.lanes]

    def copy(self, ref, send, recv, chip, core):
        return pltpu.make_async_remote_copy(
            src_ref=ref, dst_ref=ref, send_sem=send, recv_sem=recv,
            device_id={"dap": chip * 2 + core}, device_id_type=pl.DeviceIdType.MESH)

    def near(self, step):
        return lax.rem(self.chip + step + self.chips, self.chips)

    def ring(self, side, hop, chip, piece=None):
        return self.copy(self.block(chip, self.core, piece), self.ring_send.at[side, hop], self.ring_recv.at[side, hop],
                         self.near(1 - 2 * side), self.core)

    def across(self, slot, chip, part, piece=None):
        return self.copy(self.block(chip, part, piece), self.core_send.at[slot], self.core_recv.at[slot],
                         self.chip, 1 - self.core)

    def event(self, hop):
        if hop == 0:
            @pl.when(self.core == self.color)
            def _():
                self.across(0, self.chip, 1 - self.core).start()
                for side in range(2):
                    self.ring(side, 0, self.chip).start()
                self.across(1, self.chip, self.core).start()

            @pl.when(self.core != self.color)
            def _():
                self.across(0, self.chip, self.core).wait_recv()
                for side in range(2):
                    self.ring(side, 0, self.chip).start()
            return
        last = self.chips // 2
        for side in range(2):
            origin = self.near((2 * side - 1) * hop)
            piece = side if hop == last else None
            self.ring(side, hop - 1, origin, piece).wait_recv()
            if hop < last:
                self.ring(side, hop, origin, side if hop == last - 1 else None).start()
            self.across(2 + 2 * (hop - 1) + side, origin, self.core, piece).start()

    def finish(self):
        last = self.chips // 2

        @pl.when(self.core != self.color)
        def _():
            self.across(1, self.chip, 1 - self.core).wait_recv()

        for hop in range(1, last + 1):
            for side in range(2):
                origin = self.near((2 * side - 1) * hop)
                piece = side if hop == last else None
                self.across(2 + 2 * (hop - 1) + side, origin, 1 - self.core, piece).wait_recv()

    def drain(self):
        last = self.chips // 2

        @pl.when(self.core == self.color)
        def _():
            self.across(0, self.chip, 1 - self.core).wait_send()
            self.across(1, self.chip, self.core).wait_send()

        for side in range(2):
            for hop in range(last):
                self.ring(side, hop, self.chip, side if hop == last - 1 else None).wait_send()
            for hop in range(1, last + 1):
                self.across(2 + 2 * (hop - 1) + side, self.chip, self.core, side if hop == last else None).wait_send()


N_STREAMS = 14
N_LOADS = 64


def layers_kernel(chips, m_hbm, z_hbm, wq_hbm, wab_hbm, wgate_hbm, wout_hbm, w_in_ref, b_in_ref, opm_norm_ref, mask_in,
                  bq_ref, norm_in_ref, b_ab_ref, b_gate_ref, norm_out_ref, b_o_ref, out_hbm,
                  b_buf, t_buf, a_ref, z_ref, at_ref, g_ref, q_scr, fa, fb, b_scr, wq_ref, wall_ref, wo_ref, vec_ref,
                  bias_ref, mask_ref, ring_send, ring_recv, core_send, core_recv, local_sem):
    me = lax.axis_index("dap")
    chip, core = me // 2, lax.rem(me, 2)
    rows, cols, dim = z_hbm.shape
    seqs = m_hbm.shape[0]
    layers = a_ref.shape[0]
    pairs = rows // 2
    half = cols // 2
    own = pl.ds(pl.multiple_of(chip * rows, rows), rows)

    barrier = pltpu.get_barrier_semaphore()
    right, left = lax.rem(chip + 1, chips), lax.rem(chip + chips - 1, chips)
    for there in (right * 2 + core, left * 2 + core, chip * 2 + 1 - core):
        pl.semaphore_signal(barrier, inc=1, device_id={"dap": there}, device_id_type=pl.DeviceIdType.MESH)

    used = [0]

    def load(src, dst):
        copy = pltpu.make_async_copy(src, dst, local_sem.at[used[0]])
        used[0] += 1
        copy.start()
        return copy

    m_ref = t_buf.at[layers - 1, 0]
    z_raw = t_buf.at[layers - 1, 1]
    chunks = seqs // LANES
    m_loads = [load(m_hbm.at[pl.ds(a * LANES, LANES)], m_ref.at[:, pl.ds(a * rows, rows), :]) for a in range(chunks)]
    z_loads = [load(z_hbm.at[:, pl.ds((2 * c + h) * rows, rows), :],
                    z_raw.at[pl.ds(0, rows), pl.ds(c * rows, rows), pl.ds(h * dim, dim)])
               for h in range(2) for c in range(chips)]
    w_loads = []
    for l in range(layers):
        cd, ab = wq_hbm.shape[1], wab_hbm.shape[1]
        lanes = pl.ds(0, dim)
        w_loads.append(load(wq_hbm.at[l], q_scr.at[l, :, lanes]))
        w_loads.append(load(wab_hbm.at[l], q_scr.at[2 + l, pl.ds(0, ab), lanes]))
        w_loads.append(load(wgate_hbm.at[l], q_scr.at[4 + l, pl.ds(0, dim), lanes]))
        w_loads.append(load(wout_hbm.at[l], q_scr.at[4 + l, pl.ds(dim, dim), lanes]))

    where = (chip, core, chips)
    count = [0]

    def stream(buf, color, lo, lanes):
        sems = tuple(s.at[count[0]] for s in (ring_send, ring_recv, core_send, core_recv))
        count[0] += 1
        return Stream(buf, color, lo, lanes, rows, sems, where)

    width = b_buf.shape[2]
    full_b = pl.ds(0, seqs)
    full_t = pl.ds(0, cols)
    b1 = [[stream(b_buf.at[0, q], q, (0, width // 2), pl.ds(s * (seqs // 2), seqs // 2)) for q in range(2)]
          for s in range(2)]
    b2 = [stream(b_buf.at[1, q], q, (0, width // 2), full_b) for q in range(2)]
    t1 = [[stream(t_buf.at[0, q], q, (s * dim // 4, dim // 4), full_t) for s in range(2)] for q in range(2)]
    t2 = [[stream(t_buf.at[1, q], q, (0, dim // 2), pl.ds(k * half, half)) for q in range(2)] for k in range(2)]

    def column(row):
        return jnp.broadcast_to(row, (LANES, row.shape[1])).T

    for l in range(layers):
        bias_ref[l] = column(b_in_ref[l])[: 2 * width]

    def project(l, first, n):
        def b_out(l, lanes, v):
            b_buf[l, core, :, own, lanes] = v

        project_rows(l, first, n, m_ref, w_in_ref, opm_norm_ref, bias_ref, a_ref, b_out, fa, fb, b_scr)

    def vectors():
        bq, b_gate, b_o = (r[...].astype(F32) for r in (bq_ref, b_gate_ref, b_o_ref))
        for l in range(layers):
            norm_in, b_ab, norm_out = (r[l].astype(F32) for r in (norm_in_ref, b_ab_ref, norm_out_ref))
            table = ((V_BQ, bq, l), (V_BP, b_ab, 2), (V_BG, b_ab, 3), (V_AP, b_ab, 0), (V_AG, b_ab, 1),
                     (V_GATE, b_gate, l), (V_NI0, norm_in, 0), (V_NI1, norm_in, 1), (V_NO0, norm_out, 0),
                     (V_NO1, norm_out, 1), (V_BO, b_o, l))
            for v, src, r in table:
                vec_ref[l, v] = column(src[r : r + 1])

    def masks():
        to = lax.broadcasted_iota(jnp.int32, (cols, cols), 1)
        frm = lax.broadcasted_iota(jnp.int32, (cols, cols), 0)
        q, rest = to // half, to % half
        perm = (frm == (rest // rows) * (2 * rows) + q * rows + rest % rows).astype(F32).astype(BF16)
        mask = jnp.dot(mask_in[...].astype(F32).astype(BF16), perm, preferred_element_type=F32)
        for h in range(2):
            mask_ref[h] = mask[:, h * half : (h + 1) * half]

    def weights(l):
        prepare_wq(l, q_scr.at[l, :, pl.ds(0, dim)], fa, wq_ref)
        ab = wab_hbm.shape[1]
        fa[0, 0:ab, :] = q_scr[2 + l, 0:ab, 0:dim].astype(F32)
        for slot, q in enumerate((2, 3, 0, 1)):
            wall_ref[l, slot * dim : (slot + 1) * dim, :] = fa[0, pl.ds(q, dim, stride=4), :].T.astype(BF16)
        wall_ref[l, 4 * dim : 5 * dim, :] = q_scr[4 + l, 0:dim, 0:dim].astype(F32).T.astype(BF16)
        wo_ref[l] = q_scr[4 + l, dim : 2 * dim, 0:dim].astype(F32).T.astype(BF16)

    def pair_in():
        def step(p, _):
            for h in range(2):
                for e in range(2):
                    x = z_raw[e * pairs + p, :, h * dim : (h + 1) * dim].astype(F32)
                    z_ref[h, p, :, e * half : (e + 1) * half] = x.T.astype(BF16)
            return 0

        lax.fori_loop(0, pairs, step, 0)

    def opm(l, h):
        opm_half(l, h, a_ref, b_buf.at[l], wq_ref, vec_ref, z_ref, q_scr)

    def gate(l, h):
        def a_out(c, h, v):
            at_ref[l, c, :, h * LANES : (h + 1) * LANES] = v

        def b_out(c, h, v):
            t_buf[l, core, c, own, h * LANES : (h + 1) * LANES] = v

        gate_half(l, h, z_ref, mask_ref, wall_ref, vec_ref, fa, fb, g_ref, a_out, b_out)

    def triangle(l, jh):
        triangle_half(jh, at_ref.at[l], t_buf.at[l], fa)

    def finish(l, jh):
        finish_half(l, jh, fa, g_ref, z_ref, wo_ref, vec_ref)

    def pair_out(h):
        def step(p, _):
            for e in range(2):
                x = z_ref[h, p, :, e * half : (e + 1) * half].astype(F32)
                q_scr[p, h * half : (h + 1) * half, e * dim : (e + 1) * dim] = x.T.astype(BF16)
            return 0

        lax.fori_loop(0, pairs, step, 0)
        return [load(q_scr.at[:, pl.ds(h * half + c * rows, rows), pl.ds(e * dim, dim)],
                     out_hbm.at[pl.ds(e * pairs, pairs), pl.ds((2 * c + h) * rows, rows), :])
                for e in range(2) for c in range(chips)]

    def events(hop, *streams):
        for s in streams:
            s.event(hop)

    def wait(copies):
        for copy in copies:
            copy.wait()

    wait(m_loads[: chunks // 2])
    project(0, 0, chunks // 2)
    pl.semaphore_wait(barrier, 3)
    events(0, *b1[0])
    wait(m_loads[chunks // 2 :])
    project(0, chunks // 2, chunks // 2)
    vectors()
    events(0, *b1[1])
    events(1, *b1[0])
    events(1, *b1[1])
    wait(w_loads)
    weights(0)
    events(2, *b1[0])
    masks()
    wait(z_loads)
    pair_in()
    events(2, *b1[1])
    project(1, 0, chunks // 2)
    events(3, *b1[0])
    project(1, chunks // 2, chunks // 2)
    events(3, *b1[1])
    weights(1)
    events(0, *b2)
    events(4, *b1[0])
    events(4, *b1[1])
    for s in range(2):
        b1[s][0].finish()
    opm(0, 0)
    events(1, b2[0])
    for s in range(2):
        b1[s][1].finish()
    opm(0, 1)
    events(1, b2[1])
    gate(0, 0)
    events(2, b2[0])
    gate(0, 1)
    events(2, b2[1])
    events(0, *t1[0])
    events(3, *b2)
    events(1, *t1[0])
    events(4, *b2)
    events(2, *t1[0])
    events(0, *t1[1])
    events(3, *t1[0])
    events(4, *t1[0])
    for s in t1[0]:
        s.finish()
    triangle(0, 0)
    events(1, *t1[1])
    finish(0, 0)
    events(2, t1[1][0])
    for s in b2:
        s.finish()
    opm(1, 0)
    events(2, t1[1][1])
    events(3, *t1[1])
    gate(1, 0)
    events(0, *t2[0])
    events(4, *t1[1])
    for s in t1[1]:
        s.finish()
    triangle(0, 1)
    finish(0, 1)
    events(1, *t2[0])
    opm(1, 1)
    events(2, *t2[0])
    gate(1, 1)
    events(0, *t2[1])
    events(3, *t2[0])
    events(1, *t2[1])
    events(4, *t2[0])
    events(2, *t2[1])
    events(3, *t2[1])
    events(4, *t2[1])
    stores = []
    for q in range(2):
        t2[0][q].finish()
        t2[1][q].finish()
        triangle(1, q)
        finish(1, q)
        stores += pair_out(q)
    for s in b1[0] + b1[1] + b2 + t1[0] + t1[1] + t2[0] + t2[1]:
        s.drain()
    wait(stores)


def solution(mesh):
    size = mesh.shape["dap"]
    chips = size // 2
    hops = chips // 2
    pair_spec = P(("batch", "dap"), None, None)
    mask_spec = P(("batch", "dap"), None)
    msa_spec = P(None, ("batch", "dap"), None)
    any_spec = pl.BlockSpec(memory_space=pl.ANY)
    vmem_spec = pl.BlockSpec(memory_space=pltpu.VMEM)

    def device_fn(pair_act, pair_mask, msa_act, opm_norm, opm_w_in, opm_b_in, opm_w_out, opm_b_out, tri_norm_in,
                  tri_w_ab, tri_b_ab, tri_w_gate, tri_b_gate, tri_norm_out, tri_w_out, tri_b_out):
        rows, cols, dim = pair_act.shape
        seqs, _, mdim = msa_act.shape
        layers = opm_norm.shape[0]
        width = opm_w_in.shape[-1]
        pairs = rows // 2
        half = cols // 2
        z_shape = (2, pairs, dim, 2 * half)

        w_in = jnp.transpose(opm_w_in, (0, 2, 3, 1)).reshape(layers, 2 * width, mdim)
        b_in = jnp.pad(opm_b_in.reshape(layers, 1, 2 * width), ((0, 0), (0, 0), (0, dim - 2 * width))).astype(F32)
        w_ab = tri_w_ab.reshape(layers, dim * 4, dim)

        return pl.pallas_call(
            functools.partial(layers_kernel, chips),
            out_shape=jax.ShapeDtypeStruct(pair_act.shape, BF16),
            in_specs=[any_spec] * 6 + [vmem_spec] * 10,
            out_specs=any_spec,
            scratch_shapes=[pltpu.VMEM((layers, 2, width, half, seqs), BF16),
                            pltpu.VMEM((layers, 2, dim, half, cols), BF16),
                            pltpu.VMEM((layers, rows * width, seqs), BF16),
                            pltpu.VMEM(z_shape, BF16),
                            pltpu.VMEM((layers, dim, rows, cols), BF16),
                            pltpu.VMEM(z_shape, F32),
                            pltpu.VMEM((pairs, width * width, 2 * half), BF16),
                            pltpu.VMEM((2, pairs * dim, LANES), F32),
                            pltpu.VMEM((2, pairs * dim, LANES), F32),
                            pltpu.VMEM((width * rows, LANES), F32),
                            pltpu.VMEM((layers, dim, width * width), BF16),
                            pltpu.VMEM((layers, 5 * dim, dim), BF16),
                            pltpu.VMEM((layers, dim, dim), BF16),
                            pltpu.VMEM((layers, V_BIN, dim, LANES), F32),
                            pltpu.VMEM((layers, 2 * width, LANES), F32),
                            pltpu.VMEM((2, rows, half), F32),
                            pltpu.SemaphoreType.DMA((N_STREAMS, 2, hops)),
                            pltpu.SemaphoreType.DMA((N_STREAMS, 2, hops)),
                            pltpu.SemaphoreType.DMA((N_STREAMS, 2 + 2 * hops)),
                            pltpu.SemaphoreType.DMA((N_STREAMS, 2 + 2 * hops)),
                            pltpu.SemaphoreType.DMA((N_LOADS,))],
            compiler_params=pltpu.CompilerParams(vmem_limit_bytes=VMEM_LIMIT, collective_id=0, has_side_effects=True),
            name="layers",
        )(msa_act, pair_act, opm_w_out, w_ab, tri_w_gate, tri_w_out, w_in, b_in, opm_norm, pair_mask,
          opm_b_out, tri_norm_in, tri_b_ab, tri_b_gate, tri_norm_out, tri_b_out)

    return jax.shard_map(device_fn, mesh=mesh, in_specs=(pair_spec, mask_spec, msa_spec) + (P(),) * 13,
                         out_specs=pair_spec, check_vma=False)
```

```python
import functools
import math

import jax
import jax.numpy as jnp
from jax import lax
from jax.experimental import pallas as pl
from jax.experimental.pallas import tpu as pltpu
from jax.sharding import PartitionSpec as P

F32 = jnp.float32
BF16 = jnp.bfloat16
EPS = 1e-5
VMEM_LIMIT = 63 * 1024 * 1024
NT = (((1,), (1,)), ((), ()))
LANES = 128

V_BQ, V_BP, V_BG, V_AP, V_AG, V_GATE, V_NI0, V_NI1, V_NO0, V_NO1, V_BO, V_BIN = range(12)


def sigmoid(x):
    return 1.0 / (1.0 + jnp.exp(-x))


def norm_rows(x, scale, offset):
    inv = 1.0 / x.shape[0]
    xc = x - jnp.sum(x, axis=0, keepdims=True) * inv
    var = jnp.sum(xc * xc, axis=0, keepdims=True) * inv
    return (xc * lax.rsqrt(var + EPS) * scale + offset).astype(BF16)


def twice(x):
    return jnp.concatenate([x, x], axis=1)


def project_rows(l, chunk, m_ref, w_ref, norm_ref, bias_ref, a_ref, b_out, xa, xb, scr):
    width = w_ref.shape[1] // 2
    dim = w_ref.shape[2]
    rows = scr.shape[0] // width
    depth = xa.shape[1] // rows
    block = 16
    scale, offset = norm_ref[l, 0:1].astype(F32), norm_ref[l, 1:2].astype(F32)

    at = pl.ds(chunk * rows, rows)
    lanes = pl.ds(chunk * LANES, LANES)

    for part, x_ref in enumerate((xa, xb)):
        def normalize(s, _):
            x = m_ref[pl.ds(part * depth + s * block, block), at, :].astype(F32).reshape(block * rows, dim)
            xc = x - jnp.sum(x, axis=1, keepdims=True) * (1.0 / dim)
            var = jnp.sum(xc * xc, axis=1, keepdims=True) * (1.0 / dim)
            xn = xc * lax.rsqrt(var + EPS)
            to = pl.ds(pl.multiple_of(s * block * rows, block * rows), block * rows)
            for f in range(dim // LANES):
                x_ref[f, to, :] = xn[:, f * LANES : (f + 1) * LANES]
            return 0

        lax.fori_loop(0, depth // block, normalize, 0)

    def residue(t2, _):
        for u in range(2):
            r = 2 * t2 + u
            xn = jnp.concatenate(
                [jnp.concatenate([x_ref[f, pl.ds(r, depth, stride=rows), :] for x_ref in (xa, xb)], axis=0)
                 for f in range(dim // LANES)], axis=1)
            mn = (xn * scale + offset).astype(BF16)
            out = lax.dot_general(w_ref[l], mn, NT, preferred_element_type=F32) + bias_ref[l]
            a_ref[l, pl.ds(pl.multiple_of(r * width, width), width), lanes] = out[:width].astype(BF16)
            scr[pl.ds(r, width, stride=rows), :] = out[width:]
        return 0

    lax.fori_loop(0, rows // 2, residue, 0)
    b_out(l, lanes, scr[...].astype(BF16).reshape(width, rows, LANES))


def prepare_wq(l, raw_ref, tmp_ref, wq_ref):
    cd = raw_ref.shape[0]
    width = math.isqrt(cd)
    tmp_ref[0, :, :] = raw_ref[...].astype(F32)
    for g in range(cd // LANES):
        per = LANES // width
        w = jnp.concatenate([tmp_ref[0, pl.ds(g * per + d, width, stride=width), :] for d in range(per)], axis=0)
        wq_ref[l, :, g * LANES : (g + 1) * LANES] = w.T.astype(BF16)


def outer_half(l, h, part, parts, a_ref, b_ref, q_ref):
    pairs, cd, lanes2 = q_ref.shape
    seqs = a_ref.shape[2]
    width = a_ref.shape[1] // (2 * pairs)
    half = lanes2 // 2
    scale = 1.0 / seqs

    def outer(t, _):
        rhs = b_ref[h, pl.ds(2 * t, 2)].reshape(2 * half, seqs)
        out = lax.dot_general(a_ref[l], rhs, NT, preferred_element_type=F32)
        out = (out * scale).astype(BF16)
        for d in range(2):
            blk = out[:, d * half : (d + 1) * half].reshape(2 * pairs, width, half)
            at = pl.ds(pl.multiple_of((2 * t + d) * width, width), width)
            for e in range(2):
                q_ref[:, at, e * half : (e + 1) * half] = blk[e * pairs : (e + 1) * pairs]
        return 0

    steps = cd // width // 2 // parts
    lax.fori_loop(part * steps, (part + 1) * steps, outer, 0)


def opm_half(l, h, wq_ref, vec_ref, z_ref, q_ref):
    pairs = q_ref.shape[0]
    bq = twice(vec_ref[l, V_BQ])

    def project(p, _):
        u = jnp.dot(wq_ref[l], q_ref[p], preferred_element_type=F32) + bq
        z_ref[h, p] = (z_ref[h, p].astype(F32) + u.astype(BF16).astype(F32)).astype(BF16)
        return 0

    lax.fori_loop(0, pairs, project, 0)


def gate_half(l, h, z_ref, mask_ref, wall_ref, vec_ref, fa_ref, fb_ref, g_ref, a_out, b_out):
    pairs = z_ref.shape[1]
    dim = z_ref.shape[2]
    half = z_ref.shape[3] // 2

    def project(p, _):
        zn = norm_rows(z_ref[h, p].astype(F32), twice(vec_ref[l, V_NI0]), twice(vec_ref[l, V_NI1]))
        mask = jnp.concatenate([mask_ref[h, pl.ds(p + e * pairs, 1), :] for e in range(2)], axis=1)
        at = pl.ds(pl.multiple_of(p * dim, dim), dim)

        def proj(q, v):
            w = wall_ref[l, q * dim : (q + 1) * dim]
            return jnp.dot(w, zn, preferred_element_type=F32) + twice(vec_ref[l, v])

        for q, f_ref, vp, vg in ((0, fb_ref, V_BP, V_BG), (2, fa_ref, V_AP, V_AG)):
            val = mask * sigmoid(proj(q + 1, vg)) * proj(q, vp)
            f_ref[0, at, :] = val[:, :half]
            f_ref[1, at, :] = val[:, half:]
        g_ref[h, p] = sigmoid(proj(4, V_GATE))
        return 0

    lax.fori_loop(0, pairs, project, 0)

    for f_ref, out in ((fb_ref, b_out), (fa_ref, a_out)):
        def relayout(t, _):
            for u in range(8):
                c = t * 8 + u
                lo = f_ref[0, pl.ds(c, pairs, stride=dim), :]
                hi = f_ref[1, pl.ds(c, pairs, stride=dim), :]
                out(c, h, jnp.concatenate([lo, hi], axis=0).astype(BF16))
            return 0

        lax.fori_loop(0, dim // 8, relayout, 0)


def triangle_half(jh, k, a_ref, b_ref, o_ref):
    dim = a_ref.shape[0]
    pairs = a_ref.shape[1] // 2

    def step(t, _):
        for u in range(8):
            c = t * 8 + u
            o = lax.dot_general(a_ref[c, :, k], b_ref[jh, c, :, k], NT, preferred_element_type=F32)
            o_ref[0, pl.ds(c, pairs, stride=dim), :] = o[:pairs]
            o_ref[1, pl.ds(c, pairs, stride=dim), :] = o[pairs:]
        return 0

    lax.fori_loop(0, dim // 8, step, 0)


def finish_half(l, jh, o_refs, g_ref, z_ref, wo_ref, vec_ref):
    pairs = z_ref.shape[1]
    dim = z_ref.shape[2]

    def step(p, _):
        at = pl.ds(pl.multiple_of(p * dim, dim), dim)
        o = sum(jnp.concatenate([o_ref[0, at, :], o_ref[1, at, :]], axis=1) for o_ref in o_refs)
        on = norm_rows(o, twice(vec_ref[l, V_NO0]), twice(vec_ref[l, V_NO1]))
        u = jnp.dot(wo_ref[l], on, preferred_element_type=F32) + twice(vec_ref[l, V_BO])
        z_ref[jh, p] = (z_ref[jh, p].astype(F32) + g_ref[jh, p] * u.astype(BF16).astype(F32)).astype(BF16)
        return 0

    lax.fori_loop(0, pairs, step, 0)


class Stream:
    def __init__(self, buf, color, lo, lanes, rows, sems, where):
        self.buf, self.color, self.rows, self.lanes = buf, color, rows, lanes
        self.base, self.size = lo
        self.part = buf.shape[0] // 2
        self.ring_send, self.ring_recv, self.core_send, self.core_recv = sems
        self.chip, self.core, self.chips = where
        self.sent = []

    def block(self, chip, part, piece=None):
        lo, n = part * self.part + self.base, self.size
        if piece is not None:
            n = n // 2
            lo = lo + piece * n
        rows = pl.ds(pl.multiple_of(chip * self.rows, self.rows), self.rows)
        return self.buf.at[pl.ds(lo, n), rows, self.lanes]

    def copy(self, ref, send, recv, chip, core):
        return pltpu.make_async_remote_copy(
            src_ref=ref, dst_ref=ref, send_sem=send, recv_sem=recv,
            device_id={"dap": chip * 2 + core}, device_id_type=pl.DeviceIdType.MESH)

    def near(self, step):
        return lax.rem(self.chip + step + self.chips, self.chips)

    def ring(self, side, hop, chip, piece=None):
        return self.copy(self.block(chip, self.core, piece), self.ring_send.at[side, hop], self.ring_recv.at[side, hop],
                         self.near(1 - 2 * side), self.core)

    def across(self, slot, chip, part, piece=None):
        return self.copy(self.block(chip, part, piece), self.core_send.at[slot], self.core_recv.at[slot],
                         self.chip, 1 - self.core)

    def event(self, hop):
        if hop == -1:
            @pl.when(self.core == self.color)
            def _():
                self.across(0, self.chip, 1 - self.core).start()
                for side in range(2):
                    self.ring(side, 0, self.chip).start()
                self.across(1, self.chip, self.core).start()
            return
        if hop == 0:
            @pl.when(self.core != self.color)
            def _():
                self.across(0, self.chip, self.core).wait_recv()
                for side in range(2):
                    self.ring(side, 0, self.chip).start()
            return
        last = self.chips // 2
        for side in range(2):
            origin = self.near((2 * side - 1) * hop)
            piece = side if hop == last else None
            self.ring(side, hop - 1, origin, piece).wait_recv()
            if hop < last:
                self.ring(side, hop, origin, side if hop == last - 1 else None).start()
            self.across(2 + 2 * (hop - 1) + side, origin, self.core, piece).start()

    def finish(self):
        last = self.chips // 2

        @pl.when(self.core != self.color)
        def _():
            self.across(1, self.chip, 1 - self.core).wait_recv()

        for hop in range(1, last + 1):
            for side in range(2):
                origin = self.near((2 * side - 1) * hop)
                piece = side if hop == last else None
                self.across(2 + 2 * (hop - 1) + side, origin, 1 - self.core, piece).wait_recv()

    def drain(self):
        last = self.chips // 2

        @pl.when(self.core == self.color)
        def _():
            self.across(0, self.chip, 1 - self.core).wait_send()
            self.across(1, self.chip, self.core).wait_send()

        for side in range(2):
            for hop in range(last):
                self.ring(side, hop, self.chip, side if hop == last - 1 else None).wait_send()
            for hop in range(1, last + 1):
                self.across(2 + 2 * (hop - 1) + side, self.chip, self.core, side if hop == last else None).wait_send()


ORDER = (
    "p0", ("b100", -1), ("b101", -1), "p1", ("b100", 0), ("b101", 0), ("b110", -1), ("b111", -1), "p2", ("b110", 0),
    ("b111", 0), "p3", ("b120", -1), ("b121", -1), ("b100", 1), ("b101", 1), "vec", ("b120", 0), ("b121", 0), "w0",
    ("b110", 1), ("b111", 1), "mask", "pin", "q0", ("b100", 2), "q1", ("b101", 2), "q2", ("b120", 1), ("b121", 1),
    "q3", ("b110", 2), ("b111", 2), "w1", ("b100", 3), ("b101", 3), ("b120", 2), ("b121", 2), ("b110", 3),
    ("b111", 3), ("b100", 4), ("b101", 4), ("b20", -1), ("b20", 0), ("b120", 3), ("b121", 3), ("b110", 4),
    ("b111", 4), ("b21", -1), ("b21", 0), ("b20", 1), ("b120", 4), ("b121", 4), "O00a", "O00b", ("b21", 1), "O00p",
    "G00", ("b20", 2), "O01a", "O01b", ("b21", 2), "O01p", "G01", ("t100", -1), ("b20", 3), ("t101", -1),
    ("t100", 0), ("b21", 3), ("t101", 0), ("t100", 1), ("b20", 4), ("b21", 4), ("t101", 1), ("t100", 2),
    ("t101", 2), ("t100", 3), ("t110", -1), ("t110", 0), ("t101", 3), ("t100", 4), ("t111", -1), ("t111", 0),
    ("t110", 1), ("t101", 4), "T00", ("t111", 1), "N00", "O10a", "O10b", ("t110", 2), "O10p", "G10", ("t111", 2),
    ("t200", -1), ("t201", -1), ("t200", 0), ("t201", 0), ("t110", 3), ("t111", 3), ("t200", 1), ("t201", 1),
    ("t110", 4), ("t111", 4), "T01", ("t200", 2), "N01", "O11a", "O11b", ("t201", 2), "O11p", "G11", ("t210", -1),
    ("t200", 3), ("t210", 0), ("t201", 3), ("t211", -1), ("t211", 0), ("t210", 1), ("t200", 4), ("t201", 4), "K1",
    ("t211", 1), ("t210", 2), ("t211", 2), ("t210", 3), ("t211", 3), ("t210", 4), "T10", ("t211", 4), "N10", "X10",
    "L1", "N11", "X11",
)
NEEDS = {
    "O00a": ("b100", "b110", "b120",),
    "O01a": ("b101", "b111", "b121",),
    "T00": ("t100", "t101",),
    "O10a": ("b20",),
    "T01": ("t110", "t111",),
    "O11a": ("b21",),
    "K1": ("t201",),
    "T10": ("t200", "t210",),
    "L1": ("t211",),
}
N_STREAMS = 16
N_LOADS = 32


def layers_kernel(chips, m_hbm, z_hbm, wq_hbm, wab_hbm, wgate_hbm, wout_hbm, w_in_ref, b_in_ref, opm_norm_ref, mask_in,
                  bq_ref, norm_in_ref, b_ab_ref, b_gate_ref, norm_out_ref, b_o_ref, out_hbm,
                  b_buf, t_buf, a_ref, z_ref, at_ref, g_ref, q_scr, fa, fb, b_scr, wq_ref, wall_ref, wo_ref, vec_ref,
                  bias_ref, mask_ref, ring_send, ring_recv, core_send, core_recv, local_sem):
    me = lax.axis_index("dap")
    chip, core = me // 2, lax.rem(me, 2)
    rows, cols, dim = z_hbm.shape
    seqs = m_hbm.shape[0]
    layers = a_ref.shape[0]
    pairs = rows // 2
    half = cols // 2
    own = pl.ds(pl.multiple_of(chip * rows, rows), rows)

    barrier = pltpu.get_barrier_semaphore()
    right, left = lax.rem(chip + 1, chips), lax.rem(chip + chips - 1, chips)
    for there in (right * 2 + core, left * 2 + core, chip * 2 + 1 - core):
        pl.semaphore_signal(barrier, inc=1, device_id={"dap": there}, device_id_type=pl.DeviceIdType.MESH)

    used = [0]

    def load(src, dst):
        copy = pltpu.make_async_copy(src, dst, local_sem.at[used[0] % N_LOADS])
        used[0] += 1
        copy.start()
        return copy

    m_ref = t_buf.at[layers - 1, 0]
    z_raw = t_buf.at[layers - 1, 1]
    chunks = seqs // LANES
    m_loads = [load(m_hbm.at[pl.ds(a * LANES, LANES)], m_ref.at[:, pl.ds(a * rows, rows), :]) for a in range(chunks)]
    z_loads = [load(z_hbm.at[:, pl.ds((2 * c + h) * rows, rows), :],
                    z_raw.at[pl.ds(0, rows), pl.ds(c * rows, rows), pl.ds(h * dim, dim)])
               for h in range(2) for c in range(chips)]
    w_loads = []
    for l in range(layers):
        cd, ab = wq_hbm.shape[1], wab_hbm.shape[1]
        lanes = pl.ds(0, dim)
        w_loads.append(load(wq_hbm.at[l], q_scr.at[l, :, lanes]))
        w_loads.append(load(wab_hbm.at[l], q_scr.at[2 + l, pl.ds(0, ab), lanes]))
        w_loads.append(load(wgate_hbm.at[l], q_scr.at[4 + l, pl.ds(0, dim), lanes]))
        w_loads.append(load(wout_hbm.at[l], q_scr.at[4 + l, pl.ds(dim, dim), lanes]))

    where = (chip, core, chips)
    count = [0]

    def stream(buf, color, lo, lanes):
        sems = tuple(s.at[count[0]] for s in (ring_send, ring_recv, core_send, core_recv))
        count[0] += 1
        return Stream(buf, color, lo, lanes, rows, sems, where)

    width = b_buf.shape[2]
    full_b = pl.ds(0, seqs)
    full_t = pl.ds(0, cols)
    named = {}
    for s, (lo, n) in enumerate(((0, 1), (1, 1), (2, chunks - 2))):
        for q in range(2):
            named[f"b1{s}{q}"] = stream(b_buf.at[0, q], q, (0, width // 2), pl.ds(lo * LANES, n * LANES))
    for q in range(2):
        named[f"b2{q}"] = stream(b_buf.at[1, q], q, (0, width // 2), full_b)
        for s in range(2):
            named[f"t1{q}{s}"] = stream(t_buf.at[0, q], q, (s * dim // 4, dim // 4), full_t)
            named[f"t2{s}{q}"] = stream(t_buf.at[1, q], q, (0, dim // 2), pl.ds(s * half, half))

    def column(row):
        return jnp.broadcast_to(row, (LANES, row.shape[1])).T

    for l in range(layers):
        bias_ref[l] = column(b_in_ref[l])[: 2 * width]

    def project(l, chunk):
        def b_out(l, lanes, v):
            b_buf[l, core, :, own, lanes] = v

        project_rows(l, chunk, m_ref, w_in_ref, opm_norm_ref, bias_ref, a_ref, b_out, fa, fb, b_scr)

    def vectors():
        bq, b_gate, b_o = (r[...].astype(F32) for r in (bq_ref, b_gate_ref, b_o_ref))
        for l in range(layers):
            norm_in, b_ab, norm_out = (r[l].astype(F32) for r in (norm_in_ref, b_ab_ref, norm_out_ref))
            table = ((V_BQ, bq, l), (V_BP, b_ab, 2), (V_BG, b_ab, 3), (V_AP, b_ab, 0), (V_AG, b_ab, 1),
                     (V_GATE, b_gate, l), (V_NI0, norm_in, 0), (V_NI1, norm_in, 1), (V_NO0, norm_out, 0),
                     (V_NO1, norm_out, 1), (V_BO, b_o, l))
            for v, src, r in table:
                vec_ref[l, v] = column(src[r : r + 1])

    def masks():
        to = lax.broadcasted_iota(jnp.int32, (cols, cols), 1)
        frm = lax.broadcasted_iota(jnp.int32, (cols, cols), 0)
        q, rest = to // half, to % half
        perm = (frm == (rest // rows) * (2 * rows) + q * rows + rest % rows).astype(F32).astype(BF16)
        mask = jnp.dot(mask_in[...].astype(F32).astype(BF16), perm, preferred_element_type=F32)
        for h in range(2):
            mask_ref[h] = mask[:, h * half : (h + 1) * half]

    def weights(l):
        prepare_wq(l, q_scr.at[l, :, pl.ds(0, dim)], fa, wq_ref)
        ab = wab_hbm.shape[1]
        fa[0, 0:ab, :] = q_scr[2 + l, 0:ab, 0:dim].astype(F32)
        for slot, q in enumerate((2, 3, 0, 1)):
            wall_ref[l, slot * dim : (slot + 1) * dim, :] = fa[0, pl.ds(q, dim, stride=4), :].T.astype(BF16)
        wall_ref[l, 4 * dim : 5 * dim, :] = q_scr[4 + l, 0:dim, 0:dim].astype(F32).T.astype(BF16)
        wo_ref[l] = q_scr[4 + l, dim : 2 * dim, 0:dim].astype(F32).T.astype(BF16)

    def pair_in():
        def step(p, _):
            for h in range(2):
                for e in range(2):
                    x = z_raw[e * pairs + p, :, h * dim : (h + 1) * dim].astype(F32)
                    z_ref[h, p, :, e * half : (e + 1) * half] = x.T.astype(BF16)
            return 0

        lax.fori_loop(0, pairs, step, 0)

    def outer(l, h, part):
        outer_half(l, h, part, 2, a_ref, b_buf.at[l], q_scr)

    def opm(l, h):
        opm_half(l, h, wq_ref, vec_ref, z_ref, q_scr)

    def gate(l, h):
        def a_out(c, h, v):
            at_ref[l, c, :, h * LANES : (h + 1) * LANES] = v

        def b_out(c, h, v):
            t_buf[l, core, c, own, h * LANES : (h + 1) * LANES] = v

        gate_half(l, h, z_ref, mask_ref, wall_ref, vec_ref, fa, fb, g_ref, a_out, b_out)

    def triangle(l, jh, k=full_t, o_ref=fa):
        triangle_half(jh, k, at_ref.at[l], t_buf.at[l], o_ref)

    def finish(l, jh, *o_refs):
        finish_half(l, jh, o_refs or (fa,), g_ref, z_ref, wo_ref, vec_ref)

    def pair_out(h):
        def step(p, _):
            for e in range(2):
                x = z_ref[h, p, :, e * half : (e + 1) * half].astype(F32)
                q_scr[p, h * half : (h + 1) * half, e * dim : (e + 1) * dim] = x.T.astype(BF16)
            return 0

        lax.fori_loop(0, pairs, step, 0)
        return [load(q_scr.at[:, pl.ds(h * half + c * rows, rows), pl.ds(e * dim, dim)],
                     out_hbm.at[pl.ds(e * pairs, pairs), pl.ds((2 * c + h) * rows, rows), :])
                for e in range(2) for c in range(chips)]

    stores = []

    def first_project(chunk):
        m_loads[chunk].wait()
        project(0, chunk)
        if chunk == 0:
            pl.semaphore_wait(barrier, 3)

    def first_weights():
        for copy in w_loads:
            copy.wait()
        weights(0)

    def first_pairs():
        for copy in z_loads:
            copy.wait()
        pair_in()

    tasks = {"vec": vectors, "mask": masks, "w0": first_weights, "w1": lambda: weights(1), "pin": first_pairs,
             "K1": lambda: triangle(1, 1, pl.ds(0, half), fb), "L1": lambda: triangle(1, 1, pl.ds(half, half), fa),
             "N11": lambda: finish(1, 1, fa, fb)}
    for c in range(chunks):
        tasks[f"p{c}"] = functools.partial(first_project, c)
        tasks[f"q{c}"] = functools.partial(project, 1, c)
    for l in range(layers):
        for h in range(2):
            for part, letter in enumerate("ab"):
                tasks[f"O{l}{h}{letter}"] = functools.partial(outer, l, h, part)
            tasks[f"O{l}{h}p"] = functools.partial(opm, l, h)
            tasks[f"G{l}{h}"] = functools.partial(gate, l, h)
            tasks[f"T{l}{h}"] = functools.partial(triangle, l, h)
            tasks.setdefault(f"N{l}{h}", functools.partial(finish, l, h))
    for h in range(2):
        tasks[f"X1{h}"] = lambda h=h: stores.extend(pair_out(h))

    for item in ORDER:
        if item in tasks:
            for name in NEEDS.get(item, ()):
                named[name].finish()
            tasks[item]()
        else:
            name, hop = item
            named[name].event(hop)
    for s in named.values():
        s.drain()
    for copy in stores:
        copy.wait()


def solution(mesh):
    size = mesh.shape["dap"]
    chips = size // 2
    hops = chips // 2
    pair_spec = P(("batch", "dap"), None, None)
    mask_spec = P(("batch", "dap"), None)
    msa_spec = P(None, ("batch", "dap"), None)
    any_spec = pl.BlockSpec(memory_space=pl.ANY)
    vmem_spec = pl.BlockSpec(memory_space=pltpu.VMEM)

    def device_fn(pair_act, pair_mask, msa_act, opm_norm, opm_w_in, opm_b_in, opm_w_out, opm_b_out, tri_norm_in,
                  tri_w_ab, tri_b_ab, tri_w_gate, tri_b_gate, tri_norm_out, tri_w_out, tri_b_out):
        rows, cols, dim = pair_act.shape
        seqs, _, mdim = msa_act.shape
        layers = opm_norm.shape[0]
        width = opm_w_in.shape[-1]
        pairs = rows // 2
        half = cols // 2
        z_shape = (2, pairs, dim, 2 * half)

        w_in = jnp.transpose(opm_w_in, (0, 2, 3, 1)).reshape(layers, 2 * width, mdim)
        b_in = jnp.pad(opm_b_in.reshape(layers, 1, 2 * width), ((0, 0), (0, 0), (0, dim - 2 * width))).astype(F32)
        w_ab = tri_w_ab.reshape(layers, dim * 4, dim)

        return pl.pallas_call(
            functools.partial(layers_kernel, chips),
            out_shape=jax.ShapeDtypeStruct(pair_act.shape, BF16),
            in_specs=[any_spec] * 6 + [vmem_spec] * 10,
            out_specs=any_spec,
            scratch_shapes=[pltpu.VMEM((layers, 2, width, half, seqs), BF16),
                            pltpu.VMEM((layers, 2, dim, half, cols), BF16),
                            pltpu.VMEM((layers, rows * width, seqs), BF16),
                            pltpu.VMEM(z_shape, BF16),
                            pltpu.VMEM((layers, dim, rows, cols), BF16),
                            pltpu.VMEM(z_shape, F32),
                            pltpu.VMEM((pairs, width * width, 2 * half), BF16),
                            pltpu.VMEM((2, pairs * dim, LANES), F32),
                            pltpu.VMEM((2, pairs * dim, LANES), F32),
                            pltpu.VMEM((width * rows, LANES), F32),
                            pltpu.VMEM((layers, dim, width * width), BF16),
                            pltpu.VMEM((layers, 5 * dim, dim), BF16),
                            pltpu.VMEM((layers, dim, dim), BF16),
                            pltpu.VMEM((layers, V_BIN, dim, LANES), F32),
                            pltpu.VMEM((layers, 2 * width, LANES), F32),
                            pltpu.VMEM((2, rows, half), F32),
                            pltpu.SemaphoreType.DMA((N_STREAMS, 2, hops)),
                            pltpu.SemaphoreType.DMA((N_STREAMS, 2, hops)),
                            pltpu.SemaphoreType.DMA((N_STREAMS, 2 + 2 * hops)),
                            pltpu.SemaphoreType.DMA((N_STREAMS, 2 + 2 * hops)),
                            pltpu.SemaphoreType.DMA((N_LOADS,))],
            compiler_params=pltpu.CompilerParams(vmem_limit_bytes=VMEM_LIMIT, collective_id=0, has_side_effects=True),
            name="layers",
        )(msa_act, pair_act, opm_w_out, w_ab, tri_w_gate, tri_w_out, w_in, b_in, opm_norm, pair_mask,
          opm_b_out, tri_norm_in, tri_b_ab, tri_b_gate, tri_norm_out, tri_b_out)

    return jax.shard_map(device_fn, mesh=mesh, in_specs=(pair_spec, mask_spec, msa_spec) + (P(),) * 13,
                         out_specs=pair_spec, check_vma=False)
```

```python
import functools
import math

import jax
import jax.numpy as jnp
from jax import lax
from jax.experimental import pallas as pl
from jax.experimental.pallas import tpu as pltpu
from jax.sharding import PartitionSpec as P

F32 = jnp.float32
BF16 = jnp.bfloat16
EPS = 1e-5
VMEM_LIMIT = 63 * 1024 * 1024
NT = (((1,), (1,)), ((), ()))
LANES = 128

V_BQ, V_BP, V_BG, V_AP, V_AG, V_GATE, V_NI0, V_NI1, V_NO0, V_NO1, V_BO, V_BIN = range(12)


def sigmoid(x):
    return 1.0 / (1.0 + jnp.exp(-x))


def norm_rows(x, scale, offset):
    inv = 1.0 / x.shape[0]
    xc = x - jnp.sum(x, axis=0, keepdims=True) * inv
    var = jnp.sum(xc * xc, axis=0, keepdims=True) * inv
    return (xc * lax.rsqrt(var + EPS) * scale + offset).astype(BF16)


def twice(x):
    return jnp.concatenate([x, x], axis=1)


def project_rows(l, chunk, m_ref, w_ref, norm_ref, bias_ref, a_ref, b_out, xa, xb, scr):
    width = w_ref.shape[1] // 2
    dim = w_ref.shape[2]
    rows = scr.shape[0] // width
    depth = xa.shape[1] // rows
    block = 16
    scale, offset = norm_ref[l, 0:1].astype(F32), norm_ref[l, 1:2].astype(F32)

    at = pl.ds(chunk * rows, rows)
    lanes = pl.ds(chunk * LANES, LANES)

    for part, x_ref in enumerate((xa, xb)):
        def normalize(s, _):
            x = m_ref[pl.ds(part * depth + s * block, block), at, :].astype(F32).reshape(block * rows, dim)
            xc = x - jnp.sum(x, axis=1, keepdims=True) * (1.0 / dim)
            var = jnp.sum(xc * xc, axis=1, keepdims=True) * (1.0 / dim)
            xn = xc * lax.rsqrt(var + EPS)
            to = pl.ds(pl.multiple_of(s * block * rows, block * rows), block * rows)
            for f in range(dim // LANES):
                x_ref[f, to, :] = xn[:, f * LANES : (f + 1) * LANES]
            return 0

        lax.fori_loop(0, depth // block, normalize, 0)

    def residue(t2, _):
        for u in range(2):
            r = 2 * t2 + u
            xn = jnp.concatenate(
                [jnp.concatenate([x_ref[f, pl.ds(r, depth, stride=rows), :] for x_ref in (xa, xb)], axis=0)
                 for f in range(dim // LANES)], axis=1)
            mn = (xn * scale + offset).astype(BF16)
            out = lax.dot_general(w_ref[l], mn, NT, preferred_element_type=F32) + bias_ref[l]
            a_ref[l, pl.ds(pl.multiple_of(r * width, width), width), lanes] = out[:width].astype(BF16)
            scr[pl.ds(r, width, stride=rows), :] = out[width:]
        return 0

    lax.fori_loop(0, rows // 2, residue, 0)
    b_out(l, lanes, scr[...].astype(BF16).reshape(width, rows, LANES))


def prepare_wq(l, raw_ref, tmp_ref, wq_ref):
    cd = raw_ref.shape[0]
    width = math.isqrt(cd)
    tmp_ref[0, :, :] = raw_ref[...].astype(F32)
    for g in range(cd // LANES):
        per = LANES // width
        w = jnp.concatenate([tmp_ref[0, pl.ds(g * per + d, width, stride=width), :] for d in range(per)], axis=0)
        wq_ref[l, :, g * LANES : (g + 1) * LANES] = w.T.astype(BF16)


def outer_half(l, h, part, parts, a_ref, b_ref, q_ref):
    pairs, cd, lanes2 = q_ref.shape
    seqs = a_ref.shape[2]
    width = a_ref.shape[1] // (2 * pairs)
    half = lanes2 // 2
    scale = 1.0 / seqs

    def outer(t, _):
        rhs = b_ref[h, pl.ds(2 * t, 2)].reshape(2 * half, seqs)
        out = lax.dot_general(a_ref[l], rhs, NT, preferred_element_type=F32)
        out = (out * scale).astype(BF16)
        for d in range(2):
            blk = out[:, d * half : (d + 1) * half].reshape(2 * pairs, width, half)
            at = pl.ds(pl.multiple_of((2 * t + d) * width, width), width)
            for e in range(2):
                q_ref[:, at, e * half : (e + 1) * half] = blk[e * pairs : (e + 1) * pairs]
        return 0

    steps = cd // width // 2 // parts
    lax.fori_loop(part * steps, (part + 1) * steps, outer, 0)


def opm_half(l, h, wq_ref, vec_ref, z_ref, q_ref):
    pairs = q_ref.shape[0]
    bq = twice(vec_ref[l, V_BQ])

    def project(p, _):
        u = jnp.dot(wq_ref[l], q_ref[p], preferred_element_type=F32) + bq
        z_ref[h, p] = (z_ref[h, p].astype(F32) + u.astype(BF16).astype(F32)).astype(BF16)
        return 0

    lax.fori_loop(0, pairs, project, 0)


def gate_half(l, h, z_ref, mask_ref, wall_ref, vec_ref, fa_ref, fb_ref, g_ref, a_out, b_out):
    pairs = z_ref.shape[1]
    dim = z_ref.shape[2]
    half = z_ref.shape[3] // 2

    def project(p, _):
        zn = norm_rows(z_ref[h, p].astype(F32), twice(vec_ref[l, V_NI0]), twice(vec_ref[l, V_NI1]))
        mask = jnp.concatenate([mask_ref[h, pl.ds(p + e * pairs, 1), :] for e in range(2)], axis=1)
        at = pl.ds(pl.multiple_of(p * dim, dim), dim)

        def proj(q, v):
            w = wall_ref[l, q * dim : (q + 1) * dim]
            return jnp.dot(w, zn, preferred_element_type=F32) + twice(vec_ref[l, v])

        for q, f_ref, vp, vg in ((0, fb_ref, V_BP, V_BG), (2, fa_ref, V_AP, V_AG)):
            val = mask * sigmoid(proj(q + 1, vg)) * proj(q, vp)
            f_ref[0, at, :] = val[:, :half]
            f_ref[1, at, :] = val[:, half:]
        g_ref[h, p] = sigmoid(proj(4, V_GATE))
        return 0

    lax.fori_loop(0, pairs, project, 0)

    for f_ref, out in ((fb_ref, b_out), (fa_ref, a_out)):
        def relayout(t, _):
            for u in range(8):
                c = t * 8 + u
                lo = f_ref[0, pl.ds(c, pairs, stride=dim), :]
                hi = f_ref[1, pl.ds(c, pairs, stride=dim), :]
                out(c, h, jnp.concatenate([lo, hi], axis=0).astype(BF16))
            return 0

        lax.fori_loop(0, dim // 8, relayout, 0)


def triangle_half(jh, k, add, a_ref, b_ref, o_ref):
    dim = a_ref.shape[0]
    pairs = a_ref.shape[1] // 2

    def step(t, _):
        for u in range(8):
            c = t * 8 + u
            o = lax.dot_general(a_ref[c, :, k], b_ref[jh, c, :, k], NT, preferred_element_type=F32)
            for e in range(2):
                part, at = o[e * pairs : (e + 1) * pairs], pl.ds(c, pairs, stride=dim)
                o_ref[e, at, :] = o_ref[e, at, :] + part if add else part
        return 0

    lax.fori_loop(0, dim // 8, step, 0)


def finish_half(l, jh, o_refs, g_ref, z_ref, wo_ref, vec_ref):
    pairs = z_ref.shape[1]
    dim = z_ref.shape[2]

    def step(p, _):
        at = pl.ds(pl.multiple_of(p * dim, dim), dim)
        o = sum(jnp.concatenate([o_ref[0, at, :], o_ref[1, at, :]], axis=1) for o_ref in o_refs)
        on = norm_rows(o, twice(vec_ref[l, V_NO0]), twice(vec_ref[l, V_NO1]))
        u = jnp.dot(wo_ref[l], on, preferred_element_type=F32) + twice(vec_ref[l, V_BO])
        z_ref[jh, p] = (z_ref[jh, p].astype(F32) + g_ref[jh, p] * u.astype(BF16).astype(F32)).astype(BF16)
        return 0

    lax.fori_loop(0, pairs, step, 0)


class Stream:
    def __init__(self, buf, color, lo, lanes, rows, sems, where):
        self.buf, self.color, self.rows, self.lanes = buf, color, rows, lanes
        self.base, self.size = lo
        self.part = buf.shape[0] // 2
        self.ring_send, self.ring_recv, self.core_send, self.core_recv = sems
        self.chip, self.core, self.chips = where
        self.sent = []

    def block(self, chip, part, piece=None):
        lo, n = part * self.part + self.base, self.size
        if piece is not None:
            n = n // 2
            lo = lo + piece * n
        rows = pl.ds(pl.multiple_of(chip * self.rows, self.rows), self.rows)
        return self.buf.at[pl.ds(lo, n), rows, self.lanes]

    def copy(self, ref, send, recv, chip, core):
        return pltpu.make_async_remote_copy(
            src_ref=ref, dst_ref=ref, send_sem=send, recv_sem=recv,
            device_id={"dap": chip * 2 + core}, device_id_type=pl.DeviceIdType.MESH)

    def near(self, step):
        return lax.rem(self.chip + step + self.chips, self.chips)

    def ring(self, side, hop, chip, piece=None):
        return self.copy(self.block(chip, self.core, piece), self.ring_send.at[side, hop], self.ring_recv.at[side, hop],
                         self.near(1 - 2 * side), self.core)

    def across(self, slot, chip, part, piece=None):
        return self.copy(self.block(chip, part, piece), self.core_send.at[slot], self.core_recv.at[slot],
                         self.chip, 1 - self.core)

    def event(self, hop):
        if hop == -1:
            @pl.when(self.core == self.color)
            def _():
                self.across(0, self.chip, 1 - self.core).start()
                for side in range(2):
                    self.ring(side, 0, self.chip).start()
                self.across(1, self.chip, self.core).start()
            return
        if hop == 0:
            @pl.when(self.core != self.color)
            def _():
                self.across(0, self.chip, self.core).wait_recv()
                for side in range(2):
                    self.ring(side, 0, self.chip).start()
            return
        last = self.chips // 2
        for side in range(2):
            origin = self.near((2 * side - 1) * hop)
            piece = side if hop == last else None
            self.ring(side, hop - 1, origin, piece).wait_recv()
            if hop < last:
                self.ring(side, hop, origin, side if hop == last - 1 else None).start()
            self.across(2 + 2 * (hop - 1) + side, origin, self.core, piece).start()

    def finish(self):
        last = self.chips // 2

        @pl.when(self.core != self.color)
        def _():
            self.across(1, self.chip, 1 - self.core).wait_recv()

        for hop in range(1, last + 1):
            for side in range(2):
                origin = self.near((2 * side - 1) * hop)
                piece = side if hop == last else None
                self.across(2 + 2 * (hop - 1) + side, origin, 1 - self.core, piece).wait_recv()

    def drain(self):
        last = self.chips // 2

        @pl.when(self.core == self.color)
        def _():
            self.across(0, self.chip, 1 - self.core).wait_send()
            self.across(1, self.chip, self.core).wait_send()

        for side in range(2):
            for hop in range(last):
                self.ring(side, hop, self.chip, side if hop == last - 1 else None).wait_send()
            for hop in range(1, last + 1):
                self.across(2 + 2 * (hop - 1) + side, self.chip, self.core, side if hop == last else None).wait_send()


ORDER = (
    "p0", ("b100", -1), ("b101", -1), ("b100", 0), "p1", ("b101", 0), ("b110", -1), ("b110", 0), ("b111", -1), "p2",
    ("b111", 0), ("b100", 1), ("b101", 1), "p3", ("b121", -1), ("b120", -1), "vec", ("b110", 1), "w0", "mask",
    ("b121", 0), ("b100", 2), ("b120", 0), ("b101", 2), ("b110", 2), "pin", ("b111", 1), "q0", ("b120", 1), "q1",
    ("b110", 3), ("b121", 1), "q2", ("b120", 2), ("b100", 3), ("b121", 2), ("b111", 2), "q3", ("b120", 3),
    ("b20", -1), ("b110", 4), "w1", ("b100", 4), ("b101", 3), ("b20", 0), ("b111", 3), ("b21", -1), ("b21", 0),
    ("b121", 3), ("b120", 4), "O00a", "O00b", ("b20", 1), ("b101", 4), "O00p", ("b121", 4), ("b111", 4), ("b21", 1),
    "G00", "O01a", ("b20", 2), "O01b", ("b21", 2), "O01p", "G01", ("t100", -1), ("t110", -1), ("t100", 0),
    ("t101", -1), ("t101", 0), ("t100", 1), ("t101", 1), ("t100", 2), ("t101", 2), ("t100", 3), ("b20", 3),
    ("t110", 0), ("t101", 3), ("t111", -1), ("t100", 4), ("t111", 0), ("t101", 4), ("t110", 1), "T00", "N00",
    ("b20", 4), ("t111", 1), "O10a", ("t110", 2), "O10b", ("b21", 3), "O10p", ("t111", 2), "G10", ("t200", -1),
    ("t200", 0), ("b21", 4), ("t110", 3), ("t111", 3), ("t201", -1), ("t201", 0), ("t111", 4), ("t110", 4),
    ("t200", 1), "T01", ("t201", 1), "N01", "O11a", ("t200", 2), "O11b", "O11p", ("t201", 2), "G11", ("t211", -1),
    ("t200", 3), ("t210", -1), ("t210", 0), ("t211", 0), ("t200", 4), ("t201", 3), ("t210", 1), ("t211", 1),
    ("t210", 2), ("t211", 2), ("t201", 4), "K0", ("t210", 3), "K1", ("t211", 3), ("t210", 4), "L0", ("t211", 4),
    "N10", "X10", "L1", "N11", "X11",
)
NEEDS = {
    "O00a": ("b100", "b110", "b120",),
    "O01a": ("b101", "b111", "b121",),
    "T00": ("t100", "t101",),
    "O10a": ("b20",),
    "T01": ("t110", "t111",),
    "O11a": ("b21",),
    "K0": ("t200",),
    "K1": ("t201",),
    "L0": ("t210",),
    "L1": ("t211",),
}
N_STREAMS = 16
N_LOADS = 32


def layers_kernel(chips, m_hbm, z_hbm, wq_hbm, wab_hbm, wgate_hbm, wout_hbm, w_in_ref, b_in_ref, opm_norm_ref, mask_in,
                  bq_ref, norm_in_ref, b_ab_ref, b_gate_ref, norm_out_ref, b_o_ref, out_hbm,
                  b_buf, t_buf, a_ref, z_ref, at_ref, g_ref, q_scr, fa, fb, b_scr, wq_ref, wall_ref, wo_ref, vec_ref,
                  bias_ref, mask_ref, ring_send, ring_recv, core_send, core_recv, local_sem):
    me = lax.axis_index("dap")
    chip, core = me // 2, lax.rem(me, 2)
    rows, cols, dim = z_hbm.shape
    seqs = m_hbm.shape[0]
    layers = a_ref.shape[0]
    pairs = rows // 2
    half = cols // 2
    own = pl.ds(pl.multiple_of(chip * rows, rows), rows)

    barrier = pltpu.get_barrier_semaphore()
    right, left = lax.rem(chip + 1, chips), lax.rem(chip + chips - 1, chips)
    for there in (right * 2 + core, left * 2 + core, chip * 2 + 1 - core):
        pl.semaphore_signal(barrier, inc=1, device_id={"dap": there}, device_id_type=pl.DeviceIdType.MESH)

    used = [0]

    def load(src, dst):
        copy = pltpu.make_async_copy(src, dst, local_sem.at[used[0] % N_LOADS])
        used[0] += 1
        copy.start()
        return copy

    m_ref = t_buf.at[layers - 1, 0]
    z_raw = t_buf.at[layers - 1, 1]
    chunks = seqs // LANES
    m_loads = [load(m_hbm.at[pl.ds(a * LANES, LANES)], m_ref.at[:, pl.ds(a * rows, rows), :]) for a in range(chunks)]
    z_loads = [load(z_hbm.at[:, pl.ds((2 * c + h) * rows, rows), :],
                    z_raw.at[pl.ds(0, rows), pl.ds(c * rows, rows), pl.ds(h * dim, dim)])
               for h in range(2) for c in range(chips)]
    w_loads = []
    for l in range(layers):
        cd, ab = wq_hbm.shape[1], wab_hbm.shape[1]
        lanes = pl.ds(0, dim)
        w_loads.append(load(wq_hbm.at[l], q_scr.at[l, :, lanes]))
        w_loads.append(load(wab_hbm.at[l], q_scr.at[2 + l, pl.ds(0, ab), lanes]))
        w_loads.append(load(wgate_hbm.at[l], q_scr.at[4 + l, pl.ds(0, dim), lanes]))
        w_loads.append(load(wout_hbm.at[l], q_scr.at[4 + l, pl.ds(dim, dim), lanes]))

    where = (chip, core, chips)
    count = [0]

    def stream(buf, color, lo, lanes):
        sems = tuple(s.at[count[0]] for s in (ring_send, ring_recv, core_send, core_recv))
        count[0] += 1
        return Stream(buf, color, lo, lanes, rows, sems, where)

    width = b_buf.shape[2]
    full_b = pl.ds(0, seqs)
    full_t = pl.ds(0, cols)
    named = {}
    for s, (lo, n) in enumerate(((0, 1), (1, 1), (2, chunks - 2))):
        for q in range(2):
            named[f"b1{s}{q}"] = stream(b_buf.at[0, q], q, (0, width // 2), pl.ds(lo * LANES, n * LANES))
    for q in range(2):
        named[f"b2{q}"] = stream(b_buf.at[1, q], q, (0, width // 2), full_b)
        for s in range(2):
            named[f"t1{q}{s}"] = stream(t_buf.at[0, q], q, (s * dim // 4, dim // 4), full_t)
            named[f"t2{s}{q}"] = stream(t_buf.at[1, q], q, (0, dim // 2), pl.ds(s * half, half))

    def column(row):
        return jnp.broadcast_to(row, (LANES, row.shape[1])).T

    for l in range(layers):
        for q in range(2):
            at = pl.ds(q * width, width)
            bias_ref[l, at, :] = column(b_in_ref[l].astype(F32)[q : q + 1])

    def project(l, chunk):
        def b_out(l, lanes, v):
            b_buf[l, core, :, own, lanes] = v

        project_rows(l, chunk, m_ref, w_in_ref, opm_norm_ref, bias_ref, a_ref, b_out, fa, fb, b_scr)

    def vectors():
        bq, b_gate, b_o = (r[...].astype(F32) for r in (bq_ref, b_gate_ref, b_o_ref))
        for l in range(layers):
            norm_in, b_ab, norm_out = (r[l].astype(F32) for r in (norm_in_ref, b_ab_ref, norm_out_ref))
            table = ((V_BQ, bq, l), (V_BP, b_ab, 2), (V_BG, b_ab, 3), (V_AP, b_ab, 0), (V_AG, b_ab, 1),
                     (V_GATE, b_gate, l), (V_NI0, norm_in, 0), (V_NI1, norm_in, 1), (V_NO0, norm_out, 0),
                     (V_NO1, norm_out, 1), (V_BO, b_o, l))
            for v, src, r in table:
                vec_ref[l, v] = column(src[r : r + 1])

    def masks():
        to = lax.broadcasted_iota(jnp.int32, (cols, cols), 1)
        frm = lax.broadcasted_iota(jnp.int32, (cols, cols), 0)
        q, rest = to // half, to % half
        perm = (frm == (rest // rows) * (2 * rows) + q * rows + rest % rows).astype(F32).astype(BF16)
        mask = jnp.dot(mask_in[...].astype(F32).astype(BF16), perm, preferred_element_type=F32)
        for h in range(2):
            mask_ref[h] = mask[:, h * half : (h + 1) * half]

    def weights(l):
        prepare_wq(l, q_scr.at[l, :, pl.ds(0, dim)], fa, wq_ref)
        ab = wab_hbm.shape[1]
        fa[0, 0:ab, :] = q_scr[2 + l, 0:ab, 0:dim].astype(F32)
        for slot, q in enumerate((2, 3, 0, 1)):
            wall_ref[l, slot * dim : (slot + 1) * dim, :] = fa[0, pl.ds(q, dim, stride=4), :].T.astype(BF16)
        wall_ref[l, 4 * dim : 5 * dim, :] = q_scr[4 + l, 0:dim, 0:dim].astype(F32).T.astype(BF16)
        wo_ref[l] = q_scr[4 + l, dim : 2 * dim, 0:dim].astype(F32).T.astype(BF16)

    def pair_in():
        def step(p, _):
            for h in range(2):
                for e in range(2):
                    x = z_raw[e * pairs + p, :, h * dim : (h + 1) * dim].astype(F32)
                    z_ref[h, p, :, e * half : (e + 1) * half] = x.T.astype(BF16)
            return 0

        lax.fori_loop(0, pairs, step, 0)

    def outer(l, h, part):
        outer_half(l, h, part, 2, a_ref, b_buf.at[l], q_scr)

    def opm(l, h):
        opm_half(l, h, wq_ref, vec_ref, z_ref, q_scr)

    def gate(l, h):
        def a_out(c, h, v):
            at_ref[l, c, :, h * LANES : (h + 1) * LANES] = v

        def b_out(c, h, v):
            t_buf[l, core, c, own, h * LANES : (h + 1) * LANES] = v

        gate_half(l, h, z_ref, mask_ref, wall_ref, vec_ref, fa, fb, g_ref, a_out, b_out)

    def triangle(l, jh, k=full_t, o_ref=fa, add=False):
        triangle_half(jh, k, add, at_ref.at[l], t_buf.at[l], o_ref)

    def finish(l, jh, *o_refs):
        finish_half(l, jh, o_refs or (fa,), g_ref, z_ref, wo_ref, vec_ref)

    def pair_out(h):
        def step(p, _):
            for e in range(2):
                x = z_ref[h, p, :, e * half : (e + 1) * half].astype(F32)
                q_scr[p, h * half : (h + 1) * half, e * dim : (e + 1) * dim] = x.T.astype(BF16)
            return 0

        lax.fori_loop(0, pairs, step, 0)
        return [load(q_scr.at[:, pl.ds(h * half + c * rows, rows), pl.ds(e * dim, dim)],
                     out_hbm.at[pl.ds(e * pairs, pairs), pl.ds((2 * c + h) * rows, rows), :])
                for e in range(2) for c in range(chips)]

    stores = []

    def first_project(chunk):
        m_loads[chunk].wait()
        project(0, chunk)
        if chunk == 0:
            pl.semaphore_wait(barrier, 3)

    def first_weights():
        for copy in w_loads:
            copy.wait()
        weights(0)

    def first_pairs():
        for copy in z_loads:
            copy.wait()
        pair_in()

    tasks = {"vec": vectors, "mask": masks, "w0": first_weights, "w1": lambda: weights(1), "pin": first_pairs,
             "K0": lambda: triangle(1, 0, pl.ds(0, half)), "L0": lambda: triangle(1, 0, pl.ds(half, half), add=True),
             "K1": lambda: triangle(1, 1, pl.ds(0, half), fb), "L1": lambda: triangle(1, 1, pl.ds(half, half), fa),
             "N11": lambda: finish(1, 1, fa, fb)}
    for c in range(chunks):
        tasks[f"p{c}"] = functools.partial(first_project, c)
        tasks[f"q{c}"] = functools.partial(project, 1, c)
    for l in range(layers):
        for h in range(2):
            for part, letter in enumerate("ab"):
                tasks[f"O{l}{h}{letter}"] = functools.partial(outer, l, h, part)
            tasks[f"O{l}{h}p"] = functools.partial(opm, l, h)
            tasks[f"G{l}{h}"] = functools.partial(gate, l, h)
            tasks[f"T{l}{h}"] = functools.partial(triangle, l, h)
            tasks.setdefault(f"N{l}{h}", functools.partial(finish, l, h))
    for h in range(2):
        tasks[f"X1{h}"] = lambda h=h: stores.extend(pair_out(h))

    for item in ORDER:
        if item in tasks:
            for name in NEEDS.get(item, ()):
                named[name].finish()
            tasks[item]()
        else:
            name, hop = item
            named[name].event(hop)
    for s in named.values():
        s.drain()
    for copy in stores:
        copy.wait()


def solution(mesh):
    size = mesh.shape["dap"]
    chips = size // 2
    hops = chips // 2
    pair_spec = P(("batch", "dap"), None, None)
    mask_spec = P(("batch", "dap"), None)
    msa_spec = P(None, ("batch", "dap"), None)
    any_spec = pl.BlockSpec(memory_space=pl.ANY)
    vmem_spec = pl.BlockSpec(memory_space=pltpu.VMEM)

    def device_fn(pair_act, pair_mask, msa_act, opm_norm, opm_w_in, opm_b_in, opm_w_out, opm_b_out, tri_norm_in,
                  tri_w_ab, tri_b_ab, tri_w_gate, tri_b_gate, tri_norm_out, tri_w_out, tri_b_out):
        rows, cols, dim = pair_act.shape
        seqs, _, mdim = msa_act.shape
        layers = opm_norm.shape[0]
        width = opm_w_in.shape[-1]
        pairs = rows // 2
        half = cols // 2
        z_shape = (2, pairs, dim, 2 * half)

        w_in = jnp.transpose(opm_w_in, (0, 2, 3, 1)).reshape(layers, 2 * width, mdim)
        w_ab = tri_w_ab.reshape(layers, dim * 4, dim)

        return pl.pallas_call(
            functools.partial(layers_kernel, chips),
            out_shape=jax.ShapeDtypeStruct(pair_act.shape, BF16),
            in_specs=[any_spec] * 6 + [vmem_spec] * 10,
            out_specs=any_spec,
            scratch_shapes=[pltpu.VMEM((layers, 2, width, half, seqs), BF16),
                            pltpu.VMEM((layers, 2, dim, half, cols), BF16),
                            pltpu.VMEM((layers, rows * width, seqs), BF16),
                            pltpu.VMEM(z_shape, BF16),
                            pltpu.VMEM((layers, dim, rows, cols), BF16),
                            pltpu.VMEM(z_shape, F32),
                            pltpu.VMEM((pairs, width * width, 2 * half), BF16),
                            pltpu.VMEM((2, pairs * dim, LANES), F32),
                            pltpu.VMEM((2, pairs * dim, LANES), F32),
                            pltpu.VMEM((width * rows, LANES), F32),
                            pltpu.VMEM((layers, dim, width * width), BF16),
                            pltpu.VMEM((layers, 5 * dim, dim), BF16),
                            pltpu.VMEM((layers, dim, dim), BF16),
                            pltpu.VMEM((layers, V_BIN, dim, LANES), F32),
                            pltpu.VMEM((layers, 2 * width, LANES), F32),
                            pltpu.VMEM((2, rows, half), F32),
                            pltpu.SemaphoreType.DMA((N_STREAMS, 2, hops)),
                            pltpu.SemaphoreType.DMA((N_STREAMS, 2, hops)),
                            pltpu.SemaphoreType.DMA((N_STREAMS, 2 + 2 * hops)),
                            pltpu.SemaphoreType.DMA((N_STREAMS, 2 + 2 * hops)),
                            pltpu.SemaphoreType.DMA((N_LOADS,))],
            compiler_params=pltpu.CompilerParams(vmem_limit_bytes=VMEM_LIMIT, collective_id=0, has_side_effects=True),
            name="layers",
        )(msa_act, pair_act, opm_w_out, w_ab, tri_w_gate, tri_w_out, w_in, opm_b_in, opm_norm, pair_mask,
          opm_b_out, tri_norm_in, tri_b_ab, tri_b_gate, tri_norm_out, tri_b_out)

    return jax.shard_map(device_fn, mesh=mesh, in_specs=(pair_spec, mask_spec, msa_spec) + (P(),) * 13,
                         out_specs=pair_spec, check_vma=False)
```

```python
import functools
import math

import jax
import jax.numpy as jnp
from jax import lax
from jax.experimental import pallas as pl
from jax.experimental.pallas import tpu as pltpu
from jax.sharding import PartitionSpec as P

F32 = jnp.float32
BF16 = jnp.bfloat16
EPS = 1e-5
VMEM_LIMIT = 63 * 1024 * 1024
NT = (((1,), (1,)), ((), ()))
LANES = 128

V_BQ, V_BP, V_BG, V_AP, V_AG, V_GATE, V_NI0, V_NI1, V_NO0, V_NO1, V_BO, V_BIN = range(12)


def sigmoid(x):
    return 1.0 / (1.0 + jnp.exp(-x))


def norm_rows(x, scale, offset):
    inv = 1.0 / x.shape[0]
    xc = x - jnp.sum(x, axis=0, keepdims=True) * inv
    var = jnp.sum(xc * xc, axis=0, keepdims=True) * inv
    return (xc * lax.rsqrt(var + EPS) * scale + offset).astype(BF16)


def twice(x):
    return jnp.concatenate([x, x], axis=1)


def project_rows(l, chunk, m_ref, w_ref, norm_ref, bias_ref, a_ref, b_out, xa, xb, scr):
    width = w_ref.shape[1] // 2
    dim = w_ref.shape[2]
    rows = scr.shape[0] // width
    depth = xa.shape[1] // rows
    block = 16
    scale, offset = norm_ref[l, 0:1].astype(F32), norm_ref[l, 1:2].astype(F32)

    at = pl.ds(chunk * rows, rows)
    lanes = pl.ds(chunk * LANES, LANES)

    for part, x_ref in enumerate((xa, xb)):
        def normalize(s, _):
            x = m_ref[pl.ds(part * depth + s * block, block), at, :].astype(F32).reshape(block * rows, dim)
            xc = x - jnp.sum(x, axis=1, keepdims=True) * (1.0 / dim)
            var = jnp.sum(xc * xc, axis=1, keepdims=True) * (1.0 / dim)
            xn = xc * lax.rsqrt(var + EPS)
            to = pl.ds(pl.multiple_of(s * block * rows, block * rows), block * rows)
            for f in range(dim // LANES):
                x_ref[f, to, :] = xn[:, f * LANES : (f + 1) * LANES]
            return 0

        lax.fori_loop(0, depth // block, normalize, 0)

    def residue(t2, _):
        for u in range(2):
            r = 2 * t2 + u
            xn = jnp.concatenate(
                [jnp.concatenate([x_ref[f, pl.ds(r, depth, stride=rows), :] for x_ref in (xa, xb)], axis=0)
                 for f in range(dim // LANES)], axis=1)
            mn = (xn * scale + offset).astype(BF16)
            out = lax.dot_general(w_ref[l], mn, NT, preferred_element_type=F32) + bias_ref[l]
            a_ref[l, pl.ds(pl.multiple_of(r * width, width), width), lanes] = out[:width].astype(BF16)
            scr[pl.ds(r, width, stride=rows), :] = out[width:]
        return 0

    lax.fori_loop(0, rows // 2, residue, 0)
    b_out(l, lanes, scr[...].astype(BF16).reshape(width, rows, LANES))


def prepare_wq(l, raw_ref, tmp_ref, wq_ref):
    cd = raw_ref.shape[0]
    width = math.isqrt(cd)
    tmp_ref[0, :, :] = raw_ref[...].astype(F32)
    for g in range(cd // LANES):
        per = LANES // width
        w = jnp.concatenate([tmp_ref[0, pl.ds(g * per + d, width, stride=width), :] for d in range(per)], axis=0)
        wq_ref[l, :, g * LANES : (g + 1) * LANES] = w.T.astype(BF16)


def outer_half(l, h, part, parts, a_ref, b_ref, q_ref):
    pairs, cd, lanes2 = q_ref.shape
    seqs = a_ref.shape[2]
    width = a_ref.shape[1] // (2 * pairs)
    half = lanes2 // 2
    scale = 1.0 / seqs

    def outer(t, _):
        rhs = b_ref[h, pl.ds(2 * t, 2)].reshape(2 * half, seqs)
        out = lax.dot_general(a_ref[l], rhs, NT, preferred_element_type=F32)
        out = (out * scale).astype(BF16)
        for d in range(2):
            blk = out[:, d * half : (d + 1) * half].reshape(2 * pairs, width, half)
            at = pl.ds(pl.multiple_of((2 * t + d) * width, width), width)
            for e in range(2):
                q_ref[:, at, e * half : (e + 1) * half] = blk[e * pairs : (e + 1) * pairs]
        return 0

    steps = cd // width // 2 // parts
    lax.fori_loop(part * steps, (part + 1) * steps, outer, 0)


def opm_half(l, h, wq_ref, vec_ref, z_ref, q_ref):
    pairs = q_ref.shape[0]
    bq = twice(vec_ref[l, V_BQ])

    def project(p, _):
        u = jnp.dot(wq_ref[l], q_ref[p], preferred_element_type=F32) + bq
        z_ref[h, p] = (z_ref[h, p].astype(F32) + u.astype(BF16).astype(F32)).astype(BF16)
        return 0

    lax.fori_loop(0, pairs, project, 0)


def gate_half(l, h, z_ref, mask_ref, wall_ref, vec_ref, fa_ref, fb_ref, g_ref, a_out, b_out):
    pairs = z_ref.shape[1]
    dim = z_ref.shape[2]
    half = z_ref.shape[3] // 2

    def project(p, _):
        zn = norm_rows(z_ref[h, p].astype(F32), twice(vec_ref[l, V_NI0]), twice(vec_ref[l, V_NI1]))
        mask = jnp.concatenate([mask_ref[h, pl.ds(p + e * pairs, 1), :] for e in range(2)], axis=1)
        at = pl.ds(pl.multiple_of(p * dim, dim), dim)

        def proj(q, v):
            w = wall_ref[l, q * dim : (q + 1) * dim]
            return jnp.dot(w, zn, preferred_element_type=F32) + twice(vec_ref[l, v])

        for q, f_ref, vp, vg in ((0, fb_ref, V_BP, V_BG), (2, fa_ref, V_AP, V_AG)):
            val = mask * sigmoid(proj(q + 1, vg)) * proj(q, vp)
            f_ref[0, at, :] = val[:, :half]
            f_ref[1, at, :] = val[:, half:]
        g_ref[h, p] = sigmoid(proj(4, V_GATE))
        return 0

    lax.fori_loop(0, pairs, project, 0)

    for f_ref, out in ((fb_ref, b_out), (fa_ref, a_out)):
        def relayout(t, _):
            for u in range(8):
                c = t * 8 + u
                lo = f_ref[0, pl.ds(c, pairs, stride=dim), :]
                hi = f_ref[1, pl.ds(c, pairs, stride=dim), :]
                out(c, h, jnp.concatenate([lo, hi], axis=0).astype(BF16))
            return 0

        lax.fori_loop(0, dim // 8, relayout, 0)


def triangle_half(jh, k, add, a_ref, b_ref, o_ref):
    dim = a_ref.shape[0]
    pairs = a_ref.shape[1] // 2

    def step(t, _):
        for u in range(8):
            c = t * 8 + u
            o = lax.dot_general(a_ref[c, :, k], b_ref[jh, c, :, k], NT, preferred_element_type=F32)
            for e in range(2):
                part, at = o[e * pairs : (e + 1) * pairs], pl.ds(c, pairs, stride=dim)
                o_ref[e, at, :] = o_ref[e, at, :] + part if add else part
        return 0

    lax.fori_loop(0, dim // 8, step, 0)


def finish_half(l, jh, o_refs, g_ref, z_ref, wo_ref, vec_ref, store=None):
    pairs = z_ref.shape[1]
    dim = z_ref.shape[2]

    def step(p, _):
        at = pl.ds(pl.multiple_of(p * dim, dim), dim)
        o = sum(jnp.concatenate([o_ref[0, at, :], o_ref[1, at, :]], axis=1) for o_ref in o_refs)
        on = norm_rows(o, twice(vec_ref[l, V_NO0]), twice(vec_ref[l, V_NO1]))
        u = jnp.dot(wo_ref[l], on, preferred_element_type=F32) + twice(vec_ref[l, V_BO])
        z_new = (z_ref[jh, p].astype(F32) + g_ref[jh, p] * u.astype(BF16).astype(F32)).astype(BF16)
        if store is None:
            z_ref[jh, p] = z_new
        else:
            store(p, z_new.astype(F32))
        return 0

    lax.fori_loop(0, pairs, step, 0)


class Stream:
    def __init__(self, buf, color, lo, lanes, rows, sems, where):
        self.buf, self.color, self.rows, self.lanes = buf, color, rows, lanes
        self.base, self.size = lo
        self.part = buf.shape[0] // 2
        self.ring_send, self.ring_recv, self.core_send, self.core_recv = sems
        self.chip, self.core, self.chips = where
        self.sent = []

    def block(self, chip, part, piece=None):
        lo, n = part * self.part + self.base, self.size
        if piece is not None:
            n = n // 2
            lo = lo + piece * n
        rows = pl.ds(pl.multiple_of(chip * self.rows, self.rows), self.rows)
        return self.buf.at[pl.ds(lo, n), rows, self.lanes]

    def copy(self, ref, send, recv, chip, core):
        return pltpu.make_async_remote_copy(
            src_ref=ref, dst_ref=ref, send_sem=send, recv_sem=recv,
            device_id={"dap": chip * 2 + core}, device_id_type=pl.DeviceIdType.MESH)

    def near(self, step):
        return lax.rem(self.chip + step + self.chips, self.chips)

    def ring(self, side, hop, chip, piece=None):
        return self.copy(self.block(chip, self.core, piece), self.ring_send.at[side, hop], self.ring_recv.at[side, hop],
                         self.near(1 - 2 * side), self.core)

    def across(self, slot, chip, part, piece=None):
        return self.copy(self.block(chip, part, piece), self.core_send.at[slot], self.core_recv.at[slot],
                         self.chip, 1 - self.core)

    def event(self, hop):
        if hop == -1:
            @pl.when(self.core == self.color)
            def _():
                self.across(0, self.chip, 1 - self.core).start()
                for side in range(2):
                    self.ring(side, 0, self.chip).start()
                self.across(1, self.chip, self.core).start()
            return
        if hop == 0:
            @pl.when(self.core != self.color)
            def _():
                self.across(0, self.chip, self.core).wait_recv()
                for side in range(2):
                    self.ring(side, 0, self.chip).start()
            return
        last = self.chips // 2
        for side in range(2):
            origin = self.near((2 * side - 1) * hop)
            piece = side if hop == last else None
            self.ring(side, hop - 1, origin, piece).wait_recv()
            if hop < last:
                self.ring(side, hop, origin, side if hop == last - 1 else None).start()
            self.across(2 + 2 * (hop - 1) + side, origin, self.core, piece).start()

    def finish(self):
        last = self.chips // 2

        @pl.when(self.core != self.color)
        def _():
            self.across(1, self.chip, 1 - self.core).wait_recv()

        for hop in range(1, last + 1):
            for side in range(2):
                origin = self.near((2 * side - 1) * hop)
                piece = side if hop == last else None
                self.across(2 + 2 * (hop - 1) + side, origin, 1 - self.core, piece).wait_recv()

    def drain(self):
        last = self.chips // 2

        @pl.when(self.core == self.color)
        def _():
            self.across(0, self.chip, 1 - self.core).wait_send()
            self.across(1, self.chip, self.core).wait_send()

        for side in range(2):
            for hop in range(last):
                self.ring(side, hop, self.chip, side if hop == last - 1 else None).wait_send()
            for hop in range(1, last + 1):
                self.across(2 + 2 * (hop - 1) + side, self.chip, self.core, side if hop == last else None).wait_send()


ORDER = (
    "p0", ("b100", -1), ("b101", -1), ("b100", 0), "p1", ("b101", 0), ("b110", -1), ("b110", 0), ("b111", -1), "p2",
    ("b111", 0), ("b100", 1), ("b101", 1), "p3", ("b121", -1), ("b120", -1), "vec", ("b110", 1), "w0", "mask",
    ("b121", 0), ("b100", 2), ("b120", 0), ("b101", 2), ("b110", 2), "pin", ("b111", 1), "q0", ("b120", 1), "q1",
    ("b110", 3), ("b121", 1), "q2", ("b120", 2), ("b100", 3), ("b121", 2), ("b111", 2), "q3", ("b120", 3),
    ("b20", -1), ("b110", 4), "w1", ("b100", 4), ("b101", 3), ("b20", 0), ("b111", 3), ("b21", -1), ("b21", 0),
    ("b121", 3), ("b120", 4), "O00a", "O00b", ("b20", 1), ("b101", 4), "O00p", ("b121", 4), ("b111", 4), ("b21", 1),
    "G00", "O01a", ("b20", 2), "O01b", ("b21", 2), "O01p", "G01", ("t100", -1), ("t110", -1), ("t100", 0),
    ("t101", -1), ("t101", 0), ("t100", 1), ("t101", 1), ("t100", 2), ("t101", 2), ("t100", 3), ("b20", 3),
    ("t110", 0), ("t101", 3), ("t111", -1), ("t100", 4), ("t111", 0), ("t101", 4), ("t110", 1), "T00", "N00",
    ("b20", 4), ("t111", 1), "O10a", ("t110", 2), "O10b", ("b21", 3), "O10p", ("t111", 2), "G10", ("t200", -1),
    ("t200", 0), ("b21", 4), ("t110", 3), ("t111", 3), ("t201", -1), ("t201", 0), ("t111", 4), ("t110", 4),
    ("t200", 1), "T01", ("t201", 1), "N01", "O11a", ("t200", 2), "O11b", "O11p", ("t201", 2), "G11", ("t211", -1),
    ("t200", 3), ("t210", -1), ("t210", 0), ("t211", 0), ("t200", 4), ("t201", 3), ("t210", 1), ("t211", 1),
    ("t210", 2), ("t211", 2), ("t201", 4), "K0", ("t210", 3), "K1", ("t211", 3), ("t210", 4), "L0", ("t211", 4),
    "N10", "X10", "L1", "Y11",
)
NEEDS = {
    "O00a": ("b100", "b110", "b120",),
    "O01a": ("b101", "b111", "b121",),
    "T00": ("t100", "t101",),
    "O10a": ("b20",),
    "T01": ("t110", "t111",),
    "O11a": ("b21",),
    "K0": ("t200",),
    "K1": ("t201",),
    "L0": ("t210",),
    "L1": ("t211",),
}
N_STREAMS = 16
N_LOADS = 28


def layers_kernel(chips, m_hbm, z_hbm, wq_hbm, wab_hbm, wgate_hbm, wout_hbm, w_in_ref, b_in_ref, opm_norm_ref, mask_in,
                  bq_ref, norm_in_ref, b_ab_ref, b_gate_ref, norm_out_ref, b_o_ref, out_hbm,
                  b_buf, t_buf, a_ref, z_ref, at_ref, g_ref, q_scr, fa, fb, b_scr, wq_ref, wall_ref, wo_ref, vec_ref,
                  bias_ref, mask_ref, ring_send, ring_recv, core_send, core_recv, local_sem, out_sem):
    me = lax.axis_index("dap")
    chip, core = me // 2, lax.rem(me, 2)
    rows, cols, dim = z_hbm.shape
    seqs = m_hbm.shape[0]
    layers = a_ref.shape[0]
    pairs = rows // 2
    half = cols // 2
    own = pl.ds(pl.multiple_of(chip * rows, rows), rows)

    barrier = pltpu.get_barrier_semaphore()
    right, left = lax.rem(chip + 1, chips), lax.rem(chip + chips - 1, chips)
    for there in (right * 2 + core, left * 2 + core, chip * 2 + 1 - core):
        pl.semaphore_signal(barrier, inc=1, device_id={"dap": there}, device_id_type=pl.DeviceIdType.MESH)

    used = [0]

    def load(src, dst):
        copy = pltpu.make_async_copy(src, dst, local_sem.at[used[0] % N_LOADS])
        used[0] += 1
        copy.start()
        return copy

    m_ref = t_buf.at[layers - 1, 0]
    z_raw = t_buf.at[layers - 1, 1]
    chunks = seqs // LANES
    m_loads = [load(m_hbm.at[pl.ds(a * LANES, LANES)], m_ref.at[:, pl.ds(a * rows, rows), :]) for a in range(chunks)]
    z_loads, w_loads = [], []

    def later_loads():
        z_loads.extend([load(z_hbm.at[:, pl.ds((2 * c + h) * rows, rows), :],
                        z_raw.at[pl.ds(0, rows), pl.ds(c * rows, rows), pl.ds(h * dim, dim)])
                   for h in range(2) for c in range(chips)])
        for l in range(layers):
            cd, ab = wq_hbm.shape[1], wab_hbm.shape[1]
            lanes = pl.ds(0, dim)
            w_loads.append(load(wq_hbm.at[l], q_scr.at[l, :, lanes]))
            w_loads.append(load(wab_hbm.at[l], q_scr.at[2 + l, pl.ds(0, ab), lanes]))
            w_loads.append(load(wgate_hbm.at[l], q_scr.at[4 + l, pl.ds(0, dim), lanes]))
            w_loads.append(load(wout_hbm.at[l], q_scr.at[4 + l, pl.ds(dim, dim), lanes]))

    where = (chip, core, chips)
    count = [0]

    def stream(buf, color, lo, lanes):
        sems = tuple(s.at[count[0]] for s in (ring_send, ring_recv, core_send, core_recv))
        count[0] += 1
        return Stream(buf, color, lo, lanes, rows, sems, where)

    width = b_buf.shape[2]
    full_b = pl.ds(0, seqs)
    full_t = pl.ds(0, cols)
    named = {}
    for s, (lo, n) in enumerate(((0, 1), (1, 1), (2, chunks - 2))):
        for q in range(2):
            named[f"b1{s}{q}"] = stream(b_buf.at[0, q], q, (0, width // 2), pl.ds(lo * LANES, n * LANES))
    for q in range(2):
        named[f"b2{q}"] = stream(b_buf.at[1, q], q, (0, width // 2), full_b)
        for s in range(2):
            named[f"t1{q}{s}"] = stream(t_buf.at[0, q], q, (s * dim // 4, dim // 4), full_t)
            named[f"t2{s}{q}"] = stream(t_buf.at[1, q], q, (0, dim // 2), pl.ds(s * half, half))

    def column(row):
        return jnp.broadcast_to(row, (LANES, row.shape[1])).T

    for l in range(layers):
        for q in range(2):
            at = pl.ds(q * width, width)
            bias_ref[l, at, :] = column(b_in_ref[l].astype(F32)[q : q + 1])

    def project(l, chunk):
        def b_out(l, lanes, v):
            b_buf[l, core, :, own, lanes] = v

        project_rows(l, chunk, m_ref, w_in_ref, opm_norm_ref, bias_ref, a_ref, b_out, fa, fb, b_scr)

    def vectors():
        bq, b_gate, b_o = (r[...].astype(F32) for r in (bq_ref, b_gate_ref, b_o_ref))
        for l in range(layers):
            norm_in, b_ab, norm_out = (r[l].astype(F32) for r in (norm_in_ref, b_ab_ref, norm_out_ref))
            table = ((V_BQ, bq, l), (V_BP, b_ab, 2), (V_BG, b_ab, 3), (V_AP, b_ab, 0), (V_AG, b_ab, 1),
                     (V_GATE, b_gate, l), (V_NI0, norm_in, 0), (V_NI1, norm_in, 1), (V_NO0, norm_out, 0),
                     (V_NO1, norm_out, 1), (V_BO, b_o, l))
            for v, src, r in table:
                vec_ref[l, v] = column(src[r : r + 1])

    def masks():
        to = lax.broadcasted_iota(jnp.int32, (cols, cols), 1)
        frm = lax.broadcasted_iota(jnp.int32, (cols, cols), 0)
        q, rest = to // half, to % half
        perm = (frm == (rest // rows) * (2 * rows) + q * rows + rest % rows).astype(F32).astype(BF16)
        mask = jnp.dot(mask_in[...].astype(F32).astype(BF16), perm, preferred_element_type=F32)
        for h in range(2):
            mask_ref[h] = mask[:, h * half : (h + 1) * half]

    def weights(l):
        prepare_wq(l, q_scr.at[l, :, pl.ds(0, dim)], fa, wq_ref)
        ab = wab_hbm.shape[1]
        fa[0, 0:ab, :] = q_scr[2 + l, 0:ab, 0:dim].astype(F32)
        for slot, q in enumerate((2, 3, 0, 1)):
            wall_ref[l, slot * dim : (slot + 1) * dim, :] = fa[0, pl.ds(q, dim, stride=4), :].T.astype(BF16)
        wall_ref[l, 4 * dim : 5 * dim, :] = q_scr[4 + l, 0:dim, 0:dim].astype(F32).T.astype(BF16)
        wo_ref[l] = q_scr[4 + l, dim : 2 * dim, 0:dim].astype(F32).T.astype(BF16)

    def pair_in():
        def step(p, _):
            for h in range(2):
                for e in range(2):
                    x = z_raw[e * pairs + p, :, h * dim : (h + 1) * dim].astype(F32)
                    z_ref[h, p, :, e * half : (e + 1) * half] = x.T.astype(BF16)
            return 0

        lax.fori_loop(0, pairs, step, 0)

    def outer(l, h, part):
        outer_half(l, h, part, 2, a_ref, b_buf.at[l], q_scr)

    def opm(l, h):
        opm_half(l, h, wq_ref, vec_ref, z_ref, q_scr)

    def gate(l, h):
        def a_out(c, h, v):
            at_ref[l, c, :, h * LANES : (h + 1) * LANES] = v

        def b_out(c, h, v):
            t_buf[l, core, c, own, h * LANES : (h + 1) * LANES] = v

        gate_half(l, h, z_ref, mask_ref, wall_ref, vec_ref, fa, fb, g_ref, a_out, b_out)

    def triangle(l, jh, k=full_t, o_ref=fa, add=False):
        triangle_half(jh, k, add, at_ref.at[l], t_buf.at[l], o_ref)

    def finish(l, jh, *o_refs):
        finish_half(l, jh, o_refs or (fa,), g_ref, z_ref, wo_ref, vec_ref)

    def handed(h, p, e):
        row = e * pairs + p
        return pltpu.make_async_copy(at_ref.at[0, pl.ds(row * chips, chips), :, pl.ds(h * half, half)],
                                     out_hbm.at[row, :, h], out_sem.at[h, p, e])

    def last_columns(h, *o_refs):
        def store(p, x):
            for e in range(2):
                block = x[:, e * half : (e + 1) * half].T.astype(BF16).reshape(chips, rows, dim)
                at_ref[0, pl.ds((e * pairs + p) * chips, chips), :, h * half : (h + 1) * half] = block
            for e in range(2):
                handed(h, p, e).start()

        finish_half(layers - 1, h, o_refs, g_ref, z_ref, wo_ref, vec_ref, store)

    def first_project(chunk):
        m_loads[chunk].wait()
        if chunk == 0:
            later_loads()
        project(0, chunk)
        if chunk == 0:
            pl.semaphore_wait(barrier, 3)

    def first_weights():
        for copy in w_loads:
            copy.wait()
        weights(0)

    def first_pairs():
        for copy in z_loads:
            copy.wait()
        pair_in()

    tasks = {"vec": vectors, "mask": masks, "w0": first_weights, "w1": lambda: weights(1), "pin": first_pairs,
             "K0": lambda: triangle(1, 0, pl.ds(0, half)), "L0": lambda: triangle(1, 0, pl.ds(half, half), add=True),
             "K1": lambda: triangle(1, 1, pl.ds(0, half), fb), "N10": lambda: last_columns(0, fa), "L1": lambda: triangle(1, 1, pl.ds(half, half), fa), "Y11": lambda: last_columns(1, fa, fb),
             "X10": lambda: None}
    for c in range(chunks):
        tasks[f"p{c}"] = functools.partial(first_project, c)
        tasks[f"q{c}"] = functools.partial(project, 1, c)
    for l in range(layers):
        for h in range(2):
            for part, letter in enumerate("ab"):
                tasks[f"O{l}{h}{letter}"] = functools.partial(outer, l, h, part)
            tasks[f"O{l}{h}p"] = functools.partial(opm, l, h)
            tasks[f"G{l}{h}"] = functools.partial(gate, l, h)
            tasks[f"T{l}{h}"] = functools.partial(triangle, l, h)
            tasks.setdefault(f"N{l}{h}", functools.partial(finish, l, h))
    for item in ORDER:
        if item in tasks:
            for name in NEEDS.get(item, ()):
                named[name].finish()
            tasks[item]()
        else:
            name, hop = item
            named[name].event(hop)
    for s in named.values():
        s.drain()
    for h in range(2):
        for p in range(pairs):
            for e in range(2):
                handed(h, p, e).wait()


def solution(mesh):
    size = mesh.shape["dap"]
    chips = size // 2
    hops = chips // 2
    pair_spec = P(("batch", "dap"), None, None)
    mask_spec = P(("batch", "dap"), None)
    msa_spec = P(None, ("batch", "dap"), None)
    any_spec = pl.BlockSpec(memory_space=pl.ANY)
    vmem_spec = pl.BlockSpec(memory_space=pltpu.VMEM)

    def device_fn(pair_act, pair_mask, msa_act, opm_norm, opm_w_in, opm_b_in, opm_w_out, opm_b_out, tri_norm_in,
                  tri_w_ab, tri_b_ab, tri_w_gate, tri_b_gate, tri_norm_out, tri_w_out, tri_b_out):
        rows, cols, dim = pair_act.shape
        seqs, _, mdim = msa_act.shape
        layers = opm_norm.shape[0]
        width = opm_w_in.shape[-1]
        pairs = rows // 2
        half = cols // 2
        z_shape = (2, pairs, dim, 2 * half)

        w_in = jnp.transpose(opm_w_in, (0, 2, 3, 1)).reshape(layers, 2 * width, mdim)
        w_ab = tri_w_ab.reshape(layers, dim * 4, dim)

        return pl.pallas_call(
            functools.partial(layers_kernel, chips),
            out_shape=jax.ShapeDtypeStruct((rows, chips, 2, rows, dim), BF16),
            in_specs=[any_spec] * 6 + [vmem_spec] * 10,
            out_specs=any_spec,
            scratch_shapes=[pltpu.VMEM((layers, 2, width, half, seqs), BF16),
                            pltpu.VMEM((layers, 2, dim, half, cols), BF16),
                            pltpu.VMEM((layers, rows * width, seqs), BF16),
                            pltpu.VMEM(z_shape, BF16),
                            pltpu.VMEM((layers, dim, rows, cols), BF16),
                            pltpu.VMEM(z_shape, F32),
                            pltpu.VMEM((pairs, width * width, 2 * half), BF16),
                            pltpu.VMEM((2, pairs * dim, LANES), F32),
                            pltpu.VMEM((2, pairs * dim, LANES), F32),
                            pltpu.VMEM((width * rows, LANES), F32),
                            pltpu.VMEM((layers, dim, width * width), BF16),
                            pltpu.VMEM((layers, 5 * dim, dim), BF16),
                            pltpu.VMEM((layers, dim, dim), BF16),
                            pltpu.VMEM((layers, V_BIN, dim, LANES), F32),
                            pltpu.VMEM((layers, 2 * width, LANES), F32),
                            pltpu.VMEM((2, rows, half), F32),
                            pltpu.SemaphoreType.DMA((N_STREAMS, 2, hops)),
                            pltpu.SemaphoreType.DMA((N_STREAMS, 2, hops)),
                            pltpu.SemaphoreType.DMA((N_STREAMS, 2 + 2 * hops)),
                            pltpu.SemaphoreType.DMA((N_STREAMS, 2 + 2 * hops)),
                            pltpu.SemaphoreType.DMA((N_LOADS,)),
                            pltpu.SemaphoreType.DMA((2, pairs, 2))],
            compiler_params=pltpu.CompilerParams(vmem_limit_bytes=VMEM_LIMIT, collective_id=0, has_side_effects=True),
            name="layers",
        )(msa_act, pair_act, opm_w_out, w_ab, tri_w_gate, tri_w_out, w_in, opm_b_in, opm_norm, pair_mask,
          opm_b_out, tri_norm_in, tri_b_ab, tri_b_gate, tri_norm_out, tri_b_out).reshape(pair_act.shape)

    return jax.shard_map(device_fn, mesh=mesh, in_specs=(pair_spec, mask_spec, msa_spec) + (P(),) * 13,
                         out_specs=pair_spec, check_vma=False)
```

```python
import functools
import math

import jax
import jax.numpy as jnp
from jax import lax
from jax.experimental import pallas as pl
from jax.experimental.pallas import tpu as pltpu
from jax.sharding import PartitionSpec as P

F32 = jnp.float32
BF16 = jnp.bfloat16
EPS = 1e-5
VMEM_LIMIT = 63 * 1024 * 1024
NT = (((1,), (1,)), ((), ()))
LANES = 128

V_BQ, V_BP, V_BG, V_AP, V_AG, V_GATE, V_NI0, V_NI1, V_NO0, V_NO1, V_BO, V_BIN = range(12)


def sigmoid(x):
    return 1.0 / (1.0 + jnp.exp(-x))


def norm_rows(x, scale, offset):
    inv = 1.0 / x.shape[0]
    xc = x - jnp.sum(x, axis=0, keepdims=True) * inv
    var = jnp.sum(xc * xc, axis=0, keepdims=True) * inv
    return (xc * lax.rsqrt(var + EPS) * scale + offset).astype(BF16)


def twice(x):
    return jnp.concatenate([x, x], axis=1)


def project_rows(l, chunk, m_ref, w_ref, norm_ref, bias_ref, a_ref, b_out, xa, xb, scr):
    width = w_ref.shape[1] // 2
    dim = w_ref.shape[2]
    rows = scr.shape[0] // width
    depth = xa.shape[1] // rows
    block = 16
    scale, offset = norm_ref[l, 0:1].astype(F32), norm_ref[l, 1:2].astype(F32)

    at = pl.ds(chunk * rows, rows)
    lanes = pl.ds(chunk * LANES, LANES)

    for part, x_ref in enumerate((xa, xb)):
        def normalize(s, _):
            x = m_ref[pl.ds(part * depth + s * block, block), at, :].astype(F32).reshape(block * rows, dim)
            xc = x - jnp.sum(x, axis=1, keepdims=True) * (1.0 / dim)
            var = jnp.sum(xc * xc, axis=1, keepdims=True) * (1.0 / dim)
            xn = xc * lax.rsqrt(var + EPS)
            to = pl.ds(pl.multiple_of(s * block * rows, block * rows), block * rows)
            for f in range(dim // LANES):
                x_ref[f, to, :] = xn[:, f * LANES : (f + 1) * LANES]
            return 0

        lax.fori_loop(0, depth // block, normalize, 0)

    def residue(t2, _):
        for u in range(2):
            r = 2 * t2 + u
            xn = jnp.concatenate(
                [jnp.concatenate([x_ref[f, pl.ds(r, depth, stride=rows), :] for x_ref in (xa, xb)], axis=0)
                 for f in range(dim // LANES)], axis=1)
            mn = (xn * scale + offset).astype(BF16)
            out = lax.dot_general(w_ref[l], mn, NT, preferred_element_type=F32) + bias_ref[l]
            a_ref[l, pl.ds(pl.multiple_of(r * width, width), width), lanes] = out[:width].astype(BF16)
            scr[pl.ds(r, width, stride=rows), :] = out[width:]
        return 0

    lax.fori_loop(0, rows // 2, residue, 0)
    b_out(l, lanes, scr[...].astype(BF16).reshape(width, rows, LANES))


def prepare_wq(l, raw_ref, tmp_ref, wq_ref):
    cd = raw_ref.shape[0]
    width = math.isqrt(cd)
    tmp_ref[0, :, :] = raw_ref[...].astype(F32)
    for g in range(cd // LANES):
        per = LANES // width
        w = jnp.concatenate([tmp_ref[0, pl.ds(g * per + d, width, stride=width), :] for d in range(per)], axis=0)
        wq_ref[l, :, g * LANES : (g + 1) * LANES] = w.T.astype(BF16)


def outer_half(l, h, part, parts, a_ref, b_ref, q_ref):
    pairs, cd, lanes2 = q_ref.shape
    seqs = a_ref.shape[2]
    width = a_ref.shape[1] // (2 * pairs)
    half = lanes2 // 2
    scale = 1.0 / seqs

    def outer(t, _):
        rhs = b_ref[h, pl.ds(2 * t, 2)].reshape(2 * half, seqs)
        out = lax.dot_general(a_ref[l], rhs, NT, preferred_element_type=F32)
        out = (out * scale).astype(BF16)
        for d in range(2):
            blk = out[:, d * half : (d + 1) * half].reshape(2 * pairs, width, half)
            at = pl.ds(pl.multiple_of((2 * t + d) * width, width), width)
            for e in range(2):
                q_ref[:, at, e * half : (e + 1) * half] = blk[e * pairs : (e + 1) * pairs]
        return 0

    steps = cd // width // 2 // parts
    lax.fori_loop(part * steps, (part + 1) * steps, outer, 0)


def opm_half(l, h, wq_ref, vec_ref, z_ref, q_ref):
    pairs = q_ref.shape[0]
    bq = twice(vec_ref[l, V_BQ])

    def project(p, _):
        u = jnp.dot(wq_ref[l], q_ref[p], preferred_element_type=F32) + bq
        z_ref[h, p] = (z_ref[h, p].astype(F32) + u.astype(BF16).astype(F32)).astype(BF16)
        return 0

    lax.fori_loop(0, pairs, project, 0)


def gate_half(l, h, z_ref, mask_ref, wall_ref, vec_ref, fa_ref, fb_ref, g_ref, a_out, b_out):
    pairs = z_ref.shape[1]
    dim = z_ref.shape[2]
    half = z_ref.shape[3] // 2

    def project(p, _):
        zn = norm_rows(z_ref[h, p].astype(F32), twice(vec_ref[l, V_NI0]), twice(vec_ref[l, V_NI1]))
        mask = jnp.concatenate([mask_ref[h, pl.ds(p + e * pairs, 1), :] for e in range(2)], axis=1)
        at = pl.ds(pl.multiple_of(p * dim, dim), dim)

        def proj(q, v):
            w = wall_ref[l, q * dim : (q + 1) * dim]
            return jnp.dot(w, zn, preferred_element_type=F32) + twice(vec_ref[l, v])

        for q, f_ref, vp, vg in ((0, fb_ref, V_BP, V_BG), (2, fa_ref, V_AP, V_AG)):
            val = mask * sigmoid(proj(q + 1, vg)) * proj(q, vp)
            f_ref[0, at, :] = val[:, :half]
            f_ref[1, at, :] = val[:, half:]
        g_ref[h, p] = sigmoid(proj(4, V_GATE))
        return 0

    lax.fori_loop(0, pairs, project, 0)

    for f_ref, out in ((fb_ref, b_out), (fa_ref, a_out)):
        def relayout(t, _):
            for u in range(8):
                c = t * 8 + u
                lo = f_ref[0, pl.ds(c, pairs, stride=dim), :]
                hi = f_ref[1, pl.ds(c, pairs, stride=dim), :]
                out(c, h, jnp.concatenate([lo, hi], axis=0).astype(BF16))
            return 0

        lax.fori_loop(0, dim // 8, relayout, 0)


def triangle_half(jh, k, add, groups, a_ref, b_ref, o_ref):
    dim = a_ref.shape[0]
    pairs = a_ref.shape[1] // 2

    def step(t, _):
        for u in range(8):
            c = t * 8 + u
            o = lax.dot_general(a_ref[c, :, k], b_ref[jh, c, :, k], NT, preferred_element_type=F32)
            for e in range(2):
                part, at = o[e * pairs : (e + 1) * pairs], pl.ds(c, pairs, stride=dim)
                o_ref[e, at, :] = o_ref[e, at, :] + part if add else part
        return 0

    for lo, hi in groups or ((0, dim),):
        lax.fori_loop(lo // 8, hi // 8, step, 0)


def finish_half(l, jh, o_refs, g_ref, z_ref, wo_ref, vec_ref, store=None):
    pairs = z_ref.shape[1]
    dim = z_ref.shape[2]

    def step(p, _):
        at = pl.ds(pl.multiple_of(p * dim, dim), dim)
        o = sum(jnp.concatenate([o_ref[0, at, :], o_ref[1, at, :]], axis=1) for o_ref in o_refs)
        on = norm_rows(o, twice(vec_ref[l, V_NO0]), twice(vec_ref[l, V_NO1]))
        u = jnp.dot(wo_ref[l], on, preferred_element_type=F32) + twice(vec_ref[l, V_BO])
        z_new = (z_ref[jh, p].astype(F32) + g_ref[jh, p] * u.astype(BF16).astype(F32)).astype(BF16)
        if store is None:
            z_ref[jh, p] = z_new
        else:
            store(p, z_new.astype(F32))
        return 0

    lax.fori_loop(0, pairs, step, 0)


class Stream:
    def __init__(self, buf, color, lo, lanes, rows, sems, where):
        self.buf, self.color, self.rows, self.lanes = buf, color, rows, lanes
        self.base, self.size = lo
        self.part = buf.shape[0] // 2
        self.ring_send, self.ring_recv, self.core_send, self.core_recv = sems
        self.chip, self.core, self.chips = where
        self.sent = []

    def block(self, chip, part, piece=None):
        lo, n = part * self.part + self.base, self.size
        if piece is not None:
            n = n // 2
            lo = lo + piece * n
        rows = pl.ds(pl.multiple_of(chip * self.rows, self.rows), self.rows)
        return self.buf.at[pl.ds(lo, n), rows, self.lanes]

    def copy(self, ref, send, recv, chip, core):
        return pltpu.make_async_remote_copy(
            src_ref=ref, dst_ref=ref, send_sem=send, recv_sem=recv,
            device_id={"dap": chip * 2 + core}, device_id_type=pl.DeviceIdType.MESH)

    def near(self, step):
        return lax.rem(self.chip + step + self.chips, self.chips)

    def ring(self, side, hop, chip, piece=None):
        return self.copy(self.block(chip, self.core, piece), self.ring_send.at[side, hop], self.ring_recv.at[side, hop],
                         self.near(1 - 2 * side), self.core)

    def across(self, slot, chip, part, piece=None):
        return self.copy(self.block(chip, part, piece), self.core_send.at[slot], self.core_recv.at[slot],
                         self.chip, 1 - self.core)

    def event(self, hop):
        if hop == -1:
            @pl.when(self.core == self.color)
            def _():
                self.across(0, self.chip, 1 - self.core).start()
                for side in range(2):
                    self.ring(side, 0, self.chip).start()
                self.across(1, self.chip, self.core).start()
            return
        if hop == 0:
            @pl.when(self.core != self.color)
            def _():
                self.across(0, self.chip, self.core).wait_recv()
                for side in range(2):
                    self.ring(side, 0, self.chip).start()
            return
        last = self.chips // 2
        for side in range(2):
            origin = self.near((2 * side - 1) * hop)
            piece = side if hop == last else None
            self.ring(side, hop - 1, origin, piece).wait_recv()
            if hop < last:
                self.ring(side, hop, origin, side if hop == last - 1 else None).start()
            self.across(2 + 2 * (hop - 1) + side, origin, self.core, piece).start()

    def finish(self):
        last = self.chips // 2

        @pl.when(self.core != self.color)
        def _():
            self.across(1, self.chip, 1 - self.core).wait_recv()

        def hop_came(hop, _):
            for side in range(2):
                origin = self.near((2 * side - 1) * hop)
                self.across(2 * hop + side, origin, 1 - self.core).wait_recv()
            return 0

        lax.fori_loop(1, last, hop_came, 0)
        for side in range(2):
            self.across(2 * last + side, self.near(last), 1 - self.core, side).wait_recv()

    def drain(self):
        last = self.chips // 2

        @pl.when(self.core == self.color)
        def _():
            self.across(0, self.chip, 1 - self.core).wait_send()
            self.across(1, self.chip, self.core).wait_send()

        def hop_sent(hop, _):
            for side in range(2):
                self.ring(side, hop, self.chip).wait_send()
                self.across(2 + 2 * hop + side, self.chip, self.core).wait_send()
            return 0

        lax.fori_loop(0, last - 1, hop_sent, 0)
        for side in range(2):
            self.ring(side, last - 1, self.chip, side).wait_send()
            self.across(2 * last + side, self.chip, self.core, side).wait_send()


ORDER = (
    "p0", ("b100", -1), ("b101", -1), ("b100", 0), "p1", ("b110", -1), ("b101", 0), ("b110", 0), ("b111", -1),
    ("b100", 1), "p2", ("b110", 1), ("b111", 0), ("b101", 1), "p3", ("b100", 2), ("b121", -1), ("b120", -1), "vec",
    ("b120", 0), ("b111", 1), ("b121", 0), "w0", ("b110", 2), "mask", "pin", ("b101", 2), ("b120", 1), "q0",
    ("b100", 3), ("b110", 3), ("b121", 1), "q1", ("b100", 4), ("b120", 2), "q2", ("b111", 2), ("b121", 2), "q3",
    ("b120", 3), ("b20", -1), ("b101", 3), ("b20", 0), ("b110", 4), ("b111", 3), ("b21", -1), ("b121", 3),
    ("b21", 0), ("b120", 4), "w1", "O00a", ("b111", 4), "O00b", ("b20", 1), ("b101", 4), "O00p", ("b21", 1),
    ("b121", 4), "G00", "O01a", ("b20", 2), "O01b", ("b21", 2), "O01p", "G01", ("t110", -1), ("t101", -1),
    ("t100", -1), ("t100", 0), ("b20", 3), ("t101", 0), ("t110", 0), ("b20", 4), ("t100", 1), ("t101", 1),
    ("t100", 2), ("t101", 2), ("t100", 3), ("t111", -1), ("t101", 3), ("t100", 4), ("t111", 0), ("t110", 1),
    ("t101", 4), ("t111", 1), "T00", ("b21", 3), ("t110", 2), "N00", "O10a", ("t111", 2), "O10b", "O10p",
    ("t110", 3), "G10", ("t200", -1), ("t111", 3), ("t110", 4), ("t200", 0), ("t201", -1), ("t201", 0), ("b21", 4),
    ("t111", 4), ("t200", 1), "T01", ("t201", 1), "N01", "O11a", ("t200", 2), "O11b", "O11p", ("t201", 2), "G11",
    ("t210", -1), ("t210", 0), ("t200", 3), ("t201", 3), ("t210", 1), ("t2111", -1), ("t2110", -1), ("t200", 4),
    ("t2110", 0), "K0", ("t201", 4), ("t2111", 0), ("t210", 2), ("t2110", 1), ("t210", 3), ("t2111", 1), "K1",
    ("t2110", 2), ("t210", 4), ("t2111", 2), "L0", ("t2110", 3), "N10", ("t2111", 3), ("t2110", 4), "X10",
    ("t2111", 4), "L1a", "L1b", "Y11",
)
NEEDS = {
    "O00a": ("b100", "b110", "b120",),
    "O01a": ("b101", "b111", "b121",),
    "T00": ("t100", "t101",),
    "O10a": ("b20",),
    "T01": ("t110", "t111",),
    "O11a": ("b21",),
    "K0": ("t200",),
    "K1": ("t201",),
    "L0": ("t210",),
    "L1a": ("t2110",),
    "L1b": ("t2111",),
}
N_STREAMS = 17
N_LOADS = 28


def layers_kernel(chips, m_hbm, z_hbm, wq_hbm, wab_hbm, wgate_hbm, wout_hbm, w_in_ref, b_in_ref, opm_norm_ref, mask_in,
                  bq_ref, norm_in_ref, b_ab_ref, b_gate_ref, norm_out_ref, b_o_ref, out_hbm,
                  b_buf, t_buf, a_ref, z_ref, at_ref, g_ref, q_scr, fa, fb, b_scr, wq_ref, wall_ref, wo_ref, vec_ref,
                  bias_ref, mask_ref, ring_send, ring_recv, core_send, core_recv, local_sem, out_sem):
    me = lax.axis_index("dap")
    chip, core = me // 2, lax.rem(me, 2)
    rows, cols, dim = z_hbm.shape
    seqs = m_hbm.shape[0]
    layers = a_ref.shape[0]
    pairs = rows // 2
    half = cols // 2
    own = pl.ds(pl.multiple_of(chip * rows, rows), rows)

    barrier = pltpu.get_barrier_semaphore()
    right, left = lax.rem(chip + 1, chips), lax.rem(chip + chips - 1, chips)
    for there in (right * 2 + core, left * 2 + core, chip * 2 + 1 - core):
        pl.semaphore_signal(barrier, inc=1, device_id={"dap": there}, device_id_type=pl.DeviceIdType.MESH)

    used = [0]

    def load(src, dst):
        copy = pltpu.make_async_copy(src, dst, local_sem.at[used[0] % N_LOADS])
        used[0] += 1
        copy.start()
        return copy

    m_ref = t_buf.at[layers - 1, 0]
    z_raw = t_buf.at[layers - 1, 1]
    chunks = seqs // LANES
    m_loads = [load(m_hbm.at[pl.ds(a * LANES, LANES)], m_ref.at[:, pl.ds(a * rows, rows), :]) for a in range(chunks)]
    z_loads, w_loads = [], []

    def later_loads():
        z_loads.extend([load(z_hbm.at[:, pl.ds((2 * c + h) * rows, rows), :],
                        z_raw.at[pl.ds(0, rows), pl.ds(c * rows, rows), pl.ds(h * dim, dim)])
                   for h in range(2) for c in range(chips)])
        for l in range(layers):
            cd, ab = wq_hbm.shape[1], wab_hbm.shape[1]
            lanes = pl.ds(0, dim)
            w_loads.append(load(wq_hbm.at[l], q_scr.at[l, :, lanes]))
            w_loads.append(load(wab_hbm.at[l], q_scr.at[2 + l, pl.ds(0, ab), lanes]))
            w_loads.append(load(wgate_hbm.at[l], q_scr.at[4 + l, pl.ds(0, dim), lanes]))
            w_loads.append(load(wout_hbm.at[l], q_scr.at[4 + l, pl.ds(dim, dim), lanes]))

    where = (chip, core, chips)
    count = [0]

    def stream(buf, color, lo, lanes):
        sems = tuple(s.at[count[0]] for s in (ring_send, ring_recv, core_send, core_recv))
        count[0] += 1
        return Stream(buf, color, lo, lanes, rows, sems, where)

    width = b_buf.shape[2]
    full_b = pl.ds(0, seqs)
    full_t = pl.ds(0, cols)
    named = {}
    for s, (lo, n) in enumerate(((0, 1), (1, 1), (2, chunks - 2))):
        for q in range(2):
            named[f"b1{s}{q}"] = stream(b_buf.at[0, q], q, (0, width // 2), pl.ds(lo * LANES, n * LANES))
    for q in range(2):
        named[f"b2{q}"] = stream(b_buf.at[1, q], q, (0, width // 2), full_b)
        for s in range(2):
            named[f"t1{q}{s}"] = stream(t_buf.at[0, q], q, (s * dim // 4, dim // 4), full_t)
            if (s, q) != (1, 1):
                named[f"t2{s}{q}"] = stream(t_buf.at[1, q], q, (0, dim // 2), pl.ds(s * half, half))
            named[f"t211{s}"] = stream(t_buf.at[1, 1], 1, (s * dim // 4, dim // 4), pl.ds(half, half)) if q else None

    def column(row):
        return jnp.broadcast_to(row, (LANES, row.shape[1])).T

    for l in range(layers):
        for q in range(2):
            at = pl.ds(q * width, width)
            bias_ref[l, at, :] = column(b_in_ref[l].astype(F32)[q : q + 1])

    def project(l, chunk):
        def b_out(l, lanes, v):
            b_buf[l, core, :, own, lanes] = v

        project_rows(l, chunk, m_ref, w_in_ref, opm_norm_ref, bias_ref, a_ref, b_out, fa, fb, b_scr)

    def vectors():
        bq, b_gate, b_o = (r[...].astype(F32) for r in (bq_ref, b_gate_ref, b_o_ref))
        for l in range(layers):
            norm_in, b_ab, norm_out = (r[l].astype(F32) for r in (norm_in_ref, b_ab_ref, norm_out_ref))
            table = ((V_BQ, bq, l), (V_BP, b_ab, 2), (V_BG, b_ab, 3), (V_AP, b_ab, 0), (V_AG, b_ab, 1),
                     (V_GATE, b_gate, l), (V_NI0, norm_in, 0), (V_NI1, norm_in, 1), (V_NO0, norm_out, 0),
                     (V_NO1, norm_out, 1), (V_BO, b_o, l))
            for v, src, r in table:
                vec_ref[l, v] = column(src[r : r + 1])

    def masks():
        to = lax.broadcasted_iota(jnp.int32, (cols, cols), 1)
        frm = lax.broadcasted_iota(jnp.int32, (cols, cols), 0)
        q, rest = to // half, to % half
        perm = (frm == (rest // rows) * (2 * rows) + q * rows + rest % rows).astype(F32).astype(BF16)
        mask = jnp.dot(mask_in[...].astype(F32).astype(BF16), perm, preferred_element_type=F32)
        for h in range(2):
            mask_ref[h] = mask[:, h * half : (h + 1) * half]

    def weights(l):
        prepare_wq(l, q_scr.at[l, :, pl.ds(0, dim)], fa, wq_ref)
        ab = wab_hbm.shape[1]
        fa[0, 0:ab, :] = q_scr[2 + l, 0:ab, 0:dim].astype(F32)
        for slot, q in enumerate((2, 3, 0, 1)):
            wall_ref[l, slot * dim : (slot + 1) * dim, :] = fa[0, pl.ds(q, dim, stride=4), :].T.astype(BF16)
        wall_ref[l, 4 * dim : 5 * dim, :] = q_scr[4 + l, 0:dim, 0:dim].astype(F32).T.astype(BF16)
        wo_ref[l] = q_scr[4 + l, dim : 2 * dim, 0:dim].astype(F32).T.astype(BF16)

    def pair_in():
        def step(p, _):
            for h in range(2):
                for e in range(2):
                    x = z_raw[e * pairs + p, :, h * dim : (h + 1) * dim].astype(F32)
                    z_ref[h, p, :, e * half : (e + 1) * half] = x.T.astype(BF16)
            return 0

        lax.fori_loop(0, pairs, step, 0)

    def outer(l, h, part):
        outer_half(l, h, part, 2, a_ref, b_buf.at[l], q_scr)

    def opm(l, h):
        opm_half(l, h, wq_ref, vec_ref, z_ref, q_scr)

    def gate(l, h):
        def a_out(c, h, v):
            at_ref[l, c, :, h * LANES : (h + 1) * LANES] = v

        def b_out(c, h, v):
            t_buf[l, core, c, own, h * LANES : (h + 1) * LANES] = v

        gate_half(l, h, z_ref, mask_ref, wall_ref, vec_ref, fa, fb, g_ref, a_out, b_out)

    def triangle(l, jh, k=full_t, o_ref=fa, add=False, groups=None):
        triangle_half(jh, k, add, groups, at_ref.at[l], t_buf.at[l], o_ref)

    def finish(l, jh, *o_refs):
        finish_half(l, jh, o_refs or (fa,), g_ref, z_ref, wo_ref, vec_ref)

    def handed(h, p, e):
        row = e * pairs + p
        return pltpu.make_async_copy(at_ref.at[0, pl.ds(row * chips, chips), :, pl.ds(h * half, half)],
                                     out_hbm.at[row, :, h], out_sem.at[h, p, e])

    def last_columns(h, *o_refs):
        def store(p, x):
            for e in range(2):
                block = x[:, e * half : (e + 1) * half].T.astype(BF16).reshape(chips, rows, dim)
                at_ref[0, pl.ds((e * pairs + p) * chips, chips), :, h * half : (h + 1) * half] = block
            for e in range(2):
                handed(h, p, e).start()

        finish_half(layers - 1, h, o_refs, g_ref, z_ref, wo_ref, vec_ref, store)

    def first_project(chunk):
        m_loads[chunk].wait()
        if chunk == 0:
            later_loads()
        project(0, chunk)
        if chunk == 0:
            pl.semaphore_wait(barrier, 3)

    def first_weights():
        for copy in w_loads:
            copy.wait()
        weights(0)

    def first_pairs():
        for copy in z_loads:
            copy.wait()
        pair_in()

    tasks = {"vec": vectors, "mask": masks, "w0": first_weights, "w1": lambda: weights(1), "pin": first_pairs,
             "K0": lambda: triangle(1, 0, pl.ds(0, half)), "L0": lambda: triangle(1, 0, pl.ds(half, half), add=True),
             "K1": lambda: triangle(1, 1, pl.ds(0, half), fb), "N10": lambda: last_columns(0, fa), "Y11": lambda: last_columns(1, fa, fb),
             "X10": lambda: None}
    for s, letter in enumerate("ab"):
        groups = tuple((q * dim // 2 + s * dim // 4, q * dim // 2 + (s + 1) * dim // 4) for q in range(2))
        tasks[f"L1{letter}"] = functools.partial(triangle, 1, 1, pl.ds(half, half), fa, False, groups)
    for c in range(chunks):
        tasks[f"p{c}"] = functools.partial(first_project, c)
        tasks[f"q{c}"] = functools.partial(project, 1, c)
    for l in range(layers):
        for h in range(2):
            for part, letter in enumerate("ab"):
                tasks[f"O{l}{h}{letter}"] = functools.partial(outer, l, h, part)
            tasks[f"O{l}{h}p"] = functools.partial(opm, l, h)
            tasks[f"G{l}{h}"] = functools.partial(gate, l, h)
            tasks[f"T{l}{h}"] = functools.partial(triangle, l, h)
            tasks.setdefault(f"N{l}{h}", functools.partial(finish, l, h))
    for item in ORDER:
        if item in tasks:
            for name in NEEDS.get(item, ()):
                named[name].finish()
            tasks[item]()
        else:
            name, hop = item
            named[name].event(hop)
    for s in named.values():
        s.drain()

    def handed_over(p, _):
        for h in range(2):
            for e in range(2):
                handed(h, p, e).wait()
        return 0

    lax.fori_loop(0, pairs, handed_over, 0)


def solution(mesh):
    size = mesh.shape["dap"]
    chips = size // 2
    hops = chips // 2
    pair_spec = P(("batch", "dap"), None, None)
    mask_spec = P(("batch", "dap"), None)
    msa_spec = P(None, ("batch", "dap"), None)
    any_spec = pl.BlockSpec(memory_space=pl.ANY)
    vmem_spec = pl.BlockSpec(memory_space=pltpu.VMEM)

    def device_fn(pair_act, pair_mask, msa_act, opm_norm, opm_w_in, opm_b_in, opm_w_out, opm_b_out, tri_norm_in,
                  tri_w_ab, tri_b_ab, tri_w_gate, tri_b_gate, tri_norm_out, tri_w_out, tri_b_out):
        rows, cols, dim = pair_act.shape
        seqs, _, mdim = msa_act.shape
        layers = opm_norm.shape[0]
        width = opm_w_in.shape[-1]
        pairs = rows // 2
        half = cols // 2
        z_shape = (2, pairs, dim, 2 * half)

        w_in = jnp.transpose(opm_w_in, (0, 2, 3, 1)).reshape(layers, 2 * width, mdim)
        w_ab = tri_w_ab.reshape(layers, dim * 4, dim)

        return pl.pallas_call(
            functools.partial(layers_kernel, chips),
            out_shape=jax.ShapeDtypeStruct((rows, chips, 2, rows, dim), BF16),
            in_specs=[any_spec] * 6 + [vmem_spec] * 10,
            out_specs=any_spec,
            scratch_shapes=[pltpu.VMEM((layers, 2, width, half, seqs), BF16),
                            pltpu.VMEM((layers, 2, dim, half, cols), BF16),
                            pltpu.VMEM((layers, rows * width, seqs), BF16),
                            pltpu.VMEM(z_shape, BF16),
                            pltpu.VMEM((layers, dim, rows, cols), BF16),
                            pltpu.VMEM(z_shape, F32),
                            pltpu.VMEM((pairs, width * width, 2 * half), BF16),
                            pltpu.VMEM((2, pairs * dim, LANES), F32),
                            pltpu.VMEM((2, pairs * dim, LANES), F32),
                            pltpu.VMEM((width * rows, LANES), F32),
                            pltpu.VMEM((layers, dim, width * width), BF16),
                            pltpu.VMEM((layers, 5 * dim, dim), BF16),
                            pltpu.VMEM((layers, dim, dim), BF16),
                            pltpu.VMEM((layers, V_BIN, dim, LANES), F32),
                            pltpu.VMEM((layers, 2 * width, LANES), F32),
                            pltpu.VMEM((2, rows, half), F32),
                            pltpu.SemaphoreType.DMA((N_STREAMS, 2, hops)),
                            pltpu.SemaphoreType.DMA((N_STREAMS, 2, hops)),
                            pltpu.SemaphoreType.DMA((N_STREAMS, 2 + 2 * hops)),
                            pltpu.SemaphoreType.DMA((N_STREAMS, 2 + 2 * hops)),
                            pltpu.SemaphoreType.DMA((N_LOADS,)),
                            pltpu.SemaphoreType.DMA((2, pairs, 2))],
            compiler_params=pltpu.CompilerParams(vmem_limit_bytes=VMEM_LIMIT, collective_id=0, has_side_effects=True),
            name="layers",
        )(msa_act, pair_act, opm_w_out, w_ab, tri_w_gate, tri_w_out, w_in, opm_b_in, opm_norm, pair_mask,
          opm_b_out, tri_norm_in, tri_b_ab, tri_b_gate, tri_norm_out, tri_b_out).reshape(pair_act.shape)

    return jax.shard_map(device_fn, mesh=mesh, in_specs=(pair_spec, mask_spec, msa_spec) + (P(),) * 13,
                         out_specs=pair_spec, check_vma=False)
```

```python
import functools
import math

import jax
import jax.numpy as jnp
from jax import lax
from jax.experimental import pallas as pl
from jax.experimental.pallas import tpu as pltpu
from jax.sharding import PartitionSpec as P

F32 = jnp.float32
BF16 = jnp.bfloat16
EPS = 1e-5
VMEM_LIMIT = 63 * 1024 * 1024
NT = (((1,), (1,)), ((), ()))
LANES = 128

V_BQ, V_BP, V_BG, V_AP, V_AG, V_GATE, V_NI0, V_NI1, V_NO0, V_NO1, V_BO, V_BIN = range(12)


def sigmoid(x):
    return 1.0 / (1.0 + jnp.exp(-x))


def norm_rows(x, scale, offset):
    inv = 1.0 / x.shape[0]
    xc = x - jnp.sum(x, axis=0, keepdims=True) * inv
    var = jnp.sum(xc * xc, axis=0, keepdims=True) * inv
    return (xc * lax.rsqrt(var + EPS) * scale + offset).astype(BF16)


def twice(x):
    return jnp.concatenate([x, x], axis=1)


def project_rows(l, chunk, m_ref, w_ref, norm_ref, bias_ref, a_ref, b_out, xa, xb, scr):
    width = w_ref.shape[1] // 2
    dim = w_ref.shape[2]
    rows = scr.shape[0] // width
    depth = xa.shape[1] // rows
    block = 16
    scale, offset = norm_ref[l, 0:1].astype(F32), norm_ref[l, 1:2].astype(F32)

    at = pl.ds(chunk * rows, rows)
    lanes = pl.ds(chunk * LANES, LANES)

    for part, x_ref in enumerate((xa, xb)):
        def normalize(s, _):
            x = m_ref[pl.ds(part * depth + s * block, block), at, :].astype(F32).reshape(block * rows, dim)
            xc = x - jnp.sum(x, axis=1, keepdims=True) * (1.0 / dim)
            var = jnp.sum(xc * xc, axis=1, keepdims=True) * (1.0 / dim)
            xn = xc * lax.rsqrt(var + EPS)
            to = pl.ds(pl.multiple_of(s * block * rows, block * rows), block * rows)
            for f in range(dim // LANES):
                x_ref[f, to, :] = xn[:, f * LANES : (f + 1) * LANES]
            return 0

        lax.fori_loop(0, depth // block, normalize, 0)

    def residue(t2, _):
        for u in range(2):
            r = 2 * t2 + u
            xn = jnp.concatenate(
                [jnp.concatenate([x_ref[f, pl.ds(r, depth, stride=rows), :] for x_ref in (xa, xb)], axis=0)
                 for f in range(dim // LANES)], axis=1)
            mn = (xn * scale + offset).astype(BF16)
            out = lax.dot_general(w_ref[l], mn, NT, preferred_element_type=F32) + bias_ref[l]
            a_ref[l, pl.ds(pl.multiple_of(r * width, width), width), lanes] = out[:width].astype(BF16)
            scr[pl.ds(r, width, stride=rows), :] = out[width:]
        return 0

    lax.fori_loop(0, rows // 2, residue, 0)
    b_out(l, lanes, scr[...].astype(BF16).reshape(width, rows, LANES))


def prepare_wq(l, raw_ref, tmp_ref, wq_ref):
    cd = raw_ref.shape[0]
    width = math.isqrt(cd)
    tmp_ref[0, :, :] = raw_ref[...].astype(F32)
    for g in range(cd // LANES):
        per = LANES // width
        w = jnp.concatenate([tmp_ref[0, pl.ds(g * per + d, width, stride=width), :] for d in range(per)], axis=0)
        wq_ref[l, :, g * LANES : (g + 1) * LANES] = w.T.astype(BF16)


def outer_half(l, h, part, parts, a_ref, b_ref, q_ref):
    pairs, cd, lanes2 = q_ref.shape
    seqs = a_ref.shape[2]
    width = a_ref.shape[1] // (2 * pairs)
    half = lanes2 // 2
    scale = 1.0 / seqs

    def outer(t, _):
        rhs = b_ref[h, pl.ds(2 * t, 2)].reshape(2 * half, seqs)
        out = lax.dot_general(a_ref[l], rhs, NT, preferred_element_type=F32)
        out = (out * scale).astype(BF16)
        for d in range(2):
            blk = out[:, d * half : (d + 1) * half].reshape(2 * pairs, width, half)
            at = pl.ds(pl.multiple_of((2 * t + d) * width, width), width)
            for e in range(2):
                q_ref[:, at, e * half : (e + 1) * half] = blk[e * pairs : (e + 1) * pairs]
        return 0

    steps = cd // width // 2 // parts
    lax.fori_loop(part * steps, (part + 1) * steps, outer, 0)


def opm_half(l, h, wq_ref, vec_ref, z_ref, q_ref):
    pairs = q_ref.shape[0]
    bq = twice(vec_ref[l, V_BQ])

    def project(p, _):
        u = jnp.dot(wq_ref[l], q_ref[p], preferred_element_type=F32) + bq
        z_ref[h, p] = (z_ref[h, p].astype(F32) + u.astype(BF16).astype(F32)).astype(BF16)
        return 0

    lax.fori_loop(0, pairs, project, 0)


def gate_half(l, h, z_ref, mask_ref, wall_ref, vec_ref, fa_ref, fb_ref, g_ref, a_out, b_out):
    pairs = z_ref.shape[1]
    dim = z_ref.shape[2]
    half = z_ref.shape[3] // 2

    def project(p, _):
        zn = norm_rows(z_ref[h, p].astype(F32), twice(vec_ref[l, V_NI0]), twice(vec_ref[l, V_NI1]))
        mask = jnp.concatenate([mask_ref[h, pl.ds(p + e * pairs, 1), :] for e in range(2)], axis=1)
        at = pl.ds(pl.multiple_of(p * dim, dim), dim)

        def proj(q, v):
            w = wall_ref[l, q * dim : (q + 1) * dim]
            return jnp.dot(w, zn, preferred_element_type=F32) + twice(vec_ref[l, v])

        for q, f_ref, vp, vg in ((0, fb_ref, V_BP, V_BG), (2, fa_ref, V_AP, V_AG)):
            val = mask * sigmoid(proj(q + 1, vg)) * proj(q, vp)
            f_ref[0, at, :] = val[:, :half]
            f_ref[1, at, :] = val[:, half:]
        g_ref[h, p] = sigmoid(proj(4, V_GATE))
        return 0

    lax.fori_loop(0, pairs, project, 0)

    for f_ref, out in ((fb_ref, b_out), (fa_ref, a_out)):
        def relayout(t, _):
            for u in range(8):
                c = t * 8 + u
                lo = f_ref[0, pl.ds(c, pairs, stride=dim), :]
                hi = f_ref[1, pl.ds(c, pairs, stride=dim), :]
                out(c, h, jnp.concatenate([lo, hi], axis=0).astype(BF16))
            return 0

        lax.fori_loop(0, dim // 8, relayout, 0)


def triangle_half(jh, k, add, groups, a_ref, b_ref, o_ref):
    dim = a_ref.shape[0]
    pairs = a_ref.shape[1] // 2

    def step(t, _):
        for u in range(8):
            c = t * 8 + u
            o = lax.dot_general(a_ref[c, :, k], b_ref[jh, c, :, k], NT, preferred_element_type=F32)
            for e in range(2):
                part, at = o[e * pairs : (e + 1) * pairs], pl.ds(c, pairs, stride=dim)
                o_ref[e, at, :] = o_ref[e, at, :] + part if add else part
        return 0

    for lo, hi in groups or ((0, dim),):
        lax.fori_loop(lo // 8, hi // 8, step, 0)


def finish_half(l, jh, o_refs, g_ref, z_ref, wo_ref, vec_ref, store=None):
    pairs = z_ref.shape[1]
    dim = z_ref.shape[2]

    def step(p, _):
        at = pl.ds(pl.multiple_of(p * dim, dim), dim)
        o = sum(jnp.concatenate([o_ref[0, at, :], o_ref[1, at, :]], axis=1) for o_ref in o_refs)
        on = norm_rows(o, twice(vec_ref[l, V_NO0]), twice(vec_ref[l, V_NO1]))
        u = jnp.dot(wo_ref[l], on, preferred_element_type=F32) + twice(vec_ref[l, V_BO])
        z_new = (z_ref[jh, p].astype(F32) + g_ref[jh, p] * u.astype(BF16).astype(F32)).astype(BF16)
        if store is None:
            z_ref[jh, p] = z_new
        else:
            store(p, z_new.astype(F32))
        return 0

    lax.fori_loop(0, pairs, step, 0)


class Stream:
    def __init__(self, buf, color, lo, lanes, rows, sems, where):
        self.buf, self.color, self.rows, self.lanes = buf, color, rows, lanes
        self.base, self.size = lo
        self.part = buf.shape[0] // 2
        self.ring_send, self.ring_recv, self.core_send, self.core_recv = sems
        self.chip, self.core, self.chips = where
        self.sent = []

    def block(self, chip, part, piece=None):
        lo, n = part * self.part + self.base, self.size
        if piece is not None:
            n = n // 2
            lo = lo + piece * n
        rows = pl.ds(pl.multiple_of(chip * self.rows, self.rows), self.rows)
        return self.buf.at[pl.ds(lo, n), rows, self.lanes]

    def copy(self, ref, send, recv, chip, core):
        return pltpu.make_async_remote_copy(
            src_ref=ref, dst_ref=ref, send_sem=send, recv_sem=recv,
            device_id={"dap": chip * 2 + core}, device_id_type=pl.DeviceIdType.MESH)

    def near(self, step):
        return lax.rem(self.chip + step + self.chips, self.chips)

    def ring(self, side, hop, chip, piece=None):
        return self.copy(self.block(chip, self.core, piece), self.ring_send.at[side, hop], self.ring_recv.at[side, hop],
                         self.near(1 - 2 * side), self.core)

    def across(self, slot, chip, part, piece=None):
        return self.copy(self.block(chip, part, piece), self.core_send.at[slot], self.core_recv.at[slot],
                         self.chip, 1 - self.core)

    def event(self, hop):
        if hop == -1:
            @pl.when(self.core == self.color)
            def _():
                self.across(0, self.chip, 1 - self.core).start()
                for side in range(2):
                    self.ring(side, 0, self.chip).start()
                self.across(1, self.chip, self.core).start()
            return
        if hop == 0:
            @pl.when(self.core != self.color)
            def _():
                self.across(0, self.chip, self.core).wait_recv()
                for side in range(2):
                    self.ring(side, 0, self.chip).start()
            return
        last = self.chips // 2
        for side in range(2):
            origin = self.near((2 * side - 1) * hop)
            piece = side if hop == last else None
            self.ring(side, hop - 1, origin, piece).wait_recv()
            if hop < last:
                self.ring(side, hop, origin, side if hop == last - 1 else None).start()
            self.across(2 + 2 * (hop - 1) + side, origin, self.core, piece).start()

    def finish(self):
        last = self.chips // 2

        @pl.when(self.core != self.color)
        def _():
            self.across(1, self.chip, 1 - self.core).wait_recv()

        def hop_came(hop, _):
            for side in range(2):
                origin = self.near((2 * side - 1) * hop)
                self.across(2 * hop + side, origin, 1 - self.core).wait_recv()
            return 0

        lax.fori_loop(1, last, hop_came, 0)
        for side in range(2):
            self.across(2 * last + side, self.near(last), 1 - self.core, side).wait_recv()

    def drain(self):
        last = self.chips // 2

        @pl.when(self.core == self.color)
        def _():
            self.across(0, self.chip, 1 - self.core).wait_send()
            self.across(1, self.chip, self.core).wait_send()

        def hop_sent(hop, _):
            for side in range(2):
                self.ring(side, hop, self.chip).wait_send()
                self.across(2 + 2 * hop + side, self.chip, self.core).wait_send()
            return 0

        lax.fori_loop(0, last - 1, hop_sent, 0)
        for side in range(2):
            self.ring(side, last - 1, self.chip, side).wait_send()
            self.across(2 * last + side, self.chip, self.core, side).wait_send()


ORDER = (
    "p0", ("b101", -1), ("b100", -1), ("b100", 0), "p1", ("b110", -1), ("b110", 0), ("b101", 0), ("b111", -1),
    ("b100", 1), "p2", ("b111", 0), ("b110", 1), ("b101", 1), "p3", ("b121", -1), ("b120", -1), "vec", ("b121", 0),
    ("b120", 0), ("b100", 2), "w0", ("b110", 2), "mask", ("b111", 1), ("b101", 2), "pin", ("b120", 1), "q0",
    ("b100", 3), ("b121", 1), "q1", ("b101", 3), "q2", ("b120", 2), ("b110", 3), "q3", ("b121", 2), ("b100", 4),
    "w1", ("b111", 2), ("b120", 3), ("b20", -1), ("b20", 0), ("b121", 3), ("b21", -1), ("b120", 4), ("b110", 4),
    ("b21", 0), ("b111", 3), "O00a", ("b20", 1), ("b121", 4), ("b101", 4), "O00b", "O00p", ("b111", 4), ("b21", 1),
    "G00", ("b20", 2), "O01a", "O01b", ("b21", 2), "O01p", ("b20", 3), "G01", ("t100", -1), ("t101", -1),
    ("t110", -1), ("t100", 0), ("t101", 0), ("t100", 1), ("t110", 0), ("t101", 1), ("t100", 2), ("b20", 4),
    ("t101", 2), ("t111", -1), ("t100", 3), ("t101", 3), ("t111", 0), ("t110", 1), ("t100", 4), ("t101", 4),
    ("t111", 1), "T00", ("t110", 2), "N00", "O10a", ("t111", 2), "O10b", "O10p", ("b21", 3), ("t110", 3), "G10",
    ("t111", 3), ("t200", -1), ("t200", 0), ("t111", 4), ("t201", -1), ("t201", 0), ("t110", 4), ("t200", 1), "T01",
    ("b21", 4), "N01", ("t201", 1), "O11a", ("t200", 2), "O11b", ("t201", 2), "O11p", "G11", ("t2100", -1),
    ("t2111", -1), ("t2101", -1), ("t2100", 0), ("t2110", -1), ("t201", 3), ("t2100", 1), ("t2101", 0), ("t200", 3),
    ("t2111", 0), ("t201", 4), ("t2100", 2), ("t2110", 0), ("t200", 4), ("t2101", 1), ("t2100", 3), ("t2110", 1),
    "K0", ("t2101", 2), ("t2111", 1), "K1", ("t2110", 2), ("t2100", 4), ("t2101", 3), "L0a", ("t2111", 2),
    ("t2110", 3), ("t2101", 4), ("t2111", 3), "L0b", ("t2110", 4), "N10", "X10", ("t2111", 4), "L1a", "L1b", "Y11",
)
NEEDS = {
    "O00a": ("b100", "b110", "b120",),
    "O01a": ("b101", "b111", "b121",),
    "T00": ("t100", "t101",),
    "O10a": ("b20",),
    "T01": ("t110", "t111",),
    "O11a": ("b21",),
    "K0": ("t200",),
    "K1": ("t201",),
    "L0a": ("t2100",),
    "L0b": ("t2101",),
    "L1a": ("t2110",),
    "L1b": ("t2111",),
}
N_STREAMS = 18
N_LOADS = 28


def layers_kernel(chips, m_hbm, z_hbm, wq_hbm, wab_hbm, wgate_hbm, wout_hbm, w_in_ref, b_in_ref, opm_norm_ref, mask_in,
                  bq_ref, norm_in_ref, b_ab_ref, b_gate_ref, norm_out_ref, b_o_ref, out_hbm,
                  b_buf, t_buf, a_ref, z_ref, at_ref, g_ref, q_scr, fa, fb, b_scr, wq_ref, wall_ref, wo_ref, vec_ref,
                  bias_ref, mask_ref, ring_send, ring_recv, core_send, core_recv, local_sem, out_sem):
    me = lax.axis_index("dap")
    chip, core = me // 2, lax.rem(me, 2)
    rows, cols, dim = z_hbm.shape
    seqs = m_hbm.shape[0]
    layers = a_ref.shape[0]
    pairs = rows // 2
    half = cols // 2
    own = pl.ds(pl.multiple_of(chip * rows, rows), rows)

    barrier = pltpu.get_barrier_semaphore()
    right, left = lax.rem(chip + 1, chips), lax.rem(chip + chips - 1, chips)
    for there in (right * 2 + core, left * 2 + core, chip * 2 + 1 - core):
        pl.semaphore_signal(barrier, inc=1, device_id={"dap": there}, device_id_type=pl.DeviceIdType.MESH)

    used = [0]

    def load(src, dst):
        copy = pltpu.make_async_copy(src, dst, local_sem.at[used[0] % N_LOADS])
        used[0] += 1
        copy.start()
        return copy

    m_ref = t_buf.at[layers - 1, 0]
    z_raw = t_buf.at[layers - 1, 1]
    chunks = seqs // LANES
    m_loads = [load(m_hbm.at[pl.ds(a * LANES, LANES)], m_ref.at[:, pl.ds(a * rows, rows), :]) for a in range(chunks)]
    z_loads, w_loads = [], []

    def later_loads():
        z_loads.extend([load(z_hbm.at[:, pl.ds((2 * c + h) * rows, rows), :],
                        z_raw.at[pl.ds(0, rows), pl.ds(c * rows, rows), pl.ds(h * dim, dim)])
                   for h in range(2) for c in range(chips)])
        for l in range(layers):
            cd, ab = wq_hbm.shape[1], wab_hbm.shape[1]
            lanes = pl.ds(0, dim)
            w_loads.append(load(wq_hbm.at[l], q_scr.at[l, :, lanes]))
            w_loads.append(load(wab_hbm.at[l], q_scr.at[2 + l, pl.ds(0, ab), lanes]))
            w_loads.append(load(wgate_hbm.at[l], q_scr.at[4 + l, pl.ds(0, dim), lanes]))
            w_loads.append(load(wout_hbm.at[l], q_scr.at[4 + l, pl.ds(dim, dim), lanes]))

    where = (chip, core, chips)
    count = [0]

    def stream(buf, color, lo, lanes):
        sems = tuple(s.at[count[0]] for s in (ring_send, ring_recv, core_send, core_recv))
        count[0] += 1
        return Stream(buf, color, lo, lanes, rows, sems, where)

    width = b_buf.shape[2]
    full_b = pl.ds(0, seqs)
    full_t = pl.ds(0, cols)
    named = {}
    for s, (lo, n) in enumerate(((0, 1), (1, 1), (2, chunks - 2))):
        for q in range(2):
            named[f"b1{s}{q}"] = stream(b_buf.at[0, q], q, (0, width // 2), pl.ds(lo * LANES, n * LANES))
    for q in range(2):
        named[f"b2{q}"] = stream(b_buf.at[1, q], q, (0, width // 2), full_b)
        for s in range(2):
            named[f"t1{q}{s}"] = stream(t_buf.at[0, q], q, (s * dim // 4, dim // 4), full_t)
            named[f"t21{q}{s}"] = stream(t_buf.at[1, q], q, (s * dim // 4, dim // 4), pl.ds(half, half))
        named[f"t20{q}"] = stream(t_buf.at[1, q], q, (0, dim // 2), pl.ds(0, half))

    def column(row):
        return jnp.broadcast_to(row, (LANES, row.shape[1])).T

    for l in range(layers):
        for q in range(2):
            at = pl.ds(q * width, width)
            bias_ref[l, at, :] = column(b_in_ref[l].astype(F32)[q : q + 1])

    def project(l, chunk):
        def b_out(l, lanes, v):
            b_buf[l, core, :, own, lanes] = v

        project_rows(l, chunk, m_ref, w_in_ref, opm_norm_ref, bias_ref, a_ref, b_out, fa, fb, b_scr)

    def vectors():
        bq, b_gate, b_o = (r[...].astype(F32) for r in (bq_ref, b_gate_ref, b_o_ref))
        for l in range(layers):
            norm_in, b_ab, norm_out = (r[l].astype(F32) for r in (norm_in_ref, b_ab_ref, norm_out_ref))
            table = ((V_BQ, bq, l), (V_BP, b_ab, 2), (V_BG, b_ab, 3), (V_AP, b_ab, 0), (V_AG, b_ab, 1),
                     (V_GATE, b_gate, l), (V_NI0, norm_in, 0), (V_NI1, norm_in, 1), (V_NO0, norm_out, 0),
                     (V_NO1, norm_out, 1), (V_BO, b_o, l))
            for v, src, r in table:
                vec_ref[l, v] = column(src[r : r + 1])

    def masks():
        to = lax.broadcasted_iota(jnp.int32, (cols, cols), 1)
        frm = lax.broadcasted_iota(jnp.int32, (cols, cols), 0)
        q, rest = to // half, to % half
        perm = (frm == (rest // rows) * (2 * rows) + q * rows + rest % rows).astype(F32).astype(BF16)
        mask = jnp.dot(mask_in[...].astype(F32).astype(BF16), perm, preferred_element_type=F32)
        for h in range(2):
            mask_ref[h] = mask[:, h * half : (h + 1) * half]

    def weights(l):
        prepare_wq(l, q_scr.at[l, :, pl.ds(0, dim)], fa, wq_ref)
        ab = wab_hbm.shape[1]
        fa[0, 0:ab, :] = q_scr[2 + l, 0:ab, 0:dim].astype(F32)
        for slot, q in enumerate((2, 3, 0, 1)):
            wall_ref[l, slot * dim : (slot + 1) * dim, :] = fa[0, pl.ds(q, dim, stride=4), :].T.astype(BF16)
        wall_ref[l, 4 * dim : 5 * dim, :] = q_scr[4 + l, 0:dim, 0:dim].astype(F32).T.astype(BF16)
        wo_ref[l] = q_scr[4 + l, dim : 2 * dim, 0:dim].astype(F32).T.astype(BF16)

    def pair_in():
        def step(p, _):
            for h in range(2):
                for e in range(2):
                    x = z_raw[e * pairs + p, :, h * dim : (h + 1) * dim].astype(F32)
                    z_ref[h, p, :, e * half : (e + 1) * half] = x.T.astype(BF16)
            return 0

        lax.fori_loop(0, pairs, step, 0)

    def outer(l, h, part):
        outer_half(l, h, part, 2, a_ref, b_buf.at[l], q_scr)

    def opm(l, h):
        opm_half(l, h, wq_ref, vec_ref, z_ref, q_scr)

    def gate(l, h):
        def a_out(c, h, v):
            at_ref[l, c, :, h * LANES : (h + 1) * LANES] = v

        def b_out(c, h, v):
            t_buf[l, core, c, own, h * LANES : (h + 1) * LANES] = v

        gate_half(l, h, z_ref, mask_ref, wall_ref, vec_ref, fa, fb, g_ref, a_out, b_out)

    def triangle(l, jh, k=full_t, o_ref=fa, add=False, groups=None):
        triangle_half(jh, k, add, groups, at_ref.at[l], t_buf.at[l], o_ref)

    def finish(l, jh, *o_refs):
        finish_half(l, jh, o_refs or (fa,), g_ref, z_ref, wo_ref, vec_ref)

    def handed(h, p, e):
        row = e * pairs + p
        return pltpu.make_async_copy(at_ref.at[0, pl.ds(row * chips, chips), :, pl.ds(h * half, half)],
                                     out_hbm.at[row, :, h], out_sem.at[h, p, e])

    def last_columns(h, *o_refs):
        def store(p, x):
            for e in range(2):
                block = x[:, e * half : (e + 1) * half].T.astype(BF16).reshape(chips, rows, dim)
                at_ref[0, pl.ds((e * pairs + p) * chips, chips), :, h * half : (h + 1) * half] = block
            for e in range(2):
                handed(h, p, e).start()

        finish_half(layers - 1, h, o_refs, g_ref, z_ref, wo_ref, vec_ref, store)

    def first_project(chunk):
        m_loads[chunk].wait()
        if chunk == 0:
            later_loads()
        project(0, chunk)
        if chunk == 0:
            pl.semaphore_wait(barrier, 3)

    def first_weights():
        for copy in w_loads:
            copy.wait()
        weights(0)

    def first_pairs():
        for copy in z_loads:
            copy.wait()
        pair_in()

    tasks = {"vec": vectors, "mask": masks, "w0": first_weights, "w1": lambda: weights(1), "pin": first_pairs,
             "K0": lambda: triangle(1, 0, pl.ds(0, half)),
             "K1": lambda: triangle(1, 1, pl.ds(0, half), fb), "N10": lambda: last_columns(0, fa), "Y11": lambda: last_columns(1, fa, fb),
             "X10": lambda: None}
    for s, letter in enumerate("ab"):
        groups = tuple((q * dim // 2 + s * dim // 4, q * dim // 2 + (s + 1) * dim // 4) for q in range(2))
        tasks[f"L0{letter}"] = functools.partial(triangle, 1, 0, pl.ds(half, half), fa, True, groups)
        tasks[f"L1{letter}"] = functools.partial(triangle, 1, 1, pl.ds(half, half), fa, False, groups)
    for c in range(chunks):
        tasks[f"p{c}"] = functools.partial(first_project, c)
        tasks[f"q{c}"] = functools.partial(project, 1, c)
    for l in range(layers):
        for h in range(2):
            for part, letter in enumerate("ab"):
                tasks[f"O{l}{h}{letter}"] = functools.partial(outer, l, h, part)
            tasks[f"O{l}{h}p"] = functools.partial(opm, l, h)
            tasks[f"G{l}{h}"] = functools.partial(gate, l, h)
            tasks[f"T{l}{h}"] = functools.partial(triangle, l, h)
            tasks.setdefault(f"N{l}{h}", functools.partial(finish, l, h))
    for item in ORDER:
        if item in tasks:
            for name in NEEDS.get(item, ()):
                named[name].finish()
            tasks[item]()
        else:
            name, hop = item
            named[name].event(hop)
    for s in named.values():
        s.drain()

    def handed_over(p, _):
        for h in range(2):
            for e in range(2):
                handed(h, p, e).wait()
        return 0

    lax.fori_loop(0, pairs, handed_over, 0)


def solution(mesh):
    size = mesh.shape["dap"]
    chips = size // 2
    hops = chips // 2
    pair_spec = P(("batch", "dap"), None, None)
    mask_spec = P(("batch", "dap"), None)
    msa_spec = P(None, ("batch", "dap"), None)
    any_spec = pl.BlockSpec(memory_space=pl.ANY)
    vmem_spec = pl.BlockSpec(memory_space=pltpu.VMEM)

    def device_fn(pair_act, pair_mask, msa_act, opm_norm, opm_w_in, opm_b_in, opm_w_out, opm_b_out, tri_norm_in,
                  tri_w_ab, tri_b_ab, tri_w_gate, tri_b_gate, tri_norm_out, tri_w_out, tri_b_out):
        rows, cols, dim = pair_act.shape
        seqs, _, mdim = msa_act.shape
        layers = opm_norm.shape[0]
        width = opm_w_in.shape[-1]
        pairs = rows // 2
        half = cols // 2
        z_shape = (2, pairs, dim, 2 * half)

        w_in = jnp.transpose(opm_w_in, (0, 2, 3, 1)).reshape(layers, 2 * width, mdim)
        w_ab = tri_w_ab.reshape(layers, dim * 4, dim)

        return pl.pallas_call(
            functools.partial(layers_kernel, chips),
            out_shape=jax.ShapeDtypeStruct((rows, chips, 2, rows, dim), BF16),
            in_specs=[any_spec] * 6 + [vmem_spec] * 10,
            out_specs=any_spec,
            scratch_shapes=[pltpu.VMEM((layers, 2, width, half, seqs), BF16),
                            pltpu.VMEM((layers, 2, dim, half, cols), BF16),
                            pltpu.VMEM((layers, rows * width, seqs), BF16),
                            pltpu.VMEM(z_shape, BF16),
                            pltpu.VMEM((layers, dim, rows, cols), BF16),
                            pltpu.VMEM(z_shape, F32),
                            pltpu.VMEM((pairs, width * width, 2 * half), BF16),
                            pltpu.VMEM((2, pairs * dim, LANES), F32),
                            pltpu.VMEM((2, pairs * dim, LANES), F32),
                            pltpu.VMEM((width * rows, LANES), F32),
                            pltpu.VMEM((layers, dim, width * width), BF16),
                            pltpu.VMEM((layers, 5 * dim, dim), BF16),
                            pltpu.VMEM((layers, dim, dim), BF16),
                            pltpu.VMEM((layers, V_BIN, dim, LANES), F32),
                            pltpu.VMEM((layers, 2 * width, LANES), F32),
                            pltpu.VMEM((2, rows, half), F32),
                            pltpu.SemaphoreType.DMA((N_STREAMS, 2, hops)),
                            pltpu.SemaphoreType.DMA((N_STREAMS, 2, hops)),
                            pltpu.SemaphoreType.DMA((N_STREAMS, 2 + 2 * hops)),
                            pltpu.SemaphoreType.DMA((N_STREAMS, 2 + 2 * hops)),
                            pltpu.SemaphoreType.DMA((N_LOADS,)),
                            pltpu.SemaphoreType.DMA((2, pairs, 2))],
            compiler_params=pltpu.CompilerParams(vmem_limit_bytes=VMEM_LIMIT, collective_id=0, has_side_effects=True),
            name="layers",
        )(msa_act, pair_act, opm_w_out, w_ab, tri_w_gate, tri_w_out, w_in, opm_b_in, opm_norm, pair_mask,
          opm_b_out, tri_norm_in, tri_b_ab, tri_b_gate, tri_norm_out, tri_b_out).reshape(pair_act.shape)

    return jax.shard_map(device_fn, mesh=mesh, in_specs=(pair_spec, mask_spec, msa_spec) + (P(),) * 13,
                         out_specs=pair_spec, check_vma=False)
```
